256 devices in a mesh: enc: 32 (over z, x), tp: 8 (over y, core).
Axes of the slice: x: 4, y: 4, z: 8, core: 2. Of those that a mesh axis runs over, the one named last changes fastest.
Arguments:
- grad_rows: bfloat16 [20480, 8192], P('enc', 'tp'), may hold values from -6 to 6
- features: bfloat16 [20480, 1280], P('enc'), may hold values from -6 to 6
- block_in: bfloat16 [20480, 1280], P('enc', 'tp'), may hold values from -6 to 6
- patch_counts: int32 [32, 5], replicated, may hold values from 32 to 128, as said below
- owner: int32 [32, 5], replicated, may hold values from 0 to 31, as said below
- ln1_gain: float32 [1280], replicated, may hold values from 0.5 to 1.5
- w_qkv: bfloat16 [1280, 16, 240], P(None, 'tp')
- w_out: bfloat16 [1280, 1280], P('tp'), may hold values from -0.15625 to 0.15625
- w_proj: bfloat16 [1280, 8192], P(None, 'tp'), may hold values from -0.15625 to 0.15625
Outputs:
- grad_input: bfloat16 [20480, 1280], P('enc', 'tp')
- grad_proj: float32 [1280, 8192], P('enc', 'tp')
- grad_qkv: float32 [1280, 16, 240], P('enc', 'tp')
- grad_out: float32 [1280, 1280], P('tp', 'enc')
- grad_ln1: float32 [1280], P('enc')
The draws below stay inside these ranges and needn't reach their ends.
Inputs may be any that keep to these rules, and one draw needn't show every extreme that they name: `patch_counts`: some image has exactly 128 live rows and some exactly 32. `owner`: each encoder device receives exactly 5 images, never two from the same block.
All inputs are finite; a program needn't handle non-finite values.
Results may differ from the reference program's by a relative error of at most 0.033.
Values may be sent and summed in bfloat16 or wider, within the bound.
No kernel may reach another device: no remote copies, remote signals or barrier semaphores. Data moves between devices by JAX's collectives and lax.ppermute only.
A program may use at most 64 MiB of HBM per device.

```python
import math
import jax
import jax.numpy as jnp
from jax import lax

D_LLM = 8192
D_VIT = 1280
HEADS = 16
HEAD_DIM = 80
TILE = 128
IMG_GROUP = 5
ROWS_DEV = 640
ROWS_ALL = 20480
N_ENC = 32
N_TP = 8


def image_plan(key):
    count_key, first_key, second_key, third_key = jax.random.split(jax.random.fold_in(key, 31), 4)
    counts = jax.random.randint(count_key, (N_ENC, IMG_GROUP), TILE // 4, TILE + 1).astype(jnp.int32)
    counts = counts.at[0, 0].set(TILE).at[N_ENC - 1, IMG_GROUP - 1].set(TILE // 4)
    targets = jax.random.permutation(first_key, N_ENC).astype(jnp.int32)
    starts = jax.random.permutation(second_key, N_ENC).astype(jnp.int32)
    offsets = jax.random.permutation(third_key, N_ENC).astype(jnp.int32)[:IMG_GROUP]
    positions = (starts[:, None] + offsets[None, :]) % N_ENC
    owners = jnp.take(targets, positions.reshape(-1)).reshape(N_ENC, IMG_GROUP)
    return (counts, owners.astype(jnp.int32))


def draw_patch_counts(key, part):
    return image_plan(key)[0]


def draw_owner(key, part):
    return image_plan(key)[1]


def draw_w_qkv(key, part):
    gaussian = jax.random.normal(jax.random.fold_in(key, 5), (D_VIT, HEADS, 3 * HEAD_DIM), jnp.float32) / math.sqrt(D_VIT)
    return gaussian.astype(jnp.bfloat16)


def block_levels(key, dims, cuts, smallest, top_value):
    def one(axis_at, blocks):
        heights = jax.random.uniform(jax.random.fold_in(jax.random.fold_in(key, 6), axis_at), (blocks,), jnp.float32, smallest / len(cuts), top_value / len(cuts))
        return jnp.repeat(jnp.exp(heights), dims[axis_at] // blocks).reshape((-1,) + (1,) * (len(dims) - axis_at - 1))

    factor_of = one(*cuts[0])
    for cut in cuts[1:]:
        factor_of = factor_of * one(*cut)
    return factor_of


def scatter_about(stream_key, dims, width, most, cuts=(), kind=jnp.bfloat16):
    entries = width * jax.random.normal(stream_key, dims, jnp.float32)
    if cuts:
        entries = entries * block_levels(stream_key, dims, cuts, -0.22, 0.18)
    return jnp.clip(entries, -most, most).astype(kind)


def setup_inputs(seed: int = 0) -> dict:
    keys = jax.random.split(jax.random.key(seed), 10)
    grad_rows = scatter_about(keys[0], (ROWS_ALL, D_LLM), 1.0, 6.0, ((0, 32), (1, 8)))
    features = scatter_about(keys[1], (ROWS_ALL, D_VIT), 1.0, 6.0, ((0, 32),))
    block_in = scatter_about(keys[2], (ROWS_ALL, D_VIT), 1.0, 6.0, ((0, 32), (1, 8)))
    patch_counts = draw_patch_counts(jax.random.fold_in(keys[9], 71), 0)
    owner = draw_owner(jax.random.fold_in(keys[9], 71), 0)
    ln1_gain = jnp.clip(1.0 + 0.1 * jax.random.normal(keys[5], (D_VIT,), jnp.float32), 0.5, 1.5)
    w_qkv = draw_w_qkv(jax.random.fold_in(keys[9], 71), 0)
    w_out = scatter_about(keys[7], (D_VIT, D_VIT), D_VIT ** -0.5, 0.15625, ((0, 8),))
    w_proj = scatter_about(keys[8], (D_VIT, D_LLM), D_VIT ** -0.5, 0.15625, ((1, 8),))
    return {"grad_rows": grad_rows, "features": features, "block_in": block_in, "patch_counts": patch_counts, "owner": owner, "ln1_gain": ln1_gain, "w_qkv": w_qkv, "w_out": w_out, "w_proj": w_proj}


EPSILON = 1e-05

def chop(values):
    return lax.optimization_barrier(values.astype(jnp.bfloat16)).astype(jnp.float32)

def normalize(values):
    centred = values - lax.optimization_barrier(jnp.mean(values, axis=-1, keepdims=True))
    variance = lax.optimization_barrier(jnp.mean(centred * centred, axis=-1, keepdims=True))
    inverse = lax.rsqrt(variance + EPSILON)
    return (centred * inverse, inverse)

def norm_back(incoming, normed, inverse, gain):
    scaled = incoming * gain
    inner_mean = lax.optimization_barrier(jnp.mean(scaled * normed, axis=-1, keepdims=True))
    outgoing = inverse * (scaled - lax.optimization_barrier(jnp.mean(scaled, axis=-1, keepdims=True)) - normed * inner_mean)
    return (outgoing, lax.optimization_barrier(jnp.sum(incoming * normed, axis=0)))

def block_backward(block_x, upstream_f, live, ln1_gain, w_qkv, w_out):
    rows_here = block_x.shape[0]
    normed1, inverse1 = normalize(block_x.astype(jnp.float32))
    normed_in = (normed1 * ln1_gain).astype(jnp.bfloat16)
    qkv_flat = w_qkv.reshape(D_VIT, HEADS * 3 * HEAD_DIM)
    packed = jnp.dot(normed_in, qkv_flat, preferred_element_type=jnp.float32).astype(jnp.bfloat16)
    packed = packed.reshape(IMG_GROUP, TILE, HEADS, 3, HEAD_DIM)
    queries = packed[:, :, :, 0, :].astype(jnp.float32)
    keys_part = packed[:, :, :, 1, :].astype(jnp.float32)
    values_part = packed[:, :, :, 2, :].astype(jnp.float32)
    scaling = 1.0 / HEAD_DIM ** 0.5
    scores = jnp.einsum('gqhd,gkhd->ghqk', queries, keys_part) * scaling
    same_kind = (live[:, :, None] == live[:, None, :])[:, None]
    scores = jnp.where(same_kind, scores, -1e+30)
    row_max = lax.optimization_barrier(jnp.max(scores, axis=-1, keepdims=True))
    exp_terms = jnp.exp(scores - row_max)
    probability = exp_terms / lax.optimization_barrier(jnp.sum(exp_terms, axis=-1, keepdims=True))
    prob_low = probability.astype(jnp.bfloat16)
    mixed = jnp.einsum('ghqk,gkhd->gqhd', prob_low.astype(jnp.float32), values_part).astype(jnp.bfloat16)
    mixed = mixed.reshape(rows_here, HEADS * HEAD_DIM)
    middle_b = upstream_f.astype(jnp.bfloat16)
    out_term = jnp.dot(mixed.T, middle_b, preferred_element_type=jnp.float32)
    mixed_grad = jnp.dot(middle_b, w_out.T, preferred_element_type=jnp.float32).astype(jnp.bfloat16)
    mixed_grad = mixed_grad.reshape(IMG_GROUP, TILE, HEADS, HEAD_DIM).astype(jnp.float32)
    prob_grad = jnp.einsum('gqhd,gkhd->ghqk', mixed_grad, values_part)
    score_grad = probability * (prob_grad - lax.optimization_barrier(jnp.sum(probability * prob_grad, axis=-1, keepdims=True))) * scaling
    score_grad = score_grad.astype(jnp.bfloat16).astype(jnp.float32)
    q_grad = jnp.einsum('ghqk,gkhd->gqhd', score_grad, keys_part)
    k_grad = jnp.einsum('ghqk,gqhd->gkhd', score_grad, queries)
    v_grad = jnp.einsum('ghqk,gqhd->gkhd', prob_low.astype(jnp.float32), mixed_grad)
    packed_grad = jnp.stack([q_grad, k_grad, v_grad], axis=3).astype(jnp.bfloat16)
    packed_grad = packed_grad.reshape(rows_here, HEADS * 3 * HEAD_DIM)
    qkv_term = jnp.dot(normed_in.T, packed_grad, preferred_element_type=jnp.float32).reshape(D_VIT, HEADS, 3 * HEAD_DIM)
    heads_rank = HEADS // N_TP
    attn_parts = jnp.einsum('rtj,ctj->trc', packed_grad.reshape(rows_here, N_TP, heads_rank * 3 * HEAD_DIM).astype(jnp.float32), w_qkv.reshape(D_VIT, N_TP, heads_rank * 3 * HEAD_DIM).astype(jnp.float32))
    in_sum = lax.optimization_barrier(jnp.sum(chop(attn_parts), axis=0))
    in_back, ln1_term = norm_back(in_sum, normed1, inverse1, ln1_gain)
    grad_block = (upstream_f + in_back).astype(jnp.bfloat16)
    return ((qkv_term, out_term, ln1_term), grad_block)

def reference(grad_rows, features, block_in, patch_counts, owner, ln1_gain, w_qkv, w_out, w_proj):
    items = N_ENC * IMG_GROUP
    counts = patch_counts.reshape(-1).astype(jnp.int32)
    peers = jnp.arange(N_ENC, dtype=jnp.int32)
    sends = jnp.any(owner[:, :, None] == peers[None, None, :], axis=1).astype(jnp.int32)
    rank = (jnp.cumsum(sends, axis=0) - sends).astype(jnp.int32)
    own_rank = jnp.take_along_axis(rank, owner.astype(jnp.int32), axis=1)
    dest = (owner * IMG_GROUP + own_rank).reshape(-1).astype(jnp.int32)
    line = jnp.arange(TILE, dtype=jnp.int32)
    live_src = line[None, :] < counts[:, None]
    block_llm = D_LLM // N_TP
    vis_grad = jnp.zeros((N_ENC * ROWS_DEV, D_VIT), jnp.float32)
    for tp_block in range(N_TP):
        partial_value = jnp.dot(grad_rows[:, tp_block * block_llm:(tp_block + 1) * block_llm], w_proj[:, tp_block * block_llm:(tp_block + 1) * block_llm].T, preferred_element_type=jnp.float32)
        vis_grad = vis_grad + chop(partial_value)
    vis_tiles = jnp.where(live_src[:, :, None], vis_grad.reshape(items, TILE, D_VIT), jnp.zeros((), jnp.float32))
    upstream = jnp.zeros((items, TILE, D_VIT), jnp.float32).at[dest].set(vis_tiles).reshape(N_ENC * ROWS_DEV, D_VIT)
    dest_counts = jnp.zeros((items,), jnp.int32).at[dest].set(counts)
    live_dest = (line[None, :] < dest_counts[:, None]).reshape(N_ENC, IMG_GROUP, TILE)
    kept_rows = jnp.where(live_src.reshape(-1)[:, None], features, jnp.zeros_like(features))

    def add_projector(running, pair_rows):
        return (running + chop(jnp.dot(pair_rows[0].T, pair_rows[1], preferred_element_type=jnp.float32)), None)
    grad_proj = lax.scan(add_projector, jnp.zeros((D_VIT, D_LLM), jnp.float32), (kept_rows.reshape(N_ENC, ROWS_DEV, D_VIT), grad_rows.reshape(N_ENC, ROWS_DEV, D_LLM)))[0]

    def add_term(running_sum, new_term):
        return running_sum + chop(new_term)

    def one_block(running, pieces):
        terms, grad_block = block_backward(pieces[0], pieces[1], pieces[2], ln1_gain, w_qkv, w_out)
        return (jax.tree.map(add_term, running, terms), grad_block)
    start_sums = (jnp.zeros((D_VIT, HEADS, 3 * HEAD_DIM), jnp.float32), jnp.zeros((D_VIT, D_VIT), jnp.float32), jnp.zeros((D_VIT,), jnp.float32))
    sums_out, grad_blocks = lax.scan(one_block, start_sums, (block_in.reshape(N_ENC, ROWS_DEV, D_VIT), upstream.reshape(N_ENC, ROWS_DEV, D_VIT), live_dest))
    grad_input = grad_blocks.reshape(N_ENC * ROWS_DEV, D_VIT)
    return (grad_input, grad_proj, sums_out[0], sums_out[1], sums_out[2])
```

```python
import jax
import jax.numpy as jnp
from jax import lax
from jax.experimental import pallas as pl
from jax.experimental.pallas import tpu as pltpu
from jax.sharding import Mesh
from jax.sharding import PartitionSpec as P

TILE = 128
IMG = 5
ROWS = IMG * TILE
WIDTH = 1280
HEAD = 80
LANE = 128
PEERS = 32
ENC = ("z", "x")
TP = ("y", "c")
EPSILON = 1e-05
SCALING = 1.0 / HEAD**0.5
BF = jnp.bfloat16
F32 = jnp.float32
SWAP = ((0, 1), (1, 0))


def exchanged(blocks, axis):
    return lax.all_to_all(blocks, axis, split_axis=0, concat_axis=0, tiled=True)


def dot(left, right, dim_left, dim_right):
    return lax.dot_general(
        left, right, (((dim_left,), (dim_right,)), ((), ())), preferred_element_type=F32
    )


def smem():
    return pl.BlockSpec(memory_space=pltpu.SMEM)


def normalize(values):
    centred = values - jnp.mean(values, axis=-1, keepdims=True)
    variance = jnp.mean(centred * centred, axis=-1, keepdims=True)
    inverse = lax.rsqrt(variance + EPSILON)
    return (centred * inverse, inverse)


def shifted_sum(pieces, lanes):
    total = None
    for at, piece in enumerate(pieces):
        wide = jnp.concatenate(
            [piece, jnp.zeros((piece.shape[0], lanes - LANE), piece.dtype)], axis=1
        )
        if at:
            wide = pltpu.roll(wide, HEAD * at, 1)
        total = wide if total is None else total + wide
    return total


def spread_kernel(place_ref, counts_ref, arrived_ref, out_ref):
    first_row = place_ref[0] * 16
    for image in range(IMG):
        rows = arrived_ref[0, image].astype(F32)
        for peer in range(1, 4):
            rows = rows + arrived_ref[peer, image].astype(F32)
        line = first_row + lax.broadcasted_iota(jnp.int32, rows.shape, 0)
        rows = jnp.where(line < counts_ref[image], rows, 0.0).astype(BF)
        for half in range(2):
            for group in range(10):
                out_ref[half * 10 + group, image] = rows[
                    half * 8 : half * 8 + 8, group * LANE : (group + 1) * LANE
                ]
    out_ref[20:32] = jnp.zeros((12, IMG, 8, LANE), BF)


def spread(place, counts, arrived):
    return pl.pallas_call(
        spread_kernel,
        out_shape=jax.ShapeDtypeStruct((PEERS, IMG, 8, LANE), BF),
        in_specs=[smem(), smem(), pl.BlockSpec(memory_space=pltpu.VMEM)],
        out_specs=pl.BlockSpec(memory_space=pltpu.VMEM),
        name="spread",
    )(place, counts, arrived)


def forward_kernel(index_ref, pieces_ref, out_ref):
    def step(at, carry):
        out_ref[at] = pieces_ref[index_ref[at]]
        return carry

    lax.fori_loop(0, PEERS * IMG, step, 0, unroll=8)


def forwarded(index, pieces):
    flat = pieces.reshape(PEERS * IMG, 8, LANE)
    return pl.pallas_call(
        forward_kernel,
        out_shape=jax.ShapeDtypeStruct(flat.shape, BF),
        in_specs=[smem(), pl.BlockSpec(memory_space=pltpu.VMEM)],
        out_specs=pl.BlockSpec(memory_space=pltpu.VMEM),
        name="forwarded",
    )(index, flat).reshape(pieces.shape)


def collect_kernel(pieces_ref, rows_ref, copies_ref):
    for image in range(IMG):
        for half in range(2):
            for group in range(10):
                piece = pieces_ref[half * 10 + group, image]
                at = (slice(half * 8, half * 8 + 8), slice(group * LANE, (group + 1) * LANE))
                rows_ref[image, at[0], at[1]] = piece
                for peer in range(4):
                    copies_ref[peer, image, at[0], at[1]] = piece


def collected(pieces):
    return pl.pallas_call(
        collect_kernel,
        out_shape=(
            jax.ShapeDtypeStruct((IMG, 16, WIDTH), BF),
            jax.ShapeDtypeStruct((4, IMG, 16, WIDTH), BF),
        ),
        in_specs=[pl.BlockSpec(memory_space=pltpu.VMEM)],
        out_specs=(pl.BlockSpec(memory_space=pltpu.VMEM),) * 2,
        name="collected",
    )(pieces)


def attention_kernel(
    counts_ref, block_ref, gain_ref, w_ref, normed_ref, packed_ref, prob_ref, mixed_ref
):
    normed, _ = normalize(block_ref[...].astype(F32))
    normed_in = (normed * gain_ref[...]).astype(BF)
    normed_ref[...] = normed_in
    packed = dot(normed_in, w_ref[...], 1, 0).astype(BF)
    packed_ref[...] = packed
    count = counts_ref[pl.program_id(0)]
    live_row = lax.broadcasted_iota(jnp.int32, (TILE, TILE), 0) < count
    live_col = lax.broadcasted_iota(jnp.int32, (TILE, TILE), 1) < count
    same_kind = (live_row & live_col) | (~live_row & ~live_col)
    mixed = []
    for head in range(2):
        query, key, value = (
            packed[:, (head * 3 + i) * LANE : (head * 3 + i + 1) * LANE] for i in range(3)
        )
        scores = jnp.where(same_kind, dot(query, key, 1, 1) * SCALING, -1e30)
        exp_terms = jnp.exp(scores - jnp.max(scores, axis=-1, keepdims=True))
        probability = exp_terms / jnp.sum(exp_terms, axis=-1, keepdims=True)
        prob_ref[0, head] = probability
        mixed.append(dot(probability.astype(BF), value, 1, 0))
    mixed_ref[...] = shifted_sum(mixed, 256)[:, :160].astype(BF)


def attention(counts, block, gain, w_pad):
    return pl.pallas_call(
        attention_kernel,
        grid=(IMG,),
        out_shape=(
            jax.ShapeDtypeStruct((ROWS, WIDTH), BF),
            jax.ShapeDtypeStruct((ROWS, 6 * LANE), BF),
            jax.ShapeDtypeStruct((IMG, 2, TILE, TILE), F32),
            jax.ShapeDtypeStruct((ROWS, 2 * HEAD), BF),
        ),
        in_specs=[
            smem(),
            pl.BlockSpec((TILE, WIDTH), lambda i: (i, 0)),
            pl.BlockSpec((1, WIDTH), lambda i: (0, 0)),
            pl.BlockSpec((WIDTH, 6 * LANE), lambda i: (0, 0)),
        ],
        out_specs=(
            pl.BlockSpec((TILE, WIDTH), lambda i: (i, 0)),
            pl.BlockSpec((TILE, 6 * LANE), lambda i: (i, 0)),
            pl.BlockSpec((1, 2, TILE, TILE), lambda i: (i, 0, 0, 0)),
            pl.BlockSpec((TILE, 2 * HEAD), lambda i: (i, 0)),
        ),
        name="attention",
    )(counts, block, gain, w_pad)


def backward_kernel(
    core_ref,
    own_ref,
    other_ref,
    wout_ref,
    w_ref,
    packed_ref,
    prob_ref,
    upstream_ref,
    packed_grad_ref,
    in_own_ref,
    in_other_ref,
):
    first = core_ref[0] == 0
    own = own_ref[...].reshape(64, WIDTH)
    other = other_ref[...].reshape(64, WIDTH)
    upstream = jnp.concatenate(
        [jnp.where(first, own, other), jnp.where(first, other, own)], axis=0
    )
    upstream_ref[...] = upstream
    mixed_grads = dot(upstream, wout_ref[...], 1, 1).astype(BF)
    pieces = []
    for head in range(2):
        query, key, value = (
            packed_ref[:, (head * 3 + i) * LANE : (head * 3 + i + 1) * LANE] for i in range(3)
        )
        probability = prob_ref[0, head]
        mixed_grad = mixed_grads[:, head * LANE : (head + 1) * LANE]
        prob_grad = dot(mixed_grad, value, 1, 1)
        inner = jnp.sum(probability * prob_grad, axis=-1, keepdims=True)
        score_grad = (probability * (prob_grad - inner) * SCALING).astype(BF)
        pieces.append(dot(score_grad, key, 1, 0))
        pieces.append(dot(score_grad, query, 0, 0))
        pieces.append(dot(probability.astype(BF), mixed_grad, 0, 0))
    packed_grad_ref[...] = shifted_sum(pieces, 512)[:, :480].astype(BF)
    wide = jnp.concatenate([piece.astype(BF) for piece in pieces], axis=1)
    in_part = dot(wide, w_ref[...], 1, 1).astype(BF)
    low, high = in_part[:64], in_part[64:]
    in_own_ref[...] = jnp.where(first, low, high).reshape(4, 1, 16, WIDTH)
    in_other_ref[...] = jnp.where(first, high, low).reshape(4, 1, 16, WIDTH)


def backward(core, own, other, wout_pad, w_pad, packed, prob):
    quarter = pl.BlockSpec((4, 1, 16, WIDTH), lambda i: (0, i, 0, 0))
    return pl.pallas_call(
        backward_kernel,
        grid=(IMG,),
        out_shape=(
            jax.ShapeDtypeStruct((ROWS, WIDTH), BF),
            jax.ShapeDtypeStruct((ROWS, 6 * HEAD), BF),
            jax.ShapeDtypeStruct((4, IMG, 16, WIDTH), BF),
            jax.ShapeDtypeStruct((4, IMG, 16, WIDTH), BF),
        ),
        in_specs=[
            smem(),
            quarter,
            quarter,
            pl.BlockSpec((2 * LANE, WIDTH), lambda i: (0, 0)),
            pl.BlockSpec((WIDTH, 6 * LANE), lambda i: (0, 0)),
            pl.BlockSpec((TILE, 6 * LANE), lambda i: (i, 0)),
            pl.BlockSpec((1, 2, TILE, TILE), lambda i: (i, 0, 0, 0)),
        ],
        out_specs=(
            pl.BlockSpec((TILE, WIDTH), lambda i: (i, 0)),
            pl.BlockSpec((TILE, 6 * HEAD), lambda i: (i, 0)),
            quarter,
            quarter,
        ),
        name="backward",
    )(core, own, other, wout_pad, w_pad, packed, prob)


def weights_kernel(normed_ref, upstream_ref, packed_grad_ref, mixed_ref, out_ref):
    qkv = dot(normed_ref[...], packed_grad_ref[...], 0, 0)
    out = dot(upstream_ref[...], mixed_ref[...], 0, 0)
    term = jnp.concatenate([qkv, out], axis=1).astype(BF)
    for far in range(4):
        for near in range(4):
            at = (far * 4 + near) * 40
            out_ref[near, far] = term[at : at + 40]


def weight_terms(normed, upstream, packed_grad, mixed):
    return pl.pallas_call(
        weights_kernel,
        grid=(2,),
        out_shape=jax.ShapeDtypeStruct((4, 8, 40, 640), BF),
        in_specs=[
            pl.BlockSpec((ROWS, 640), lambda i: (0, i)),
            pl.BlockSpec((ROWS, 640), lambda i: (0, i)),
            pl.BlockSpec((ROWS, 6 * HEAD), lambda i: (0, 0)),
            pl.BlockSpec((ROWS, 2 * HEAD), lambda i: (0, 0)),
        ],
        out_specs=pl.BlockSpec((4, 4, 40, 640), lambda i: (0, i, 0, 0)),
        name="weight_terms",
    )(normed, upstream, packed_grad, mixed)


def norm_back_kernel(arrived_ref, block_ref, upstream_ref, gain_ref, out_ref):
    gain = gain_ref[...]
    gain_term = None
    results = []
    for image in range(IMG):
        incoming = arrived_ref[0, image].astype(F32)
        for peer in range(1, 4):
            incoming = incoming + arrived_ref[peer, image].astype(F32)
        normed, inverse = normalize(block_ref[image].astype(F32))
        term = jnp.sum(incoming * normed, axis=0, keepdims=True)
        gain_term = term if gain_term is None else gain_term + term
        scaled = incoming * gain
        inner = jnp.mean(scaled * normed, axis=-1, keepdims=True)
        outgoing = inverse * (scaled - jnp.mean(scaled, axis=-1, keepdims=True) - normed * inner)
        results.append(upstream_ref[image].astype(F32) + outgoing)
    grads = jnp.concatenate(results, axis=0)
    spread_term = jnp.broadcast_to(gain_term, (8, WIDTH))
    row = lax.broadcasted_iota(jnp.int32, (8, 160), 0)
    terms = jnp.zeros((8, 160), F32)
    for share in range(8):
        start = share * 160 // LANE * LANE
        offset = share * 160 - start
        lanes = 256 if offset + 160 <= 256 else 384
        lanes = min(lanes, WIDTH - start)

        def part(values):
            window = values[:, start : start + lanes]
            if offset:
                window = pltpu.roll(window, lanes - offset, 1)
            return window[:, :160]

        out_ref[share, 0:80] = part(grads).astype(BF)
        terms = jnp.where(row == share, part(spread_term), terms)
    for share in range(8):
        out_ref[share, 80:88] = terms.astype(BF)


def norm_back(arrived, block_rows, upstream_rows, gain):
    return pl.pallas_call(
        norm_back_kernel,
        out_shape=jax.ShapeDtypeStruct((8, 88, 160), BF),
        in_specs=[pl.BlockSpec(memory_space=pltpu.VMEM)] * 4,
        out_specs=pl.BlockSpec(memory_space=pltpu.VMEM),
        name="norm_back",
    )(arrived, block_rows, upstream_rows, gain)


def summed(blocks):
    return blocks.astype(F32).sum(axis=0)


def shards(grad_rows, features, block_in, patch_counts, owner, ln1_gain, w_qkv, w_out, w_proj):
    device = lax.axis_index(ENC)
    core = lax.axis_index("c")
    place = core * 4 + lax.axis_index("y")
    core_word = core.reshape(1).astype(jnp.int32)
    place_word = place.reshape(1).astype(jnp.int32)
    gain = ln1_gain.reshape(1, WIDTH)

    own_counts = lax.dynamic_index_in_dim(patch_counts, device, 0, keepdims=False)
    images = jnp.arange(PEERS * IMG, dtype=jnp.int32)
    block_of = images // IMG
    owners = owner.reshape(-1)
    ahead = (owners[:, None] == owners[None, :]) & (block_of[None, :] < block_of[:, None])
    target = owners * IMG + jnp.sum(ahead.astype(jnp.int32), axis=1)
    hits = target[None, :] == images[:, None]
    source_of = jnp.sum(jnp.where(hits, images[None, :], 0), axis=1)
    all_counts = jnp.sum(jnp.where(hits, patch_counts.reshape(1, -1), 0), axis=1)
    arrived_counts = lax.dynamic_slice_in_dim(all_counts, device * IMG, IMG, 0)

    by_place = grad_rows.reshape(IMG, 2, 4, 16, -1).transpose(1, 2, 0, 3, 4)
    by_place = by_place.reshape(2, ROWS // 2, -1)
    for_other = lax.dynamic_index_in_dim(by_place, 1 - core, 0, keepdims=False)
    for_own = lax.dynamic_index_in_dim(by_place, core, 0, keepdims=False)
    part_other = dot(for_other, w_proj, 1, 1).astype(BF)
    from_other = lax.ppermute(part_other, "c", SWAP)
    part_own = dot(for_own, w_proj, 1, 1)
    pair = (part_own + from_other.astype(F32)).astype(BF)
    arrived = exchanged(pair.reshape(4, 80, WIDTH), "y").reshape(4, IMG, 16, WIDTH)
    pieces = spread(place_word, own_counts, arrived)

    passing = exchanged(pieces, ENC)
    passing = forwarded(source_of, passing)
    landed = exchanged(passing, ENC)
    upstream_rows, copies = collected(landed)
    half_own = exchanged(copies.reshape(4, 80, WIDTH), "y").reshape(4, IMG, 16, WIDTH)
    half_other = lax.ppermute(half_own, "c", SWAP)

    line = jnp.arange(TILE, dtype=jnp.int32)
    live_own = (line[None, :] < own_counts[:, None]).reshape(-1)
    kept_rows = jnp.where(live_own[:, None], features, jnp.zeros_like(features))
    proj_term = dot(kept_rows, grad_rows, 0, 0).astype(BF)
    columns = grad_rows.shape[1]
    proj_term = proj_term.reshape(8, 4, 40, columns).transpose(1, 0, 2, 3)
    proj_near = summed(exchanged(proj_term.reshape(4, 320, columns), "x")).astype(BF)
    grad_proj = summed(exchanged(proj_near.reshape(8, 40, columns), "z"))

    lines = block_in.reshape(ROWS * 160 // LANE, LANE)
    lines, pieces = lax.optimization_barrier((lines, pieces))
    lines_own = exchanged(jnp.broadcast_to(lines, (4, *lines.shape)), "y")
    lines_other = lax.ppermute(lines_own, "c", SWAP)
    first = core == 0
    both = jnp.stack(
        [jnp.where(first, lines_own, lines_other), jnp.where(first, lines_other, lines_own)], 1
    )
    block_full = both.reshape(8, ROWS, 160).transpose(1, 0, 2).reshape(ROWS, WIDTH)
    block_rows = lax.dynamic_index_in_dim(
        block_full.reshape(IMG, 8, 16, WIDTH), place, 1, keepdims=False
    )

    w_pad = jnp.pad(w_qkv.reshape(WIDTH, 6, HEAD), ((0, 0), (0, 0), (0, LANE - HEAD)))
    w_pad = w_pad.reshape(WIDTH, 6 * LANE)
    wout_pad = jnp.pad(w_out.reshape(2, HEAD, WIDTH), ((0, 0), (0, LANE - HEAD), (0, 0)))
    wout_pad = wout_pad.reshape(2 * LANE, WIDTH)
    normed_in, packed, prob, mixed = attention(arrived_counts, block_full, gain, w_pad)

    upstream, packed_grad, in_own, in_other = backward(
        core_word, half_own, half_other, wout_pad, w_pad, packed, prob
    )
    in_got = lax.ppermute(in_other, "c", SWAP)
    terms = weight_terms(normed_in, upstream, packed_grad, mixed)
    in_pair = (in_own.astype(F32) + in_got.astype(F32)).astype(BF)
    in_arrived = exchanged(in_pair.reshape(4, 80, WIDTH), "y").reshape(4, IMG, 16, WIDTH)
    term_near = summed(exchanged(terms.reshape(4, 320, 640), "x")).astype(BF)
    shares = exchanged(norm_back(in_arrived, block_rows, upstream_rows, gain), TP)
    grad_input = shares[:, :80].reshape(4, 2, IMG, 16, 160).transpose(2, 1, 0, 3, 4)
    grad_input = grad_input.reshape(ROWS, 160)
    ln1_block = summed(shares[:, 80:]).astype(BF)
    grad_ln1 = summed(exchanged(ln1_block.reshape(PEERS, 1, 40), ENC)).reshape(40)
    term_sum = summed(exchanged(term_near.reshape(8, 40, 640), "z"))
    grad_qkv = term_sum[:, :480].reshape(40, 2, 240)
    grad_out = term_sum[:, 480:].T
    return (grad_input, grad_proj, grad_qkv, grad_out, grad_ln1)


def solution(mesh):
    torus = Mesh(mesh.devices.reshape(8, 4, 4, 2), ("z", "x", "y", "c"))
    return jax.shard_map(
        shards,
        mesh=torus,
        in_specs=(
            P(ENC, TP),
            P(ENC, None),
            P(ENC, TP),
            P(),
            P(),
            P(),
            P(None, TP, None),
            P(TP, None),
            P(None, TP),
        ),
        out_specs=(P(ENC, TP), P(ENC, TP), P(ENC, TP, None), P(TP, ENC), P(ENC)),
        check_vma=False,
    )
```

```python
import jax
import jax.numpy as jnp
from jax import lax
from jax.experimental import pallas as pl
from jax.experimental.pallas import tpu as pltpu
from jax.sharding import Mesh
from jax.sharding import PartitionSpec as P

TILE = 128
IMG = 5
ROWS = IMG * TILE
WIDTH = 1280
HEAD = 80
LANE = 128
PEERS = 32
ENC = ("z", "x")
TP = ("y", "c")
EPSILON = 1e-05
SCALING = 1.0 / HEAD**0.5
BF = jnp.bfloat16
F32 = jnp.float32
SWAP = ((0, 1), (1, 0))


def exchanged(blocks, axis):
    return lax.all_to_all(blocks, axis, split_axis=0, concat_axis=0, tiled=True)


def dot(left, right, dim_left, dim_right):
    return lax.dot_general(
        left, right, (((dim_left,), (dim_right,)), ((), ())), preferred_element_type=F32
    )


def smem():
    return pl.BlockSpec(memory_space=pltpu.SMEM)


def normalize(values):
    centred = values - jnp.mean(values, axis=-1, keepdims=True)
    variance = jnp.mean(centred * centred, axis=-1, keepdims=True)
    inverse = lax.rsqrt(variance + EPSILON)
    return (centred * inverse, inverse)


def shifted_sum(pieces, lanes):
    total = None
    for at, piece in enumerate(pieces):
        wide = jnp.concatenate(
            [piece, jnp.zeros((piece.shape[0], lanes - LANE), piece.dtype)], axis=1
        )
        if at:
            wide = pltpu.roll(wide, HEAD * at, 1)
        total = wide if total is None else total + wide
    return total


def spread_kernel(place_ref, counts_ref, arrived_ref, out_ref):
    first_row = place_ref[0] * 16
    for image in range(IMG):
        rows = arrived_ref[0, image].astype(F32)
        for peer in range(1, 4):
            rows = rows + arrived_ref[peer, image].astype(F32)
        line = first_row + lax.broadcasted_iota(jnp.int32, rows.shape, 0)
        rows = jnp.where(line < counts_ref[image], rows, 0.0).astype(BF)
        for half in range(2):
            for group in range(10):
                out_ref[half * 10 + group, image] = rows[
                    half * 8 : half * 8 + 8, group * LANE : (group + 1) * LANE
                ]
    out_ref[20:32] = jnp.zeros((12, IMG, 8, LANE), BF)


def spread(place, counts, arrived):
    return pl.pallas_call(
        spread_kernel,
        out_shape=jax.ShapeDtypeStruct((PEERS, IMG, 8, LANE), BF),
        in_specs=[smem(), smem(), pl.BlockSpec(memory_space=pltpu.VMEM)],
        out_specs=pl.BlockSpec(memory_space=pltpu.VMEM),
        name="spread",
    )(place, counts, arrived)


def forward_kernel(index_ref, pieces_ref, out_ref):
    def step(at, carry):
        out_ref[at] = pieces_ref[index_ref[at]]
        return carry

    lax.fori_loop(0, PEERS * IMG, step, 0, unroll=8)


def forwarded(index, pieces):
    flat = pieces.reshape(PEERS * IMG, 8, LANE)
    return pl.pallas_call(
        forward_kernel,
        out_shape=jax.ShapeDtypeStruct(flat.shape, BF),
        in_specs=[smem(), pl.BlockSpec(memory_space=pltpu.VMEM)],
        out_specs=pl.BlockSpec(memory_space=pltpu.VMEM),
        name="forwarded",
    )(index, flat).reshape(pieces.shape)


def collect_kernel(pieces_ref, rows_ref, copies_ref):
    for image in range(IMG):
        for half in range(2):
            for group in range(10):
                piece = pieces_ref[half * 10 + group, image]
                at = (slice(half * 8, half * 8 + 8), slice(group * LANE, (group + 1) * LANE))
                rows_ref[image, at[0], at[1]] = piece
                for peer in range(4):
                    copies_ref[peer, image, at[0], at[1]] = piece


def collected(pieces):
    return pl.pallas_call(
        collect_kernel,
        out_shape=(
            jax.ShapeDtypeStruct((IMG, 16, WIDTH), BF),
            jax.ShapeDtypeStruct((4, IMG, 16, WIDTH), BF),
        ),
        in_specs=[pl.BlockSpec(memory_space=pltpu.VMEM)],
        out_specs=(pl.BlockSpec(memory_space=pltpu.VMEM),) * 2,
        name="collected",
    )(pieces)


def attention_kernel(
    words_ref,
    counts_ref,
    own_ref,
    other_ref,
    gain_ref,
    w_ref,
    normed_in_ref,
    normed_ref,
    rows_ref,
    packed_ref,
    prob_ref,
    mixed_ref,
    scratch,
):
    first = words_ref[0] == 0
    shares = []
    for near in range(4):
        own, other = own_ref[near], other_ref[near]
        shares += [jnp.where(first, own, other), jnp.where(first, other, own)]
    values = jnp.concatenate(shares, axis=0).astype(F32).T
    scratch[...] = values
    rows_ref[0] = scratch[pl.ds(pl.multiple_of(words_ref[1] * 16, 16), 16), :].astype(BF)
    normed, _ = normalize(values)
    normed_ref[...] = normed.astype(BF)
    normed_in = (normed * gain_ref[...]).astype(BF)
    normed_in_ref[...] = normed_in
    packed = dot(normed_in, w_ref[...], 1, 1).astype(BF)
    packed_ref[...] = packed
    count = counts_ref[pl.program_id(0)]
    live_row = lax.broadcasted_iota(jnp.int32, (TILE, TILE), 0) < count
    live_col = lax.broadcasted_iota(jnp.int32, (TILE, TILE), 1) < count
    same_kind = (live_row & live_col) | (~live_row & ~live_col)
    mixed = []
    for head in range(2):
        query, key, value = (
            packed[:, (head * 3 + i) * LANE : (head * 3 + i + 1) * LANE] for i in range(3)
        )
        scores = jnp.where(same_kind, dot(query, key, 1, 1) * SCALING, -1e30)
        exp_terms = jnp.exp(scores - jnp.max(scores, axis=-1, keepdims=True))
        probability = exp_terms / jnp.sum(exp_terms, axis=-1, keepdims=True)
        prob_ref[0, head] = probability
        mixed.append(dot(probability.astype(BF), value, 1, 0))
    mixed_ref[...] = shifted_sum(mixed, 256)[:, :160].astype(BF)


def attention(words, counts, own, other, gain, w_pad):
    share = pl.BlockSpec((4, 160, TILE), lambda i: (0, 0, i))
    rows = pl.BlockSpec((TILE, WIDTH), lambda i: (i, 0))
    return pl.pallas_call(
        attention_kernel,
        grid=(IMG,),
        out_shape=(
            jax.ShapeDtypeStruct((ROWS, WIDTH), BF),
            jax.ShapeDtypeStruct((ROWS, WIDTH), BF),
            jax.ShapeDtypeStruct((IMG, 16, WIDTH), BF),
            jax.ShapeDtypeStruct((ROWS, 6 * LANE), BF),
            jax.ShapeDtypeStruct((IMG, 2, TILE, TILE), F32),
            jax.ShapeDtypeStruct((ROWS, 2 * HEAD), BF),
        ),
        in_specs=[
            smem(),
            smem(),
            share,
            share,
            pl.BlockSpec((1, WIDTH), lambda i: (0, 0)),
            pl.BlockSpec((6 * LANE, WIDTH), lambda i: (0, 0)),
        ],
        out_specs=(
            rows,
            rows,
            pl.BlockSpec((1, 16, WIDTH), lambda i: (i, 0, 0)),
            pl.BlockSpec((TILE, 6 * LANE), lambda i: (i, 0)),
            pl.BlockSpec((1, 2, TILE, TILE), lambda i: (i, 0, 0, 0)),
            pl.BlockSpec((TILE, 2 * HEAD), lambda i: (i, 0)),
        ),
        scratch_shapes=[pltpu.VMEM((TILE, WIDTH), F32)],
        cost_estimate=pl.CostEstimate(
            flops=10_000_000_000, bytes_accessed=10_000_000, transcendentals=0
        ),
        name="attention",
    )(words, counts, own, other, gain, w_pad)


def backward_kernel(
    words_ref,
    own_ref,
    other_ref,
    wout_ref,
    w_ref,
    packed_ref,
    prob_ref,
    normed_ref,
    upstream_ref,
    packed_grad_ref,
    in_own_ref,
    in_other_ref,
    gain_term,
):
    step = pl.program_id(0)

    @pl.when(step == 0)
    def _():
        gain_term[...] = jnp.zeros_like(gain_term)

    @pl.when(step < IMG)
    def _():
        first = words_ref[0] == 0
        own = own_ref[...].reshape(64, WIDTH)
        other = other_ref[...].reshape(64, WIDTH)
        upstream = jnp.concatenate(
            [jnp.where(first, own, other), jnp.where(first, other, own)], axis=0
        )
        upstream_ref[...] = upstream
        mixed_grads = dot(upstream, wout_ref[...], 1, 1).astype(BF)
        pieces = []
        for head in range(2):
            query, key, value = (
                packed_ref[:, (head * 3 + i) * LANE : (head * 3 + i + 1) * LANE]
                for i in range(3)
            )
            probability = prob_ref[0, head]
            mixed_grad = mixed_grads[:, head * LANE : (head + 1) * LANE]
            prob_grad = dot(mixed_grad, value, 1, 1)
            inner = jnp.sum(probability * prob_grad, axis=-1, keepdims=True)
            score_grad = (probability * (prob_grad - inner) * SCALING).astype(BF)
            pieces.append(dot(score_grad, key, 1, 0))
            pieces.append(dot(score_grad, query, 0, 0))
            pieces.append(dot(probability.astype(BF), mixed_grad, 0, 0))
        packed_grad_ref[...] = shifted_sum(pieces, 512)[:, :480].astype(BF)
        wide = jnp.concatenate([piece.astype(BF) for piece in pieces], axis=1)
        in_part = dot(wide, w_ref[...], 1, 0).astype(BF)
        gain_term[...] += jnp.sum(
            in_part.astype(F32) * normed_ref[...].astype(F32), axis=0, keepdims=True
        )
        low, high = in_part[:64], in_part[64:]
        in_own_ref[...] = jnp.where(first, low, high).reshape(4, 1, 16, WIDTH)
        in_other_ref[...] = jnp.where(first, high, low).reshape(4, 1, 16, WIDTH)

    @pl.when(step == IMG)
    def _():
        row = lax.broadcasted_iota(jnp.int32, (16, WIDTH), 0)
        plane = jnp.where(row == 0, gain_term[...], 0.0).astype(BF)
        for peer in range(4):
            in_own_ref[peer, 0] = plane
            in_other_ref[peer, 0] = plane


def backward(words, own, other, wout_pad, w_pad, packed, prob, normed):
    def image(i):
        return jnp.minimum(i, IMG - 1)

    quarter = pl.BlockSpec((4, 1, 16, WIDTH), lambda i: (0, image(i), 0, 0))
    plane = pl.BlockSpec((4, 1, 16, WIDTH), lambda i: (0, i, 0, 0))
    rows = pl.BlockSpec((TILE, WIDTH), lambda i: (image(i), 0))
    return pl.pallas_call(
        backward_kernel,
        grid=(IMG + 1,),
        out_shape=(
            jax.ShapeDtypeStruct((ROWS, WIDTH), BF),
            jax.ShapeDtypeStruct((ROWS, 6 * HEAD), BF),
            jax.ShapeDtypeStruct((4, IMG + 1, 16, WIDTH), BF),
            jax.ShapeDtypeStruct((4, IMG + 1, 16, WIDTH), BF),
        ),
        in_specs=[
            smem(),
            quarter,
            quarter,
            pl.BlockSpec((2 * LANE, WIDTH), lambda i: (0, 0)),
            pl.BlockSpec((6 * LANE, WIDTH), lambda i: (0, 0)),
            pl.BlockSpec((TILE, 6 * LANE), lambda i: (image(i), 0)),
            pl.BlockSpec((1, 2, TILE, TILE), lambda i: (image(i), 0, 0, 0)),
            rows,
        ],
        out_specs=(
            rows,
            pl.BlockSpec((TILE, 6 * HEAD), lambda i: (image(i), 0)),
            plane,
            plane,
        ),
        scratch_shapes=[pltpu.VMEM((1, WIDTH), F32)],
        cost_estimate=pl.CostEstimate(
            flops=10_000_000_000, bytes_accessed=10_000_000, transcendentals=0
        ),
        name="backward",
    )(words, own, other, wout_pad, w_pad, packed, prob, normed)


def weights_kernel(normed_ref, upstream_ref, packed_grad_ref, mixed_ref, out_ref):
    qkv = dot(normed_ref[...], packed_grad_ref[...], 0, 0)
    out = dot(upstream_ref[...], mixed_ref[...], 0, 0)
    out_ref[...] = jnp.concatenate([qkv, out], axis=1).astype(BF)


def weight_terms(normed, upstream, packed_grad, mixed):
    return pl.pallas_call(
        weights_kernel,
        grid=(2,),
        out_shape=jax.ShapeDtypeStruct((WIDTH, 640), BF),
        in_specs=[
            pl.BlockSpec((ROWS, 640), lambda i: (0, i)),
            pl.BlockSpec((ROWS, 640), lambda i: (0, i)),
            pl.BlockSpec((ROWS, 6 * HEAD), lambda i: (0, 0)),
            pl.BlockSpec((ROWS, 2 * HEAD), lambda i: (0, 0)),
        ],
        out_specs=pl.BlockSpec((640, 640), lambda i: (i, 0)),
        cost_estimate=pl.CostEstimate(
            flops=4_000_000_000, bytes_accessed=6_000_000, transcendentals=0
        ),
        name="weight_terms",
    )(normed, upstream, packed_grad, mixed)


def norm_back_kernel(arrived_ref, block_ref, upstream_ref, gain_ref, out_ref, term_ref):
    gain = gain_ref[...]
    results = []
    for image in range(IMG + 1):
        incoming = arrived_ref[0, image].astype(F32)
        for peer in range(1, 4):
            incoming = incoming + arrived_ref[peer, image].astype(F32)
        if image == IMG:
            term_ref[...] = incoming[:8]
            continue
        normed, inverse = normalize(block_ref[image].astype(F32))
        scaled = incoming * gain
        inner = jnp.mean(scaled * normed, axis=-1, keepdims=True)
        outgoing = inverse * (scaled - jnp.mean(scaled, axis=-1, keepdims=True) - normed * inner)
        results.append(upstream_ref[image].astype(F32) + outgoing)
    grads = jnp.concatenate(results, axis=0)
    for share in range(8):
        start = share * 160 // LANE * LANE
        offset = share * 160 - start
        lanes = min(256 if offset + 160 <= 256 else 384, WIDTH - start)
        window = grads[:, start : start + lanes]
        if offset:
            window = pltpu.roll(window, lanes - offset, 1)
        out_ref[share] = window[:, :160].astype(BF)


def norm_back(arrived, block_rows, upstream_rows, gain):
    return pl.pallas_call(
        norm_back_kernel,
        out_shape=(
            jax.ShapeDtypeStruct((8, 80, 160), BF),
            jax.ShapeDtypeStruct((8, WIDTH), F32),
        ),
        in_specs=[pl.BlockSpec(memory_space=pltpu.VMEM)] * 4,
        out_specs=(pl.BlockSpec(memory_space=pltpu.VMEM),) * 2,
        name="norm_back",
    )(arrived, block_rows, upstream_rows, gain)


def summed(blocks):
    return blocks.astype(F32).sum(axis=0)


def near_sum(term, columns):
    blocks = term.reshape(8, 4, -1, columns)
    here = lax.axis_index("x")

    def rows_of(at):
        return lax.dynamic_index_in_dim(blocks, lax.rem(here + at, 4), 1, keepdims=False)

    got = [
        lax.ppermute(rows_of(at), "x", tuple((i, (i + at) % 4) for i in range(4)))
        for at in (2, 1, 3)
    ]
    total = rows_of(0).astype(F32)
    for rows in got:
        total = total + rows.astype(F32)
    return total.astype(BF)


def shards(grad_rows, features, block_in, patch_counts, owner, ln1_gain, w_qkv, w_out, w_proj):
    device = lax.axis_index(ENC)
    core = lax.axis_index("c")
    place = core * 4 + lax.axis_index("y")
    words = jnp.stack([core, place]).astype(jnp.int32)
    place_word = place.reshape(1).astype(jnp.int32)
    gain = ln1_gain.reshape(1, WIDTH)
    columns = grad_rows.shape[1]

    own_counts = lax.dynamic_index_in_dim(patch_counts, device, 0, keepdims=False)
    images = jnp.arange(PEERS * IMG, dtype=jnp.int32)
    block_of = images // IMG
    owners = owner.reshape(-1)
    ahead = (owners[:, None] == owners[None, :]) & (block_of[None, :] < block_of[:, None])
    target = owners * IMG + jnp.sum(ahead.astype(jnp.int32), axis=1)
    hits = target[None, :] == images[:, None]
    source_of = jnp.sum(jnp.where(hits, images[None, :], 0), axis=1)
    all_counts = jnp.sum(jnp.where(hits, patch_counts.reshape(1, -1), 0), axis=1)
    arrived_counts = lax.dynamic_slice_in_dim(all_counts, device * IMG, IMG, 0)

    share = jnp.broadcast_to(block_in.T, (4, 160, ROWS))
    block_own = exchanged(share, "y")
    block_other = lax.ppermute(block_own, "c", SWAP)

    by_place = grad_rows.reshape(IMG, 2, 4, 16, -1).transpose(1, 2, 0, 3, 4)
    by_place = by_place.reshape(2, ROWS // 2, -1)
    for_other = lax.dynamic_index_in_dim(by_place, 1 - core, 0, keepdims=False)
    for_own = lax.dynamic_index_in_dim(by_place, core, 0, keepdims=False)
    part_other = dot(for_other, w_proj, 1, 1).astype(BF)
    from_other = lax.ppermute(part_other, "c", SWAP)
    part_own = dot(for_own, w_proj, 1, 1)
    pair = (part_own + from_other.astype(F32)).astype(BF)
    pair, block_own, features = lax.optimization_barrier((pair, block_own, features))
    arrived = exchanged(pair.reshape(4, 80, WIDTH), "y").reshape(4, IMG, 16, WIDTH)
    pieces = spread(place_word, own_counts, arrived)

    line = jnp.arange(TILE, dtype=jnp.int32)
    live_own = (line[None, :] < own_counts[:, None]).reshape(-1)
    kept_rows = jnp.where(live_own[:, None], features, jnp.zeros_like(features))
    proj_term = dot(kept_rows, grad_rows, 0, 0).astype(BF)
    proj_near = near_sum(proj_term, columns)

    w_pad = jnp.pad(w_qkv.transpose(1, 2, 0).reshape(6, HEAD, WIDTH), ((0, 0), (0, 48), (0, 0)))
    w_pad = w_pad.reshape(6 * LANE, WIDTH)
    wout_pad = jnp.pad(w_out.reshape(2, HEAD, WIDTH), ((0, 0), (0, 48), (0, 0)))
    wout_pad = wout_pad.reshape(2 * LANE, WIDTH)
    normed_in, normed, block_rows, packed, prob, mixed = attention(
        words, arrived_counts, block_own, block_other, gain, w_pad
    )

    passing = exchanged(pieces, ENC)
    passing = forwarded(source_of, passing)
    passing, prob = lax.optimization_barrier((passing, prob))
    landed = exchanged(passing, ENC)
    upstream_rows, copies = collected(landed)
    half_own = exchanged(copies.reshape(4, 80, WIDTH), "y").reshape(4, IMG, 16, WIDTH)
    half_other = lax.ppermute(half_own, "c", SWAP)

    proj_near, half_own = lax.optimization_barrier((proj_near, half_own))
    grad_proj = summed(exchanged(proj_near, "z"))

    upstream, packed_grad, in_own, in_other = backward(
        words, half_own, half_other, wout_pad, w_pad, packed, prob, normed
    )
    in_got = lax.ppermute(in_other, "c", SWAP)
    terms = weight_terms(normed_in, upstream, packed_grad, mixed)
    in_pair = (in_own.astype(F32) + in_got.astype(F32)).astype(BF)
    in_arrived = exchanged(in_pair.reshape(4, 96, WIDTH), "y").reshape(4, IMG + 1, 16, WIDTH)
    term_near = near_sum(terms, 640)
    shares, gain_term = norm_back(in_arrived, block_rows, upstream_rows, gain)
    shares = exchanged(shares, TP)
    grad_input = shares.reshape(4, 2, IMG, 16, 160).transpose(2, 1, 0, 3, 4)
    grad_input = grad_input.reshape(ROWS, 160)
    gain_near = near_sum(gain_term[0].astype(BF).reshape(PEERS * 40, 1), 1)
    last = jnp.concatenate([term_near, jnp.pad(gain_near, ((0, 0), (0, 0), (0, 127)))], axis=2)
    last = summed(exchanged(last, "z"))
    grad_qkv = last[:, :480].reshape(40, 2, 240)
    grad_out = last[:, 480:640].T
    grad_ln1 = last[:, 640]
    return (grad_input, grad_proj, grad_qkv, grad_out, grad_ln1)


def solution(mesh):
    torus = Mesh(mesh.devices.reshape(8, 4, 4, 2), ("z", "x", "y", "c"))
    return jax.shard_map(
        shards,
        mesh=torus,
        in_specs=(
            P(ENC, TP),
            P(ENC, None),
            P(ENC, TP),
            P(),
            P(),
            P(),
            P(None, TP, None),
            P(TP, None),
            P(None, TP),
        ),
        out_specs=(P(ENC, TP), P(ENC, TP), P(ENC, TP, None), P(TP, ENC), P(ENC)),
        check_vma=False,
    )
```

```python
import jax
import jax.numpy as jnp
from jax import lax
from jax.experimental import pallas as pl
from jax.experimental.pallas import tpu as pltpu
from jax.sharding import Mesh
from jax.sharding import PartitionSpec as P


TILE = 128
IMG = 5
ROWS = IMG * TILE
WIDTH = 1280
HEAD = 80
LANE = 128
PEERS = 32
ENC = ("z", "x")
TP = ("y", "c")
EPSILON = 1e-05
SCALING = 1.0 / HEAD**0.5
BF = jnp.bfloat16
F32 = jnp.float32
SWAP = ((0, 1), (1, 0))


def exchanged(blocks, axis):
    return lax.all_to_all(blocks, axis, split_axis=0, concat_axis=0, tiled=True)


def shifted(values, axis, by):
    pairs = tuple((i, (i + by) % 4) for i in range(4))
    return lax.ppermute(values, axis, pairs)


def swapped(values):
    return lax.ppermute(values, "c", SWAP)


def dot(left, right, dim_left, dim_right):
    return lax.dot_general(
        left, right, (((dim_left,), (dim_right,)), ((), ())), preferred_element_type=F32
    )


def smem():
    return pl.BlockSpec(memory_space=pltpu.SMEM)


def normalize(values):
    centred = values - jnp.mean(values, axis=-1, keepdims=True)
    variance = jnp.mean(centred * centred, axis=-1, keepdims=True)
    inverse = lax.rsqrt(variance + EPSILON)
    return (centred * inverse, inverse)


def shifted_sum(pieces, lanes):
    total = None
    for at, piece in enumerate(pieces):
        wide = jnp.concatenate(
            [piece, jnp.zeros((piece.shape[0], lanes - LANE), piece.dtype)], axis=1
        )
        if at:
            wide = pltpu.roll(wide, HEAD * at, 1)
        total = wide if total is None else total + wide
    return total


def spread_kernel(place_ref, counts_ref, arrived_ref, out_ref):
    first_row = place_ref[0] * 16
    for image in range(IMG):
        rows = arrived_ref[0, image].astype(F32)
        for peer in range(1, 4):
            rows = rows + arrived_ref[peer, image].astype(F32)
        line = first_row + lax.broadcasted_iota(jnp.int32, rows.shape, 0)
        rows = jnp.where(line < counts_ref[image], rows, 0.0).astype(BF)
        for half in range(2):
            for group in range(10):
                out_ref[half * 10 + group, image] = rows[
                    half * 8 : half * 8 + 8, group * LANE : (group + 1) * LANE
                ]
    out_ref[20:32] = jnp.zeros((12, IMG, 8, LANE), BF)


def spread(place, counts, arrived):
    return pl.pallas_call(
        spread_kernel,
        out_shape=jax.ShapeDtypeStruct((PEERS, IMG, 8, LANE), BF),
        in_specs=[smem(), smem(), pl.BlockSpec(memory_space=pltpu.VMEM)],
        out_specs=pl.BlockSpec(memory_space=pltpu.VMEM),
        name="spread",
    )(place, counts, arrived)


def forward_kernel(index_ref, pieces_ref, out_ref):
    def step(at, carry):
        out_ref[at] = pieces_ref[index_ref[at]]
        return carry

    lax.fori_loop(0, PEERS * IMG, step, 0, unroll=8)


def forwarded(index, pieces):
    flat = pieces.reshape(PEERS * IMG, 8, LANE)
    return pl.pallas_call(
        forward_kernel,
        out_shape=jax.ShapeDtypeStruct(flat.shape, BF),
        in_specs=[smem(), pl.BlockSpec(memory_space=pltpu.VMEM)],
        out_specs=pl.BlockSpec(memory_space=pltpu.VMEM),
        name="forwarded",
    )(index, flat).reshape(pieces.shape)


def collect_kernel(pieces_ref, rows_ref, copies_ref):
    for image in range(IMG):
        for half in range(2):
            for group in range(10):
                piece = pieces_ref[half * 10 + group, image]
                at = (slice(half * 8, half * 8 + 8), slice(group * LANE, (group + 1) * LANE))
                rows_ref[image, at[0], at[1]] = piece
                for peer in range(4):
                    copies_ref[peer, image, at[0], at[1]] = piece


def collected(pieces):
    return pl.pallas_call(
        collect_kernel,
        out_shape=(
            jax.ShapeDtypeStruct((IMG, 16, WIDTH), BF),
            jax.ShapeDtypeStruct((4, IMG, 16, WIDTH), BF),
        ),
        in_specs=[pl.BlockSpec(memory_space=pltpu.VMEM)],
        out_specs=(pl.BlockSpec(memory_space=pltpu.VMEM),) * 2,
        name="collected",
    )(pieces)


def attention_kernel(
    words_ref,
    counts_ref,
    own_ref,
    other_ref,
    gain_ref,
    w_ref,
    normed_in_ref,
    normed_ref,
    rows_ref,
    packed_ref,
    prob_ref,
    mixed_ref,
    scratch,
):
    first = words_ref[0] == 0
    shares = []
    for near in range(4):
        at = lax.rem(words_ref[2] + 4 - near, 4)
        own, other = own_ref[at], other_ref[at]
        shares += [jnp.where(first, own, other), jnp.where(first, other, own)]
    values = jnp.concatenate(shares, axis=0).astype(F32).T
    scratch[...] = values
    rows_ref[0] = scratch[pl.ds(pl.multiple_of(words_ref[1] * 16, 16), 16), :].astype(BF)
    normed, _ = normalize(values)
    normed_ref[...] = normed.astype(BF)
    normed_in = (normed * gain_ref[...]).astype(BF)
    normed_in_ref[...] = normed_in
    packed = dot(normed_in, w_ref[...], 1, 1).astype(BF)
    packed_ref[...] = packed
    count = counts_ref[pl.program_id(0)]
    live_row = lax.broadcasted_iota(jnp.int32, (TILE, TILE), 0) < count
    live_col = lax.broadcasted_iota(jnp.int32, (TILE, TILE), 1) < count
    same_kind = (live_row & live_col) | (~live_row & ~live_col)
    mixed = []
    for head in range(2):
        query, key, value = (
            packed[:, (head * 3 + i) * LANE : (head * 3 + i + 1) * LANE] for i in range(3)
        )
        scores = jnp.where(same_kind, dot(query, key, 1, 1) * SCALING, -1e30)
        exp_terms = jnp.exp(scores - jnp.max(scores, axis=-1, keepdims=True))
        probability = exp_terms / jnp.sum(exp_terms, axis=-1, keepdims=True)
        prob_ref[0, head] = probability
        mixed.append(dot(probability.astype(BF), value, 1, 0))
    mixed_ref[...] = shifted_sum(mixed, 256)[:, :160].astype(BF)


def attention(words, counts, own, other, gain, w_pad):
    share = pl.BlockSpec((4, 160, TILE), lambda i: (0, 0, i))
    rows = pl.BlockSpec((TILE, WIDTH), lambda i: (i, 0))
    return pl.pallas_call(
        attention_kernel,
        grid=(IMG,),
        out_shape=(
            jax.ShapeDtypeStruct((ROWS, WIDTH), BF),
            jax.ShapeDtypeStruct((ROWS, WIDTH), BF),
            jax.ShapeDtypeStruct((IMG, 16, WIDTH), BF),
            jax.ShapeDtypeStruct((ROWS, 6 * LANE), BF),
            jax.ShapeDtypeStruct((IMG, 2, TILE, TILE), F32),
            jax.ShapeDtypeStruct((ROWS, 2 * HEAD), BF),
        ),
        in_specs=[
            smem(),
            smem(),
            share,
            share,
            pl.BlockSpec((1, WIDTH), lambda i: (0, 0)),
            pl.BlockSpec((6 * LANE, WIDTH), lambda i: (0, 0)),
        ],
        out_specs=(
            rows,
            rows,
            pl.BlockSpec((1, 16, WIDTH), lambda i: (i, 0, 0)),
            pl.BlockSpec((TILE, 6 * LANE), lambda i: (i, 0)),
            pl.BlockSpec((1, 2, TILE, TILE), lambda i: (i, 0, 0, 0)),
            pl.BlockSpec((TILE, 2 * HEAD), lambda i: (i, 0)),
        ),
        scratch_shapes=[pltpu.VMEM((TILE, WIDTH), F32)],
        cost_estimate=pl.CostEstimate(
            flops=10_000_000_000, bytes_accessed=10_000_000, transcendentals=0
        ),
        name="attention",
    )(words, counts, own, other, gain, w_pad)


def backward_kernel(
    words_ref,
    own_ref,
    other_ref,
    wout_ref,
    w_ref,
    packed_ref,
    prob_ref,
    normed_ref,
    upstream_ref,
    packed_grad_ref,
    in_own_ref,
    in_other_ref,
    gain_term,
):
    step = pl.program_id(0)

    @pl.when(step == 0)
    def _():
        gain_term[...] = jnp.zeros_like(gain_term)

    @pl.when(step < IMG)
    def _():
        first = words_ref[0] == 0
        own = own_ref[...].reshape(64, WIDTH)
        other = other_ref[...].reshape(64, WIDTH)
        upstream = jnp.concatenate(
            [jnp.where(first, own, other), jnp.where(first, other, own)], axis=0
        )
        upstream_ref[...] = upstream
        mixed_grads = dot(upstream, wout_ref[...], 1, 1).astype(BF)
        pieces = []
        for head in range(2):
            query, key, value = (
                packed_ref[:, (head * 3 + i) * LANE : (head * 3 + i + 1) * LANE]
                for i in range(3)
            )
            probability = prob_ref[0, head]
            mixed_grad = mixed_grads[:, head * LANE : (head + 1) * LANE]
            prob_grad = dot(mixed_grad, value, 1, 1)
            inner = jnp.sum(probability * prob_grad, axis=-1, keepdims=True)
            score_grad = (probability * (prob_grad - inner) * SCALING).astype(BF)
            pieces.append(dot(score_grad, key, 1, 0))
            pieces.append(dot(score_grad, query, 0, 0))
            pieces.append(dot(probability.astype(BF), mixed_grad, 0, 0))
        packed_grad_ref[...] = shifted_sum(pieces, 512)[:, :480].astype(BF)
        wide = jnp.concatenate([piece.astype(BF) for piece in pieces], axis=1)
        in_part = dot(wide, w_ref[...], 1, 0).astype(BF)
        gain_term[...] += jnp.sum(
            in_part.astype(F32) * normed_ref[...].astype(F32), axis=0, keepdims=True
        )
        low, high = in_part[:64], in_part[64:]
        in_own_ref[...] = jnp.where(first, low, high).reshape(4, 1, 16, WIDTH)
        in_other_ref[...] = jnp.where(first, high, low).reshape(4, 1, 16, WIDTH)

    @pl.when(step == IMG)
    def _():
        row = lax.broadcasted_iota(jnp.int32, (16, WIDTH), 0)
        plane = jnp.where(row == 0, gain_term[...], 0.0).astype(BF)
        for peer in range(4):
            in_own_ref[peer, 0] = plane
            in_other_ref[peer, 0] = plane


def backward(words, own, other, wout_pad, w_pad, packed, prob, normed):
    def image(i):
        return jnp.minimum(i, IMG - 1)

    quarter = pl.BlockSpec((4, 1, 16, WIDTH), lambda i: (0, image(i), 0, 0))
    plane = pl.BlockSpec((4, 1, 16, WIDTH), lambda i: (0, i, 0, 0))
    rows = pl.BlockSpec((TILE, WIDTH), lambda i: (image(i), 0))
    return pl.pallas_call(
        backward_kernel,
        grid=(IMG + 1,),
        out_shape=(
            jax.ShapeDtypeStruct((ROWS, WIDTH), BF),
            jax.ShapeDtypeStruct((ROWS, 6 * HEAD), BF),
            jax.ShapeDtypeStruct((4, IMG + 1, 16, WIDTH), BF),
            jax.ShapeDtypeStruct((4, IMG + 1, 16, WIDTH), BF),
        ),
        in_specs=[
            smem(),
            quarter,
            quarter,
            pl.BlockSpec((2 * LANE, WIDTH), lambda i: (0, 0)),
            pl.BlockSpec((6 * LANE, WIDTH), lambda i: (0, 0)),
            pl.BlockSpec((TILE, 6 * LANE), lambda i: (image(i), 0)),
            pl.BlockSpec((1, 2, TILE, TILE), lambda i: (image(i), 0, 0, 0)),
            rows,
        ],
        out_specs=(
            rows,
            pl.BlockSpec((TILE, 6 * HEAD), lambda i: (image(i), 0)),
            plane,
            plane,
        ),
        scratch_shapes=[pltpu.VMEM((1, WIDTH), F32)],
        cost_estimate=pl.CostEstimate(
            flops=10_000_000_000, bytes_accessed=10_000_000, transcendentals=0
        ),
        name="backward",
    )(words, own, other, wout_pad, w_pad, packed, prob, normed)


def weights_kernel(normed_ref, upstream_ref, packed_grad_ref, mixed_ref, out_ref):
    qkv = dot(normed_ref[...], packed_grad_ref[...], 0, 0)
    out = dot(upstream_ref[...], mixed_ref[...], 0, 0)
    out_ref[...] = jnp.concatenate([qkv, out], axis=1).astype(BF)


def weight_terms(normed, upstream, packed_grad, mixed):
    return pl.pallas_call(
        weights_kernel,
        grid=(2,),
        out_shape=jax.ShapeDtypeStruct((WIDTH, 640), BF),
        in_specs=[
            pl.BlockSpec((ROWS, 640), lambda i: (0, i)),
            pl.BlockSpec((ROWS, 640), lambda i: (0, i)),
            pl.BlockSpec((ROWS, 6 * HEAD), lambda i: (0, 0)),
            pl.BlockSpec((ROWS, 2 * HEAD), lambda i: (0, 0)),
        ],
        out_specs=pl.BlockSpec((640, 640), lambda i: (i, 0)),
        cost_estimate=pl.CostEstimate(
            flops=4_000_000_000, bytes_accessed=6_000_000, transcendentals=0
        ),
        name="weight_terms",
    )(normed, upstream, packed_grad, mixed)


def norm_back_kernel(arrived_ref, block_ref, upstream_ref, gain_ref, out_ref, term_ref):
    gain = gain_ref[...]
    results = []
    for image in range(IMG + 1):
        incoming = arrived_ref[0, image].astype(F32)
        for peer in range(1, 4):
            incoming = incoming + arrived_ref[peer, image].astype(F32)
        if image == IMG:
            term_ref[...] = incoming[:8]
            continue
        normed, inverse = normalize(block_ref[image].astype(F32))
        scaled = incoming * gain
        inner = jnp.mean(scaled * normed, axis=-1, keepdims=True)
        outgoing = inverse * (scaled - jnp.mean(scaled, axis=-1, keepdims=True) - normed * inner)
        results.append(upstream_ref[image].astype(F32) + outgoing)
    grads = jnp.concatenate(results, axis=0)
    for share in range(8):
        start = share * 160 // LANE * LANE
        offset = share * 160 - start
        lanes = min(256 if offset + 160 <= 256 else 384, WIDTH - start)
        window = grads[:, start : start + lanes]
        if offset:
            window = pltpu.roll(window, lanes - offset, 1)
        out_ref[share] = window[:, :160].astype(BF)


def norm_back(arrived, block_rows, upstream_rows, gain):
    return pl.pallas_call(
        norm_back_kernel,
        out_shape=(
            jax.ShapeDtypeStruct((8, 80, 160), BF),
            jax.ShapeDtypeStruct((8, WIDTH), F32),
        ),
        in_specs=[pl.BlockSpec(memory_space=pltpu.VMEM)] * 4,
        out_specs=(pl.BlockSpec(memory_space=pltpu.VMEM),) * 2,
        name="norm_back",
    )(arrived, block_rows, upstream_rows, gain)


def summed(blocks):
    return blocks.astype(F32).sum(axis=0)


def after(value, *earlier):
    return lax.optimization_barrier((value, *earlier))[0]


def near_sum(term, columns):
    blocks = term.reshape(8, 4, -1, columns)
    here = lax.axis_index("x")

    def rows_of(at):
        return lax.dynamic_index_in_dim(blocks, lax.rem(here + at, 4), 1, keepdims=False)

    got = [shifted(rows_of(at), "x", at) for at in (2, 1, 3)]
    own = rows_of(0)
    total = own.astype(F32)
    for rows in got:
        total = total + rows.astype(F32)
    return total.astype(BF)


def shards(grad_rows, features, block_in, patch_counts, owner, ln1_gain, w_qkv, w_out, w_proj):
    device = lax.axis_index(ENC)
    core = lax.axis_index("c")
    place = core * 4 + lax.axis_index("y")
    words = jnp.stack([core, place, lax.axis_index("y")]).astype(jnp.int32)
    place_word = place.reshape(1).astype(jnp.int32)
    gain = ln1_gain.reshape(1, WIDTH)
    columns = grad_rows.shape[1]

    own_counts = lax.dynamic_index_in_dim(patch_counts, device, 0, keepdims=False)
    images = jnp.arange(PEERS * IMG, dtype=jnp.int32)
    block_of = images // IMG
    owners = owner.reshape(-1)
    ahead = (owners[:, None] == owners[None, :]) & (block_of[None, :] < block_of[:, None])
    target = owners * IMG + jnp.sum(ahead.astype(jnp.int32), axis=1)
    hits = target[None, :] == images[:, None]
    source_of = jnp.sum(jnp.where(hits, images[None, :], 0), axis=1)
    all_counts = jnp.sum(jnp.where(hits, patch_counts.reshape(1, -1), 0), axis=1)
    arrived_counts = lax.dynamic_slice_in_dim(all_counts, device * IMG, IMG, 0)

    by_place = grad_rows.reshape(IMG, 2, 4, 16, -1).transpose(1, 2, 0, 3, 4)
    by_place = by_place.reshape(2, ROWS // 2, -1)
    for_other = lax.dynamic_index_in_dim(by_place, 1 - core, 0, keepdims=False)
    for_own = lax.dynamic_index_in_dim(by_place, core, 0, keepdims=False)
    part_other = dot(for_other, w_proj, 1, 1).astype(BF)
    from_other = swapped(part_other)
    part_own = dot(for_own, w_proj, 1, 1)
    pair = (part_own + from_other.astype(F32)).astype(BF)
    features = after(features, pair)
    arrived = exchanged(pair.reshape(4, 80, WIDTH), "y").reshape(4, IMG, 16, WIDTH)

    line = jnp.arange(TILE, dtype=jnp.int32)
    live_own = (line[None, :] < own_counts[:, None]).reshape(-1)
    kept_rows = jnp.where(live_own[:, None], features, jnp.zeros_like(features))
    proj_term = dot(kept_rows, grad_rows, 0, 0).astype(BF)
    arrived = after(arrived, proj_term)
    pieces = spread(place_word, own_counts, arrived)
    proj_near = near_sum(proj_term, columns)

    share = after(block_in.T, arrived)
    block_own = jnp.stack([share] + [shifted(share, "y", at) for at in (1, 2, 3)])
    block_other = swapped(block_own)

    w_pad = jnp.pad(w_qkv.transpose(1, 2, 0).reshape(6, HEAD, WIDTH), ((0, 0), (0, 48), (0, 0)))
    w_pad = w_pad.reshape(6 * LANE, WIDTH)
    wout_pad = jnp.pad(w_out.reshape(2, HEAD, WIDTH), ((0, 0), (0, 48), (0, 0)))
    wout_pad = wout_pad.reshape(2 * LANE, WIDTH)
    normed_in, normed, block_rows, packed, prob, mixed = attention(
        words, arrived_counts, block_own, block_other, gain, w_pad
    )

    passing = exchanged(pieces, ENC)
    passing = forwarded(source_of, passing)
    landed = after(exchanged(passing, ENC), proj_near, prob)
    upstream_rows, copies = collected(landed)
    half_own = exchanged(copies.reshape(4, 80, WIDTH), "y").reshape(4, IMG, 16, WIDTH)
    half_other = swapped(half_own)

    proj_far = exchanged(after(proj_near, half_own), "z")

    upstream, packed_grad, in_own, in_other = backward(
        words, half_own, half_other, wout_pad, w_pad, packed, prob, normed
    )
    in_got = swapped(in_other)
    terms = weight_terms(normed_in, upstream, packed_grad, mixed)
    in_pair = (in_own.astype(F32) + in_got.astype(F32)).astype(BF)
    in_pair, proj_far = lax.optimization_barrier((in_pair, proj_far))
    grad_proj = summed(proj_far)
    in_arrived = exchanged(in_pair.reshape(4, 96, WIDTH), "y").reshape(4, IMG + 1, 16, WIDTH)
    term_near = near_sum(terms, 640)
    shares, gain_term = norm_back(in_arrived, block_rows, upstream_rows, gain)
    shares = exchanged(shares, TP)
    grad_input = shares.reshape(4, 2, IMG, 16, 160).transpose(2, 1, 0, 3, 4)
    grad_input = grad_input.reshape(ROWS, 160)
    gain_near = near_sum(gain_term[0].astype(BF).reshape(PEERS * 40, 1), 1)
    last = jnp.concatenate([term_near, jnp.pad(gain_near, ((0, 0), (0, 0), (0, 127)))], axis=2)
    last = summed(exchanged(last, "z"))
    grad_qkv = last[:, :480].reshape(40, 2, 240)
    grad_out = last[:, 480:640].T
    grad_ln1 = last[:, 640]
    return (grad_input, grad_proj, grad_qkv, grad_out, grad_ln1)


def solution(mesh):
    torus = Mesh(mesh.devices.reshape(8, 4, 4, 2), ("z", "x", "y", "c"))

    return jax.shard_map(
        shards,
        mesh=torus,
        in_specs=(
            P(ENC, TP),
            P(ENC, None),
            P(ENC, TP),
            P(),
            P(),
            P(),
            P(None, TP, None),
            P(TP, None),
            P(None, TP),
        ),
        out_specs=(P(ENC, TP), P(ENC, TP), P(ENC, TP, None), P(TP, ENC), P(ENC)),
        check_vma=False,
    )
```

```python
import jax
import jax.numpy as jnp
from jax import lax
from jax.experimental import pallas as pl
from jax.experimental.pallas import tpu as pltpu
from jax.sharding import Mesh
from jax.sharding import PartitionSpec as P


TILE = 128
IMG = 5
ROWS = IMG * TILE
WIDTH = 1280
HEAD = 80
LANE = 128
PEERS = 32
ENC = ("z", "x")
TP = ("y", "c")
EPSILON = 1e-05
SCALING = 1.0 / HEAD**0.5
BF = jnp.bfloat16
F32 = jnp.float32
SWAP = ((0, 1), (1, 0))


def exchanged(blocks, axis):
    return lax.all_to_all(blocks, axis, split_axis=0, concat_axis=0, tiled=True)


def shifted(values, axis, by):
    pairs = tuple((i, (i + by) % 4) for i in range(4))
    return lax.ppermute(values, axis, pairs)


def swapped(values):
    return lax.ppermute(values, "c", SWAP)


def dot(left, right, dim_left, dim_right):
    return lax.dot_general(
        left, right, (((dim_left,), (dim_right,)), ((), ())), preferred_element_type=F32
    )


def smem():
    return pl.BlockSpec(memory_space=pltpu.SMEM)


def normalize(values):
    centred = values - jnp.mean(values, axis=-1, keepdims=True)
    variance = jnp.mean(centred * centred, axis=-1, keepdims=True)
    inverse = lax.rsqrt(variance + EPSILON)
    return (centred * inverse, inverse)


def shifted_sum(pieces, lanes):
    total = None
    for at, piece in enumerate(pieces):
        wide = jnp.concatenate(
            [piece, jnp.zeros((piece.shape[0], lanes - LANE), piece.dtype)], axis=1
        )
        if at:
            wide = pltpu.roll(wide, HEAD * at, 1)
        total = wide if total is None else total + wide
    return total


def spread_kernel(place_ref, counts_ref, arrived_ref, out_ref):
    first_row = place_ref[0] * 16
    for image in range(IMG):
        rows = arrived_ref[0, image].astype(F32)
        for peer in range(1, 4):
            rows = rows + arrived_ref[peer, image].astype(F32)
        line = first_row + lax.broadcasted_iota(jnp.int32, rows.shape, 0)
        rows = jnp.where(line < counts_ref[image], rows, 0.0).astype(BF)
        for half in range(2):
            for group in range(10):
                out_ref[half * 10 + group, image] = rows[
                    half * 8 : half * 8 + 8, group * LANE : (group + 1) * LANE
                ]
    out_ref[20:32] = jnp.zeros((12, IMG, 8, LANE), BF)


def spread(place, counts, arrived):
    return pl.pallas_call(
        spread_kernel,
        out_shape=jax.ShapeDtypeStruct((PEERS, IMG, 8, LANE), BF),
        in_specs=[smem(), smem(), pl.BlockSpec(memory_space=pltpu.VMEM)],
        out_specs=pl.BlockSpec(memory_space=pltpu.VMEM),
        name="spread",
    )(place, counts, arrived)


def forward_kernel(index_ref, pieces_ref, out_ref):
    def step(at, carry):
        out_ref[at] = pieces_ref[index_ref[at]]
        return carry

    lax.fori_loop(0, PEERS * IMG, step, 0, unroll=8)


def forwarded(index, pieces):
    flat = pieces.reshape(PEERS * IMG, 8, LANE)
    return pl.pallas_call(
        forward_kernel,
        out_shape=jax.ShapeDtypeStruct(flat.shape, BF),
        in_specs=[smem(), pl.BlockSpec(memory_space=pltpu.VMEM)],
        out_specs=pl.BlockSpec(memory_space=pltpu.VMEM),
        name="forwarded",
    )(index, flat).reshape(pieces.shape)


def collect_kernel(pieces_ref, rows_ref, copies_ref):
    for image in range(IMG):
        for half in range(2):
            for group in range(10):
                piece = pieces_ref[half * 10 + group, image]
                at = (slice(half * 8, half * 8 + 8), slice(group * LANE, (group + 1) * LANE))
                rows_ref[image, at[0], at[1]] = piece
                for peer in range(4):
                    copies_ref[peer, image, at[0], at[1]] = piece


def collected(pieces):
    return pl.pallas_call(
        collect_kernel,
        out_shape=(
            jax.ShapeDtypeStruct((IMG, 16, WIDTH), BF),
            jax.ShapeDtypeStruct((4, IMG, 16, WIDTH), BF),
        ),
        in_specs=[pl.BlockSpec(memory_space=pltpu.VMEM)],
        out_specs=(pl.BlockSpec(memory_space=pltpu.VMEM),) * 2,
        name="collected",
    )(pieces)


def attention_kernel(
    words_ref,
    counts_ref,
    own_ref,
    other_ref,
    gain_ref,
    w_ref,
    normed_in_ref,
    normed_ref,
    rows_ref,
    packed_ref,
    prob_ref,
    mixed_ref,
    scratch,
):
    first = words_ref[0] == 0
    shares = []
    for near in range(4):
        at = lax.rem(words_ref[2] + 4 - near, 4)
        own, other = own_ref[at], other_ref[at]
        shares += [jnp.where(first, own, other), jnp.where(first, other, own)]
    values = jnp.concatenate(shares, axis=0).astype(F32).T
    scratch[...] = values
    rows_ref[0] = scratch[pl.ds(pl.multiple_of(words_ref[1] * 16, 16), 16), :].astype(BF)
    normed, _ = normalize(values)
    normed_ref[...] = normed.astype(BF)
    normed_in = (normed * gain_ref[...]).astype(BF)
    normed_in_ref[...] = normed_in
    packed = dot(normed_in, w_ref[...], 1, 1).astype(BF)
    packed_ref[...] = packed
    count = counts_ref[pl.program_id(0)]
    live_row = lax.broadcasted_iota(jnp.int32, (TILE, TILE), 0) < count
    live_col = lax.broadcasted_iota(jnp.int32, (TILE, TILE), 1) < count
    same_kind = (live_row & live_col) | (~live_row & ~live_col)
    mixed = []
    for head in range(2):
        query, key, value = (
            packed[:, (head * 3 + i) * LANE : (head * 3 + i + 1) * LANE] for i in range(3)
        )
        scores = jnp.where(same_kind, dot(query, key, 1, 1) * SCALING, -1e30)
        exp_terms = jnp.exp(scores - jnp.max(scores, axis=-1, keepdims=True))
        probability = exp_terms / jnp.sum(exp_terms, axis=-1, keepdims=True)
        prob_ref[0, head] = probability
        mixed.append(dot(probability.astype(BF), value, 1, 0))
    mixed_ref[...] = shifted_sum(mixed, 256)[:, :160].astype(BF)


def attention(words, counts, own, other, gain, w_pad):
    share = pl.BlockSpec((4, 160, TILE), lambda i: (0, 0, i))
    rows = pl.BlockSpec((TILE, WIDTH), lambda i: (i, 0))
    return pl.pallas_call(
        attention_kernel,
        grid=(IMG,),
        out_shape=(
            jax.ShapeDtypeStruct((ROWS, WIDTH), BF),
            jax.ShapeDtypeStruct((ROWS, WIDTH), BF),
            jax.ShapeDtypeStruct((IMG, 16, WIDTH), BF),
            jax.ShapeDtypeStruct((ROWS, 6 * LANE), BF),
            jax.ShapeDtypeStruct((IMG, 2, TILE, TILE), F32),
            jax.ShapeDtypeStruct((ROWS, 2 * HEAD), BF),
        ),
        in_specs=[
            smem(),
            smem(),
            share,
            share,
            pl.BlockSpec((1, WIDTH), lambda i: (0, 0)),
            pl.BlockSpec((6 * LANE, WIDTH), lambda i: (0, 0)),
        ],
        out_specs=(
            rows,
            rows,
            pl.BlockSpec((1, 16, WIDTH), lambda i: (i, 0, 0)),
            pl.BlockSpec((TILE, 6 * LANE), lambda i: (i, 0)),
            pl.BlockSpec((1, 2, TILE, TILE), lambda i: (i, 0, 0, 0)),
            pl.BlockSpec((TILE, 2 * HEAD), lambda i: (i, 0)),
        ),
        scratch_shapes=[pltpu.VMEM((TILE, WIDTH), F32)],
        cost_estimate=pl.CostEstimate(
            flops=10_000_000_000, bytes_accessed=10_000_000, transcendentals=0
        ),
        name="attention",
    )(words, counts, own, other, gain, w_pad)


def backward_kernel(
    words_ref,
    own_ref,
    other_ref,
    wout_ref,
    w_ref,
    packed_ref,
    prob_ref,
    normed_ref,
    upstream_ref,
    packed_grad_ref,
    in_own_ref,
    in_other_ref,
    gain_term,
):
    step = pl.program_id(0)

    @pl.when(step == 0)
    def _():
        gain_term[...] = jnp.zeros_like(gain_term)

    @pl.when(step < IMG)
    def _():
        first = words_ref[0] == 0
        own = own_ref[...].reshape(64, WIDTH)
        other = other_ref[...].reshape(64, WIDTH)
        upstream = jnp.concatenate(
            [jnp.where(first, own, other), jnp.where(first, other, own)], axis=0
        )
        upstream_ref[...] = upstream
        mixed_grads = dot(upstream, wout_ref[...], 1, 1).astype(BF)
        pieces = []
        for head in range(2):
            query, key, value = (
                packed_ref[:, (head * 3 + i) * LANE : (head * 3 + i + 1) * LANE]
                for i in range(3)
            )
            probability = prob_ref[0, head]
            mixed_grad = mixed_grads[:, head * LANE : (head + 1) * LANE]
            prob_grad = dot(mixed_grad, value, 1, 1)
            inner = jnp.sum(probability * prob_grad, axis=-1, keepdims=True)
            score_grad = (probability * (prob_grad - inner) * SCALING).astype(BF)
            pieces.append(dot(score_grad, key, 1, 0))
            pieces.append(dot(score_grad, query, 0, 0))
            pieces.append(dot(probability.astype(BF), mixed_grad, 0, 0))
        packed_grad_ref[...] = shifted_sum(pieces, 512)[:, :480].astype(BF)
        wide = jnp.concatenate([piece.astype(BF) for piece in pieces], axis=1)
        in_part = dot(wide, w_ref[...], 1, 0).astype(BF)
        gain_term[...] += jnp.sum(
            in_part.astype(F32) * normed_ref[...].astype(F32), axis=0, keepdims=True
        )
        low, high = in_part[:64], in_part[64:]
        in_own_ref[...] = jnp.where(first, low, high).reshape(4, 1, 16, WIDTH)
        in_other_ref[...] = jnp.where(first, high, low).reshape(4, 1, 16, WIDTH)

    @pl.when(step == IMG)
    def _():
        row = lax.broadcasted_iota(jnp.int32, (16, WIDTH), 0)
        plane = jnp.where(row == 0, gain_term[...], 0.0).astype(BF)
        for peer in range(4):
            in_own_ref[peer, 0] = plane
            in_other_ref[peer, 0] = plane


def backward(words, own, other, wout_pad, w_pad, packed, prob, normed):
    def image(i):
        return jnp.minimum(i, IMG - 1)

    quarter = pl.BlockSpec((4, 1, 16, WIDTH), lambda i: (0, image(i), 0, 0))
    plane = pl.BlockSpec((4, 1, 16, WIDTH), lambda i: (0, i, 0, 0))
    rows = pl.BlockSpec((TILE, WIDTH), lambda i: (image(i), 0))
    return pl.pallas_call(
        backward_kernel,
        grid=(IMG + 1,),
        out_shape=(
            jax.ShapeDtypeStruct((ROWS, WIDTH), BF),
            jax.ShapeDtypeStruct((ROWS, 6 * HEAD), BF),
            jax.ShapeDtypeStruct((4, IMG + 1, 16, WIDTH), BF),
            jax.ShapeDtypeStruct((4, IMG + 1, 16, WIDTH), BF),
        ),
        in_specs=[
            smem(),
            quarter,
            quarter,
            pl.BlockSpec((2 * LANE, WIDTH), lambda i: (0, 0)),
            pl.BlockSpec((6 * LANE, WIDTH), lambda i: (0, 0)),
            pl.BlockSpec((TILE, 6 * LANE), lambda i: (image(i), 0)),
            pl.BlockSpec((1, 2, TILE, TILE), lambda i: (image(i), 0, 0, 0)),
            rows,
        ],
        out_specs=(
            rows,
            pl.BlockSpec((TILE, 6 * HEAD), lambda i: (image(i), 0)),
            plane,
            plane,
        ),
        scratch_shapes=[pltpu.VMEM((1, WIDTH), F32)],
        cost_estimate=pl.CostEstimate(
            flops=10_000_000_000, bytes_accessed=10_000_000, transcendentals=0
        ),
        name="backward",
    )(words, own, other, wout_pad, w_pad, packed, prob, normed)


def weights_kernel(normed_ref, upstream_ref, packed_grad_ref, mixed_ref, out_ref):
    qkv = dot(normed_ref[...], packed_grad_ref[...], 0, 0)
    out = dot(upstream_ref[...], mixed_ref[...], 0, 0)
    out_ref[...] = jnp.concatenate([qkv, out], axis=1).astype(BF)


def weight_terms(normed, upstream, packed_grad, mixed):
    return pl.pallas_call(
        weights_kernel,
        grid=(2,),
        out_shape=jax.ShapeDtypeStruct((WIDTH, 640), BF),
        in_specs=[
            pl.BlockSpec((ROWS, 640), lambda i: (0, i)),
            pl.BlockSpec((ROWS, 640), lambda i: (0, i)),
            pl.BlockSpec((ROWS, 6 * HEAD), lambda i: (0, 0)),
            pl.BlockSpec((ROWS, 2 * HEAD), lambda i: (0, 0)),
        ],
        out_specs=pl.BlockSpec((640, 640), lambda i: (i, 0)),
        cost_estimate=pl.CostEstimate(
            flops=4_000_000_000, bytes_accessed=6_000_000, transcendentals=0
        ),
        name="weight_terms",
    )(normed, upstream, packed_grad, mixed)


def norm_back_kernel(arrived_ref, block_ref, upstream_ref, gain_ref, out_ref, term_ref):
    gain = gain_ref[...]
    results = []
    for image in range(IMG + 1):
        incoming = arrived_ref[0, image].astype(F32)
        for peer in range(1, 4):
            incoming = incoming + arrived_ref[peer, image].astype(F32)
        if image == IMG:
            term_ref[...] = incoming[:8]
            continue
        normed, inverse = normalize(block_ref[image].astype(F32))
        scaled = incoming * gain
        inner = jnp.mean(scaled * normed, axis=-1, keepdims=True)
        outgoing = inverse * (scaled - jnp.mean(scaled, axis=-1, keepdims=True) - normed * inner)
        results.append(upstream_ref[image].astype(F32) + outgoing)
    grads = jnp.concatenate(results, axis=0)
    for share in range(8):
        start = share * 160 // LANE * LANE
        offset = share * 160 - start
        lanes = min(256 if offset + 160 <= 256 else 384, WIDTH - start)
        window = grads[:, start : start + lanes]
        if offset:
            window = pltpu.roll(window, lanes - offset, 1)
        out_ref[share] = window[:, :160].astype(BF)


def norm_back(arrived, block_rows, upstream_rows, gain):
    return pl.pallas_call(
        norm_back_kernel,
        out_shape=(
            jax.ShapeDtypeStruct((8, 80, 160), BF),
            jax.ShapeDtypeStruct((8, WIDTH), F32),
        ),
        in_specs=[pl.BlockSpec(memory_space=pltpu.VMEM)] * 4,
        out_specs=(pl.BlockSpec(memory_space=pltpu.VMEM),) * 2,
        name="norm_back",
    )(arrived, block_rows, upstream_rows, gain)


def summed(blocks):
    return blocks.astype(F32).sum(axis=0)


def after(value, *earlier):
    return lax.optimization_barrier((value, *earlier))[0]


def near_sum(term, columns):
    blocks = term.reshape(8, 4, -1, columns)
    here = lax.axis_index("x")

    def rows_of(at):
        return lax.dynamic_index_in_dim(blocks, lax.rem(here + at, 4), 1, keepdims=False)

    got = [shifted(rows_of(at), "x", at) for at in (2, 1, 3)]
    own = rows_of(0)
    total = own.astype(F32)
    for rows in got:
        total = total + rows.astype(F32)
    return total.astype(BF)


def shards(grad_rows, features, block_in, patch_counts, owner, ln1_gain, w_qkv, w_out, w_proj):
    device = lax.axis_index(ENC)
    core = lax.axis_index("c")
    place = core * 4 + lax.axis_index("y")
    words = jnp.stack([core, place, lax.axis_index("y")]).astype(jnp.int32)
    place_word = place.reshape(1).astype(jnp.int32)
    gain = ln1_gain.reshape(1, WIDTH)
    columns = grad_rows.shape[1]

    own_counts = lax.dynamic_index_in_dim(patch_counts, device, 0, keepdims=False)
    images = jnp.arange(PEERS * IMG, dtype=jnp.int32)
    block_of = images // IMG
    owners = owner.reshape(-1)
    ahead = (owners[:, None] == owners[None, :]) & (block_of[None, :] < block_of[:, None])
    target = owners * IMG + jnp.sum(ahead.astype(jnp.int32), axis=1)
    hits = target[None, :] == images[:, None]
    source_of = jnp.sum(jnp.where(hits, images[None, :], 0), axis=1)
    all_counts = jnp.sum(jnp.where(hits, patch_counts.reshape(1, -1), 0), axis=1)
    arrived_counts = lax.dynamic_slice_in_dim(all_counts, device * IMG, IMG, 0)

    by_place = grad_rows.reshape(IMG, 2, 4, 16, -1).transpose(1, 2, 0, 3, 4)
    by_place = by_place.reshape(2, ROWS // 2, -1)
    for_other = lax.dynamic_index_in_dim(by_place, 1 - core, 0, keepdims=False)
    for_own = lax.dynamic_index_in_dim(by_place, core, 0, keepdims=False)
    part_other = dot(for_other, w_proj, 1, 1).astype(BF)
    from_other = swapped(part_other)
    part_own = dot(for_own, w_proj, 1, 1)
    pair = (part_own + from_other.astype(F32)).astype(BF)
    features = after(features, pair)
    arrived = exchanged(pair.reshape(4, 80, WIDTH), "y").reshape(4, IMG, 16, WIDTH)

    line = jnp.arange(TILE, dtype=jnp.int32)
    live_own = (line[None, :] < own_counts[:, None]).reshape(-1)
    kept_rows = jnp.where(live_own[:, None], features, jnp.zeros_like(features))
    proj_term = dot(kept_rows, grad_rows, 0, 0).astype(BF)
    arrived = after(arrived, proj_term)
    pieces = spread(place_word, own_counts, arrived)
    proj_near = near_sum(proj_term, columns)

    share = after(block_in.T, arrived)
    block_own = jnp.stack([share] + [shifted(share, "y", at) for at in (1, 2, 3)])
    block_other = swapped(block_own)

    w_pad = jnp.pad(w_qkv.transpose(1, 2, 0).reshape(6, HEAD, WIDTH), ((0, 0), (0, 48), (0, 0)))
    w_pad = w_pad.reshape(6 * LANE, WIDTH)
    wout_pad = jnp.pad(w_out.reshape(2, HEAD, WIDTH), ((0, 0), (0, 48), (0, 0)))
    wout_pad = wout_pad.reshape(2 * LANE, WIDTH)
    normed_in, normed, block_rows, packed, prob, mixed = attention(
        words, arrived_counts, block_own, block_other, gain, w_pad
    )

    passing = exchanged(pieces, ENC)
    passing = forwarded(source_of, passing)
    landed = after(exchanged(passing, ENC), prob)
    upstream_rows, copies = collected(landed)
    half_own = exchanged(copies.reshape(4, 80, WIDTH), "y").reshape(4, IMG, 16, WIDTH)
    half_other = swapped(half_own)

    proj_far = exchanged(after(proj_near, half_own), "z")

    upstream, packed_grad, in_own, in_other = backward(
        words, half_own, half_other, wout_pad, w_pad, packed, prob, normed
    )
    in_got = swapped(in_other)
    terms = weight_terms(normed_in, upstream, packed_grad, mixed)
    in_pair = (in_own.astype(F32) + in_got.astype(F32)).astype(BF)
    in_pair, proj_far = lax.optimization_barrier((in_pair, proj_far))
    grad_proj = summed(proj_far)
    in_arrived = exchanged(in_pair.reshape(4, 96, WIDTH), "y").reshape(4, IMG + 1, 16, WIDTH)
    term_near = near_sum(terms, 640)
    shares, gain_term = norm_back(in_arrived, block_rows, upstream_rows, gain)
    shares = exchanged(shares, TP)
    grad_input = shares.reshape(4, 2, IMG, 16, 160).transpose(2, 1, 0, 3, 4)
    grad_input = grad_input.reshape(ROWS, 160)
    last = summed(exchanged(term_near, "z"))
    gain_rows = gain_term[0].astype(BF).reshape(8, 4, 40).transpose(1, 0, 2)
    gain_rows = gain_rows.reshape(4, 1, 320)
    here = lax.axis_index("x")

    def gain_of(at):
        return lax.dynamic_index_in_dim(gain_rows, lax.rem(here + at, 4), 0, keepdims=False)

    gain_sum = gain_of(0).astype(F32)
    for at in (2, 1, 3):
        gain_sum = gain_sum + shifted(gain_of(at), "x", at).astype(F32)
    gain_sum = gain_sum.reshape(8, 40)
    far = lax.axis_index("z")
    for reach in (4, 2, 1):
        upper = (far // reach) % 2 == 1
        low, high = gain_sum[:reach], gain_sum[reach:]
        sent = jnp.where(upper, low, high).astype(BF)
        got = lax.ppermute(sent, "z", tuple((i, i ^ reach) for i in range(8)))
        gain_sum = jnp.where(upper, high, low) + got.astype(F32)
    grad_qkv = last[:, :480].reshape(40, 2, 240)
    grad_out = last[:, 480:].T
    grad_ln1 = gain_sum.reshape(40)
    return (grad_input, grad_proj, grad_qkv, grad_out, grad_ln1)


def solution(mesh):
    torus = Mesh(mesh.devices.reshape(8, 4, 4, 2), ("z", "x", "y", "c"))

    return jax.shard_map(
        shards,
        mesh=torus,
        in_specs=(
            P(ENC, TP),
            P(ENC, None),
            P(ENC, TP),
            P(),
            P(),
            P(),
            P(None, TP, None),
            P(TP, None),
            P(None, TP),
        ),
        out_specs=(P(ENC, TP), P(ENC, TP), P(ENC, TP, None), P(TP, ENC), P(ENC)),
        check_vma=False,
    )
```

```python
import jax
import jax.numpy as jnp
from jax import lax
from jax.experimental import pallas as pl
from jax.experimental.pallas import tpu as pltpu
from jax.sharding import Mesh
from jax.sharding import PartitionSpec as P


TILE = 128
IMG = 5
ROWS = IMG * TILE
WIDTH = 1280
HEAD = 80
LANE = 128
PEERS = 32
ENC = ("z", "x")
TP = ("y", "c")
EPSILON = 1e-05
SCALING = 1.0 / HEAD**0.5
BF = jnp.bfloat16
F32 = jnp.float32
SWAP = ((0, 1), (1, 0))


def padded_heads(padded_ref, heads_ref):
    for at in range(heads_ref.shape[0] // HEAD):
        padded_ref[at * LANE : at * LANE + HEAD] = heads_ref[at * HEAD : (at + 1) * HEAD]
        padded_ref[at * LANE + HEAD : (at + 1) * LANE] = jnp.zeros((LANE - HEAD, WIDTH), BF)


def exchanged(blocks, axis):
    return lax.all_to_all(blocks, axis, split_axis=0, concat_axis=0, tiled=True)


def shifted(values, axis, by):
    pairs = tuple((i, (i + by) % 4) for i in range(4))
    return lax.ppermute(values, axis, pairs)


def swapped(values):
    return lax.ppermute(values, "c", SWAP)


def dot(left, right, dim_left, dim_right):
    return lax.dot_general(
        left, right, (((dim_left,), (dim_right,)), ((), ())), preferred_element_type=F32
    )


def smem():
    return pl.BlockSpec(memory_space=pltpu.SMEM)


def normalize(values):
    centred = values - jnp.mean(values, axis=-1, keepdims=True)
    variance = jnp.mean(centred * centred, axis=-1, keepdims=True)
    inverse = lax.rsqrt(variance + EPSILON)
    return (centred * inverse, inverse)


def shifted_sum(pieces, lanes):
    total = None
    for at, piece in enumerate(pieces):
        wide = jnp.concatenate(
            [piece, jnp.zeros((piece.shape[0], lanes - LANE), piece.dtype)], axis=1
        )
        if at:
            wide = pltpu.roll(wide, HEAD * at, 1)
        total = wide if total is None else total + wide
    return total


def spread_kernel(place_ref, counts_ref, arrived_ref, out_ref):
    first_row = place_ref[0] * 16
    for image in range(IMG):
        rows = arrived_ref[0, image].astype(F32)
        for peer in range(1, 4):
            rows = rows + arrived_ref[peer, image].astype(F32)
        line = first_row + lax.broadcasted_iota(jnp.int32, rows.shape, 0)
        rows = jnp.where(line < counts_ref[image], rows, 0.0).astype(BF)
        for half in range(2):
            for group in range(10):
                out_ref[half * 10 + group, image] = rows[
                    half * 8 : half * 8 + 8, group * LANE : (group + 1) * LANE
                ]
    out_ref[20:32] = jnp.zeros((12, IMG, 8, LANE), BF)


def spread(place, counts, arrived):
    return pl.pallas_call(
        spread_kernel,
        out_shape=jax.ShapeDtypeStruct((PEERS, IMG, 8, LANE), BF),
        in_specs=[smem(), smem(), pl.BlockSpec(memory_space=pltpu.VMEM)],
        out_specs=pl.BlockSpec(memory_space=pltpu.VMEM),
        name="spread",
    )(place, counts, arrived)


def forward_kernel(index_ref, pieces_ref, out_ref):
    def step(at, carry):
        out_ref[at] = pieces_ref[index_ref[at]]
        return carry

    lax.fori_loop(0, PEERS * IMG, step, 0, unroll=8)


def forwarded(index, pieces):
    flat = pieces.reshape(PEERS * IMG, 8, LANE)
    return pl.pallas_call(
        forward_kernel,
        out_shape=jax.ShapeDtypeStruct(flat.shape, BF),
        in_specs=[smem(), pl.BlockSpec(memory_space=pltpu.VMEM)],
        out_specs=pl.BlockSpec(memory_space=pltpu.VMEM),
        name="forwarded",
    )(index, flat).reshape(pieces.shape)


def collect_kernel(pieces_ref, rows_ref, copies_ref):
    for image in range(IMG):
        for half in range(2):
            for group in range(10):
                piece = pieces_ref[half * 10 + group, image]
                at = (slice(half * 8, half * 8 + 8), slice(group * LANE, (group + 1) * LANE))
                rows_ref[image, at[0], at[1]] = piece
                for peer in range(4):
                    copies_ref[peer, image, at[0], at[1]] = piece


def collected(pieces):
    return pl.pallas_call(
        collect_kernel,
        out_shape=(
            jax.ShapeDtypeStruct((IMG, 16, WIDTH), BF),
            jax.ShapeDtypeStruct((4, IMG, 16, WIDTH), BF),
        ),
        in_specs=[pl.BlockSpec(memory_space=pltpu.VMEM)],
        out_specs=(pl.BlockSpec(memory_space=pltpu.VMEM),) * 2,
        name="collected",
    )(pieces)


def attention_kernel(
    words_ref,
    counts_ref,
    own_ref,
    other_ref,
    gain_ref,
    w_ref,
    normed_in_ref,
    normed_ref,
    rows_ref,
    packed_ref,
    prob_ref,
    mixed_ref,
    scratch,
    w_pad,
):
    @pl.when(pl.program_id(0) == 0)
    def _():
        padded_heads(w_pad, w_ref)

    first = words_ref[0] == 0
    shares = []
    for near in range(4):
        at = lax.rem(words_ref[2] + 4 - near, 4)
        own, other = own_ref[at], other_ref[at]
        shares += [jnp.where(first, own, other), jnp.where(first, other, own)]
    values = jnp.concatenate(shares, axis=0).astype(F32).T
    scratch[...] = values
    rows_ref[0] = scratch[pl.ds(pl.multiple_of(words_ref[1] * 16, 16), 16), :].astype(BF)
    normed, _ = normalize(values)
    normed_ref[...] = normed.astype(BF)
    normed_in = (normed * gain_ref[...]).astype(BF)
    normed_in_ref[...] = normed_in
    packed = dot(normed_in, w_pad[...], 1, 1).astype(BF)
    packed_ref[...] = packed
    count = counts_ref[pl.program_id(0)]
    live_row = lax.broadcasted_iota(jnp.int32, (TILE, TILE), 0) < count
    live_col = lax.broadcasted_iota(jnp.int32, (TILE, TILE), 1) < count
    same_kind = (live_row & live_col) | (~live_row & ~live_col)
    mixed = []
    for head in range(2):
        query, key, value = (
            packed[:, (head * 3 + i) * LANE : (head * 3 + i + 1) * LANE] for i in range(3)
        )
        scores = jnp.where(same_kind, dot(query, key, 1, 1) * SCALING, -1e30)
        exp_terms = jnp.exp(scores - jnp.max(scores, axis=-1, keepdims=True))
        probability = exp_terms / jnp.sum(exp_terms, axis=-1, keepdims=True)
        prob_ref[0, head] = probability
        mixed.append(dot(probability.astype(BF), value, 1, 0))
    mixed_ref[...] = shifted_sum(mixed, 256)[:, :160].astype(BF)


def attention(words, counts, own, other, gain, w_heads):
    share = pl.BlockSpec((4, 160, TILE), lambda i: (0, 0, i))
    rows = pl.BlockSpec((TILE, WIDTH), lambda i: (i, 0))
    return pl.pallas_call(
        attention_kernel,
        grid=(IMG,),
        out_shape=(
            jax.ShapeDtypeStruct((ROWS, WIDTH), BF),
            jax.ShapeDtypeStruct((ROWS, WIDTH), BF),
            jax.ShapeDtypeStruct((IMG, 16, WIDTH), BF),
            jax.ShapeDtypeStruct((ROWS, 6 * LANE), BF),
            jax.ShapeDtypeStruct((IMG, 2, TILE, TILE), F32),
            jax.ShapeDtypeStruct((ROWS, 2 * HEAD), BF),
        ),
        in_specs=[
            smem(),
            smem(),
            share,
            share,
            pl.BlockSpec((1, WIDTH), lambda i: (0, 0)),
            pl.BlockSpec((6 * HEAD, WIDTH), lambda i: (0, 0)),
        ],
        out_specs=(
            rows,
            rows,
            pl.BlockSpec((1, 16, WIDTH), lambda i: (i, 0, 0)),
            pl.BlockSpec((TILE, 6 * LANE), lambda i: (i, 0)),
            pl.BlockSpec((1, 2, TILE, TILE), lambda i: (i, 0, 0, 0)),
            pl.BlockSpec((TILE, 2 * HEAD), lambda i: (i, 0)),
        ),
        scratch_shapes=[pltpu.VMEM((TILE, WIDTH), F32), pltpu.VMEM((6 * LANE, WIDTH), BF)],
        cost_estimate=pl.CostEstimate(
            flops=10_000_000_000, bytes_accessed=10_000_000, transcendentals=0
        ),
        name="attention",
    )(words, counts, own, other, gain, w_heads)


def backward_kernel(
    words_ref,
    own_ref,
    other_ref,
    wout_ref,
    w_ref,
    packed_ref,
    prob_ref,
    normed_ref,
    upstream_ref,
    packed_grad_ref,
    in_own_ref,
    in_other_ref,
    gain_term,
    w_pad,
    wout_pad,
):
    step = pl.program_id(0)

    @pl.when(step == 0)
    def _():
        gain_term[...] = jnp.zeros_like(gain_term)
        padded_heads(wout_pad, wout_ref)
        padded_heads(w_pad, w_ref)

    @pl.when(step < IMG)
    def _():
        first = words_ref[0] == 0
        own = own_ref[...].reshape(64, WIDTH)
        other = other_ref[...].reshape(64, WIDTH)
        upstream = jnp.concatenate(
            [jnp.where(first, own, other), jnp.where(first, other, own)], axis=0
        )
        upstream_ref[...] = upstream
        mixed_grads = dot(upstream, wout_pad[...], 1, 1).astype(BF)
        pieces = []
        for head in range(2):
            query, key, value = (
                packed_ref[:, (head * 3 + i) * LANE : (head * 3 + i + 1) * LANE]
                for i in range(3)
            )
            probability = prob_ref[0, head]
            mixed_grad = mixed_grads[:, head * LANE : (head + 1) * LANE]
            prob_grad = dot(mixed_grad, value, 1, 1)
            inner = jnp.sum(probability * prob_grad, axis=-1, keepdims=True)
            score_grad = (probability * (prob_grad - inner) * SCALING).astype(BF)
            pieces.append(dot(score_grad, key, 1, 0))
            pieces.append(dot(score_grad, query, 0, 0))
            pieces.append(dot(probability.astype(BF), mixed_grad, 0, 0))
        packed_grad_ref[...] = shifted_sum(pieces, 512)[:, :480].astype(BF)
        wide = jnp.concatenate([piece.astype(BF) for piece in pieces], axis=1)
        in_part = dot(wide, w_pad[...], 1, 0).astype(BF)
        gain_term[...] += jnp.sum(
            in_part.astype(F32) * normed_ref[...].astype(F32), axis=0, keepdims=True
        )
        low, high = in_part[:64], in_part[64:]
        in_own_ref[...] = jnp.where(first, low, high).reshape(4, 1, 16, WIDTH)
        in_other_ref[...] = jnp.where(first, high, low).reshape(4, 1, 16, WIDTH)

    @pl.when(step == IMG)
    def _():
        row = lax.broadcasted_iota(jnp.int32, (16, WIDTH), 0)
        plane = jnp.where(row == 0, gain_term[...], 0.0).astype(BF)
        for peer in range(4):
            in_own_ref[peer, 0] = plane
            in_other_ref[peer, 0] = plane


def backward(words, own, other, w_out, w_heads, packed, prob, normed):
    def image(i):
        return jnp.minimum(i, IMG - 1)

    quarter = pl.BlockSpec((4, 1, 16, WIDTH), lambda i: (0, image(i), 0, 0))
    plane = pl.BlockSpec((4, 1, 16, WIDTH), lambda i: (0, i, 0, 0))
    rows = pl.BlockSpec((TILE, WIDTH), lambda i: (image(i), 0))
    return pl.pallas_call(
        backward_kernel,
        grid=(IMG + 1,),
        out_shape=(
            jax.ShapeDtypeStruct((ROWS, WIDTH), BF),
            jax.ShapeDtypeStruct((ROWS, 6 * HEAD), BF),
            jax.ShapeDtypeStruct((4, IMG + 1, 16, WIDTH), BF),
            jax.ShapeDtypeStruct((4, IMG + 1, 16, WIDTH), BF),
        ),
        in_specs=[
            smem(),
            quarter,
            quarter,
            pl.BlockSpec((2 * HEAD, WIDTH), lambda i: (0, 0)),
            pl.BlockSpec((6 * HEAD, WIDTH), lambda i: (0, 0)),
            pl.BlockSpec((TILE, 6 * LANE), lambda i: (image(i), 0)),
            pl.BlockSpec((1, 2, TILE, TILE), lambda i: (image(i), 0, 0, 0)),
            rows,
        ],
        out_specs=(
            rows,
            pl.BlockSpec((TILE, 6 * HEAD), lambda i: (image(i), 0)),
            plane,
            plane,
        ),
        scratch_shapes=[
            pltpu.VMEM((1, WIDTH), F32),
            pltpu.VMEM((6 * LANE, WIDTH), BF),
            pltpu.VMEM((2 * LANE, WIDTH), BF),
        ],
        cost_estimate=pl.CostEstimate(
            flops=10_000_000_000, bytes_accessed=10_000_000, transcendentals=0
        ),
        name="backward",
    )(words, own, other, w_out, w_heads, packed, prob, normed)


def weights_kernel(
    words_ref, normed_ref, upstream_ref, packed_grad_ref, mixed_ref, *out_refs_and_scratch
):
    *out_refs, scratch = out_refs_and_scratch
    qkv = dot(normed_ref[...], packed_grad_ref[...], 0, 0)
    out = dot(upstream_ref[...], mixed_ref[...], 0, 0)
    term = jnp.concatenate([qkv, out], axis=1)
    for at in range(16):
        scratch[at] = term[at * 40 : (at + 1) * 40].astype(BF)
    for by, out_ref in enumerate(out_refs):
        near = lax.rem(words_ref[3] + by, 4)
        for far in range(4):
            out_ref[far] = scratch[far * 4 + near]


def weight_terms(words, normed, upstream, packed_grad, mixed):
    return pl.pallas_call(
        weights_kernel,
        grid=(2,),
        out_shape=(jax.ShapeDtypeStruct((8, 40, 640), BF),) * 4,
        in_specs=[
            smem(),
            pl.BlockSpec((ROWS, 640), lambda i: (0, i)),
            pl.BlockSpec((ROWS, 640), lambda i: (0, i)),
            pl.BlockSpec((ROWS, 6 * HEAD), lambda i: (0, 0)),
            pl.BlockSpec((ROWS, 2 * HEAD), lambda i: (0, 0)),
        ],
        out_specs=(pl.BlockSpec((4, 40, 640), lambda i: (i, 0, 0)),) * 4,
        scratch_shapes=[pltpu.VMEM((16, 40, 640), BF)],
        cost_estimate=pl.CostEstimate(
            flops=4_000_000_000, bytes_accessed=6_000_000, transcendentals=0
        ),
        name="weight_terms",
    )(words, normed, upstream, packed_grad, mixed)


def norm_back_kernel(arrived_ref, block_ref, upstream_ref, gain_ref, out_ref, term_ref):
    gain = gain_ref[...]
    results = []
    for image in range(IMG + 1):
        incoming = arrived_ref[0, image].astype(F32)
        for peer in range(1, 4):
            incoming = incoming + arrived_ref[peer, image].astype(F32)
        if image == IMG:
            term_ref[...] = incoming[:8]
            continue
        normed, inverse = normalize(block_ref[image].astype(F32))
        scaled = incoming * gain
        inner = jnp.mean(scaled * normed, axis=-1, keepdims=True)
        outgoing = inverse * (scaled - jnp.mean(scaled, axis=-1, keepdims=True) - normed * inner)
        results.append(upstream_ref[image].astype(F32) + outgoing)
    grads = jnp.concatenate(results, axis=0)
    for share in range(8):
        start = share * 160 // LANE * LANE
        offset = share * 160 - start
        lanes = min(256 if offset + 160 <= 256 else 384, WIDTH - start)
        window = grads[:, start : start + lanes]
        if offset:
            window = pltpu.roll(window, lanes - offset, 1)
        out_ref[share] = window[:, :160].astype(BF)


def norm_back(arrived, block_rows, upstream_rows, gain):
    return pl.pallas_call(
        norm_back_kernel,
        out_shape=(
            jax.ShapeDtypeStruct((8, 80, 160), BF),
            jax.ShapeDtypeStruct((8, WIDTH), F32),
        ),
        in_specs=[pl.BlockSpec(memory_space=pltpu.VMEM)] * 4,
        out_specs=(pl.BlockSpec(memory_space=pltpu.VMEM),) * 2,
        name="norm_back",
    )(arrived, block_rows, upstream_rows, gain)


def summed(blocks):
    return blocks.astype(F32).sum(axis=0)


def after(value, *earlier):
    return lax.optimization_barrier((value, *earlier))[0]


def rows_along(term, columns):
    blocks = term.reshape(8, 4, -1, columns)
    here = lax.axis_index("x")
    return [
        lax.dynamic_index_in_dim(blocks, lax.rem(here + at, 4), 1, keepdims=False)
        for at in range(4)
    ]


def near_sum(parts):
    got = [shifted(parts[at], "x", at) for at in (2, 1, 3)]
    total = parts[0].astype(F32)
    for rows in got:
        total = total + rows.astype(F32)
    return total.astype(BF)


def shards(grad_rows, features, block_in, patch_counts, owner, ln1_gain, w_qkv, w_out, w_proj):
    device = lax.axis_index(ENC)
    core = lax.axis_index("c")
    place = core * 4 + lax.axis_index("y")
    words = jnp.stack([core, place, lax.axis_index("y"), lax.axis_index("x")]).astype(jnp.int32)
    place_word = place.reshape(1).astype(jnp.int32)
    gain = ln1_gain.reshape(1, WIDTH)
    columns = grad_rows.shape[1]

    own_counts = lax.dynamic_index_in_dim(patch_counts, device, 0, keepdims=False)
    images = jnp.arange(PEERS * IMG, dtype=jnp.int32)
    block_of = images // IMG
    owners = owner.reshape(-1)
    ahead = (owners[:, None] == owners[None, :]) & (block_of[None, :] < block_of[:, None])
    target = owners * IMG + jnp.sum(ahead.astype(jnp.int32), axis=1)
    hits = target[None, :] == images[:, None]
    source_of = jnp.sum(jnp.where(hits, images[None, :], 0), axis=1)
    all_counts = jnp.sum(jnp.where(hits, patch_counts.reshape(1, -1), 0), axis=1)
    arrived_counts = lax.dynamic_slice_in_dim(all_counts, device * IMG, IMG, 0)

    by_place = grad_rows.reshape(IMG, 2, 4, 16, -1).transpose(1, 2, 0, 3, 4)
    by_place = by_place.reshape(2, ROWS // 2, -1)
    for_other = lax.dynamic_index_in_dim(by_place, 1 - core, 0, keepdims=False)
    for_own = lax.dynamic_index_in_dim(by_place, core, 0, keepdims=False)
    part_other = dot(for_other, w_proj, 1, 1).astype(BF)
    from_other = swapped(part_other)
    part_own = dot(for_own, w_proj, 1, 1)
    pair = (part_own + from_other.astype(F32)).astype(BF)
    features = after(features, pair)
    arrived = exchanged(pair.reshape(4, 80, WIDTH), "y").reshape(4, IMG, 16, WIDTH)

    line = jnp.arange(TILE, dtype=jnp.int32)
    live_own = (line[None, :] < own_counts[:, None]).reshape(-1)
    kept_rows = jnp.where(live_own[:, None], features, jnp.zeros_like(features))
    proj_term = dot(kept_rows, grad_rows, 0, 0).astype(BF)
    arrived = after(arrived, proj_term)
    pieces = spread(place_word, own_counts, arrived)
    proj_near = near_sum(rows_along(proj_term, columns))

    share = after(block_in.T, arrived)
    shares = [share] + [shifted(share, "y", at) for at in (1, 2, 3)]
    block_own = jnp.stack(shares)
    block_other = swapped(block_own)

    w_heads = w_qkv.transpose(1, 2, 0).reshape(6 * HEAD, WIDTH)
    normed_in, normed, block_rows, packed, prob, mixed = attention(
        words, arrived_counts, block_own, block_other, gain, w_heads
    )

    passing = exchanged(pieces, ENC)
    passing = forwarded(source_of, passing)
    landed = exchanged(passing, ENC)
    upstream_rows, copies = collected(landed)
    half_own = exchanged(copies.reshape(4, 80, WIDTH), "y").reshape(4, IMG, 16, WIDTH)
    half_other = swapped(half_own)

    proj_far = exchanged(after(proj_near, half_own), "z")

    upstream, packed_grad, in_own, in_other = backward(
        words, half_own, half_other, w_out, w_heads, packed, prob, normed
    )
    in_got = swapped(in_other)
    terms = weight_terms(words, normed_in, upstream, packed_grad, mixed)
    in_pair = (in_own.astype(F32) + in_got.astype(F32)).astype(BF)
    in_pair, proj_far = lax.optimization_barrier((in_pair, proj_far))
    grad_proj = summed(proj_far)
    in_arrived = exchanged(in_pair.reshape(4, 96, WIDTH), "y").reshape(4, IMG + 1, 16, WIDTH)
    term_near = near_sum(terms)
    shares, gain_term = norm_back(in_arrived, block_rows, upstream_rows, gain)
    shares = exchanged(shares, TP)
    grad_input = shares.reshape(4, 2, IMG, 16, 160).transpose(2, 1, 0, 3, 4)
    grad_input = grad_input.reshape(ROWS, 160)
    last = summed(exchanged(term_near, "z"))
    gain_rows = gain_term[0].astype(BF).reshape(8, 4, 40).transpose(1, 0, 2)
    gain_rows = gain_rows.reshape(4, 1, 320)
    here = lax.axis_index("x")

    def gain_of(at):
        return lax.dynamic_index_in_dim(gain_rows, lax.rem(here + at, 4), 0, keepdims=False)

    gain_sum = gain_of(0).astype(F32)
    for at in (2, 1, 3):
        gain_sum = gain_sum + shifted(gain_of(at), "x", at).astype(F32)
    gain_sum = gain_sum.reshape(8, 40)
    far = lax.axis_index("z")
    for reach in (4, 2, 1):
        upper = (far // reach) % 2 == 1
        low, high = gain_sum[:reach], gain_sum[reach:]
        sent = jnp.where(upper, low, high).astype(BF)
        got = lax.ppermute(sent, "z", tuple((i, i ^ reach) for i in range(8)))
        gain_sum = jnp.where(upper, high, low) + got.astype(F32)
    grad_qkv = last[:, :480].reshape(40, 2, 240)
    grad_out = last[:, 480:].T
    grad_ln1 = gain_sum.reshape(40)
    return (grad_input, grad_proj, grad_qkv, grad_out, grad_ln1)


def solution(mesh):
    torus = Mesh(mesh.devices.reshape(8, 4, 4, 2), ("z", "x", "y", "c"))

    return jax.shard_map(
        shards,
        mesh=torus,
        in_specs=(
            P(ENC, TP),
            P(ENC, None),
            P(ENC, TP),
            P(),
            P(),
            P(),
            P(None, TP, None),
            P(TP, None),
            P(None, TP),
        ),
        out_specs=(P(ENC, TP), P(ENC, TP), P(ENC, TP, None), P(TP, ENC), P(ENC)),
        check_vma=False,
    )
```

```python
import jax
import jax.numpy as jnp
from jax import lax
from jax.experimental import pallas as pl
from jax.experimental.pallas import tpu as pltpu
from jax.sharding import Mesh
from jax.sharding import PartitionSpec as P


TILE = 128
IMG = 5
ROWS = IMG * TILE
WIDTH = 1280
HEAD = 80
LANE = 128
PEERS = 32
ENC = ("z", "x")
TP = ("y", "c")
EPSILON = 1e-05
SCALING = 1.0 / HEAD**0.5
BF = jnp.bfloat16
F32 = jnp.float32
SWAP = ((0, 1), (1, 0))


def padded_heads(padded_ref, heads_ref):
    for at in range(heads_ref.shape[0] // HEAD):
        padded_ref[at * LANE : at * LANE + HEAD] = heads_ref[at * HEAD : (at + 1) * HEAD]
        padded_ref[at * LANE + HEAD : (at + 1) * LANE] = jnp.zeros((LANE - HEAD, WIDTH), BF)


def exchanged(blocks, axis):
    return lax.all_to_all(blocks, axis, split_axis=0, concat_axis=0, tiled=True)


def shifted(values, axis, by):
    pairs = tuple((i, (i + by) % 4) for i in range(4))
    return lax.ppermute(values, axis, pairs)


def swapped(values):
    return lax.ppermute(values, "c", SWAP)


def dot(left, right, dim_left, dim_right):
    return lax.dot_general(
        left, right, (((dim_left,), (dim_right,)), ((), ())), preferred_element_type=F32
    )


def smem():
    return pl.BlockSpec(memory_space=pltpu.SMEM)


def normalize(values):
    centred = values - jnp.mean(values, axis=-1, keepdims=True)
    variance = jnp.mean(centred * centred, axis=-1, keepdims=True)
    inverse = lax.rsqrt(variance + EPSILON)
    return (centred * inverse, inverse)


def shifted_sum(pieces, lanes):
    total = None
    for at, piece in enumerate(pieces):
        wide = jnp.concatenate(
            [piece, jnp.zeros((piece.shape[0], lanes - LANE), piece.dtype)], axis=1
        )
        if at:
            wide = pltpu.roll(wide, HEAD * at, 1)
        total = wide if total is None else total + wide
    return total


def half_rows(rows_ref):
    return jnp.concatenate(
        [rows_ref[image, 0, near] for near in range(4) for image in range(IMG)], axis=0
    )


def part_kernel(half_ref, rows_ref, w_ref, out_ref):
    out_ref[...] = dot(half_rows(rows_ref), w_ref[...], 1, 1).astype(BF)


def pair_kernel(half_ref, rows_ref, w_ref, got_ref, out_ref):
    own = dot(half_rows(rows_ref), w_ref[...], 1, 1)
    out_ref[...] = (own + got_ref[...].astype(F32)).astype(BF)


def projected(half, grad_rows, w_proj, got=None):
    depth = grad_rows.shape[1]
    rows = grad_rows.reshape(IMG, 2, 4, 16, depth)
    block = pl.BlockSpec((ROWS // 2, 256), lambda i, half: (0, i))
    kernel, extra = (part_kernel, ()) if got is None else (pair_kernel, (got,))
    return pl.pallas_call(
        kernel,
        grid_spec=pltpu.PrefetchScalarGridSpec(
            num_scalar_prefetch=1,
            grid=(WIDTH // 256,),
            in_specs=[
                pl.BlockSpec((IMG, 1, 4, 16, depth), lambda i, half: (0, half[0], 0, 0, 0)),
                pl.BlockSpec((256, depth), lambda i, half: (i, 0)),
                *(block for _ in extra),
            ],
            out_specs=block,
        ),
        out_shape=jax.ShapeDtypeStruct((ROWS // 2, WIDTH), BF),
        cost_estimate=pl.CostEstimate(
            flops=1_000_000_000, bytes_accessed=4_000_000, transcendentals=0
        ),
        name="projected",
    )(half, rows, w_proj, *extra)


def spread_kernel(place_ref, counts_ref, arrived_ref, out_ref):
    first_row = place_ref[0] * 16
    for image in range(IMG):
        rows = arrived_ref[0, image].astype(F32)
        for peer in range(1, 4):
            rows = rows + arrived_ref[peer, image].astype(F32)
        line = first_row + lax.broadcasted_iota(jnp.int32, rows.shape, 0)
        rows = jnp.where(line < counts_ref[image], rows, 0.0).astype(BF)
        for half in range(2):
            for group in range(10):
                out_ref[half * 10 + group, image] = rows[
                    half * 8 : half * 8 + 8, group * LANE : (group + 1) * LANE
                ]
    out_ref[20:32] = jnp.zeros((12, IMG, 8, LANE), BF)


def spread(place, counts, arrived):
    return pl.pallas_call(
        spread_kernel,
        out_shape=jax.ShapeDtypeStruct((PEERS, IMG, 8, LANE), BF),
        in_specs=[smem(), smem(), pl.BlockSpec(memory_space=pltpu.VMEM)],
        out_specs=pl.BlockSpec(memory_space=pltpu.VMEM),
        name="spread",
    )(place, counts, arrived)


def forward_kernel(index_ref, pieces_ref, out_ref):
    def step(at, carry):
        out_ref[at] = pieces_ref[index_ref[at]]
        return carry

    lax.fori_loop(0, PEERS * IMG, step, 0, unroll=8)


def forwarded(index, pieces):
    flat = pieces.reshape(PEERS * IMG, 8, LANE)
    return pl.pallas_call(
        forward_kernel,
        out_shape=jax.ShapeDtypeStruct(flat.shape, BF),
        in_specs=[smem(), pl.BlockSpec(memory_space=pltpu.VMEM)],
        out_specs=pl.BlockSpec(memory_space=pltpu.VMEM),
        name="forwarded",
    )(index, flat).reshape(pieces.shape)


def collect_kernel(pieces_ref, rows_ref, copies_ref):
    for image in range(IMG):
        for half in range(2):
            for group in range(10):
                piece = pieces_ref[half * 10 + group, image]
                at = (slice(half * 8, half * 8 + 8), slice(group * LANE, (group + 1) * LANE))
                rows_ref[image, at[0], at[1]] = piece
                for peer in range(4):
                    copies_ref[peer, image, at[0], at[1]] = piece


def collected(pieces):
    return pl.pallas_call(
        collect_kernel,
        out_shape=(
            jax.ShapeDtypeStruct((IMG, 16, WIDTH), BF),
            jax.ShapeDtypeStruct((4, IMG, 16, WIDTH), BF),
        ),
        in_specs=[pl.BlockSpec(memory_space=pltpu.VMEM)],
        out_specs=(pl.BlockSpec(memory_space=pltpu.VMEM),) * 2,
        name="collected",
    )(pieces)


def attention_kernel(
    words_ref,
    counts_ref,
    own_ref,
    other_ref,
    gain_ref,
    w_ref,
    normed_in_ref,
    normed_ref,
    rows_ref,
    packed_ref,
    prob_ref,
    mixed_ref,
    scratch,
    w_pad,
):
    @pl.when(pl.program_id(0) == 0)
    def _():
        padded_heads(w_pad, w_ref)

    first = words_ref[0] == 0
    shares = []
    for near in range(4):
        at = lax.rem(words_ref[2] + 4 - near, 4)
        own, other = own_ref[at], other_ref[at]
        shares += [jnp.where(first, own, other), jnp.where(first, other, own)]
    values = jnp.concatenate(shares, axis=0).astype(F32).T
    scratch[...] = values
    rows_ref[0] = scratch[pl.ds(pl.multiple_of(words_ref[1] * 16, 16), 16), :].astype(BF)
    normed, _ = normalize(values)
    normed_ref[...] = normed.astype(BF)
    normed_in = (normed * gain_ref[...]).astype(BF)
    normed_in_ref[...] = normed_in
    packed = dot(normed_in, w_pad[...], 1, 1).astype(BF)
    packed_ref[...] = packed
    count = counts_ref[pl.program_id(0)]
    live_row = lax.broadcasted_iota(jnp.int32, (TILE, TILE), 0) < count
    live_col = lax.broadcasted_iota(jnp.int32, (TILE, TILE), 1) < count
    same_kind = (live_row & live_col) | (~live_row & ~live_col)
    mixed = []
    for head in range(2):
        query, key, value = (
            packed[:, (head * 3 + i) * LANE : (head * 3 + i + 1) * LANE] for i in range(3)
        )
        scores = jnp.where(same_kind, dot(query, key, 1, 1) * SCALING, -1e30)
        exp_terms = jnp.exp(scores - jnp.max(scores, axis=-1, keepdims=True))
        probability = exp_terms / jnp.sum(exp_terms, axis=-1, keepdims=True)
        prob_ref[0, head] = probability
        mixed.append(dot(probability.astype(BF), value, 1, 0))
    mixed_ref[...] = shifted_sum(mixed, 256)[:, :160].astype(BF)


def attention(words, counts, own, other, gain, w_heads):
    share = pl.BlockSpec((4, 160, TILE), lambda i: (0, 0, i))
    rows = pl.BlockSpec((TILE, WIDTH), lambda i: (i, 0))
    return pl.pallas_call(
        attention_kernel,
        grid=(IMG,),
        out_shape=(
            jax.ShapeDtypeStruct((ROWS, WIDTH), BF),
            jax.ShapeDtypeStruct((ROWS, WIDTH), BF),
            jax.ShapeDtypeStruct((IMG, 16, WIDTH), BF),
            jax.ShapeDtypeStruct((ROWS, 6 * LANE), BF),
            jax.ShapeDtypeStruct((IMG, 2, TILE, TILE), F32),
            jax.ShapeDtypeStruct((ROWS, 2 * HEAD), BF),
        ),
        in_specs=[
            smem(),
            smem(),
            share,
            share,
            pl.BlockSpec((1, WIDTH), lambda i: (0, 0)),
            pl.BlockSpec((6 * HEAD, WIDTH), lambda i: (0, 0)),
        ],
        out_specs=(
            rows,
            rows,
            pl.BlockSpec((1, 16, WIDTH), lambda i: (i, 0, 0)),
            pl.BlockSpec((TILE, 6 * LANE), lambda i: (i, 0)),
            pl.BlockSpec((1, 2, TILE, TILE), lambda i: (i, 0, 0, 0)),
            pl.BlockSpec((TILE, 2 * HEAD), lambda i: (i, 0)),
        ),
        scratch_shapes=[pltpu.VMEM((TILE, WIDTH), F32), pltpu.VMEM((6 * LANE, WIDTH), BF)],
        cost_estimate=pl.CostEstimate(
            flops=10_000_000_000, bytes_accessed=10_000_000, transcendentals=0
        ),
        name="attention",
    )(words, counts, own, other, gain, w_heads)


def backward_kernel(
    words_ref,
    own_ref,
    other_ref,
    wout_ref,
    w_ref,
    packed_ref,
    prob_ref,
    normed_ref,
    upstream_ref,
    packed_grad_ref,
    in_own_ref,
    in_other_ref,
    gain_term,
    w_pad,
    wout_pad,
):
    step = pl.program_id(0)

    @pl.when(step == 0)
    def _():
        gain_term[...] = jnp.zeros_like(gain_term)
        padded_heads(wout_pad, wout_ref)
        padded_heads(w_pad, w_ref)

    @pl.when(step < IMG)
    def _():
        first = words_ref[0] == 0
        own = own_ref[...].reshape(64, WIDTH)
        other = other_ref[...].reshape(64, WIDTH)
        upstream = jnp.concatenate(
            [jnp.where(first, own, other), jnp.where(first, other, own)], axis=0
        )
        upstream_ref[...] = upstream
        mixed_grads = dot(upstream, wout_pad[...], 1, 1).astype(BF)
        pieces = []
        for head in range(2):
            query, key, value = (
                packed_ref[:, (head * 3 + i) * LANE : (head * 3 + i + 1) * LANE]
                for i in range(3)
            )
            probability = prob_ref[0, head]
            mixed_grad = mixed_grads[:, head * LANE : (head + 1) * LANE]
            prob_grad = dot(mixed_grad, value, 1, 1)
            inner = jnp.sum(probability * prob_grad, axis=-1, keepdims=True)
            score_grad = (probability * (prob_grad - inner) * SCALING).astype(BF)
            pieces.append(dot(score_grad, key, 1, 0))
            pieces.append(dot(score_grad, query, 0, 0))
            pieces.append(dot(probability.astype(BF), mixed_grad, 0, 0))
        packed_grad_ref[...] = shifted_sum(pieces, 512)[:, :480].astype(BF)
        wide = jnp.concatenate([piece.astype(BF) for piece in pieces], axis=1)
        in_part = dot(wide, w_pad[...], 1, 0).astype(BF)
        gain_term[...] += jnp.sum(
            in_part.astype(F32) * normed_ref[...].astype(F32), axis=0, keepdims=True
        )
        low, high = in_part[:64], in_part[64:]
        in_own_ref[...] = jnp.where(first, low, high).reshape(4, 1, 16, WIDTH)
        in_other_ref[...] = jnp.where(first, high, low).reshape(4, 1, 16, WIDTH)

    @pl.when(step == IMG)
    def _():
        row = lax.broadcasted_iota(jnp.int32, (16, WIDTH), 0)
        plane = jnp.where(row == 0, gain_term[...], 0.0).astype(BF)
        for peer in range(4):
            in_own_ref[peer, 0] = plane
            in_other_ref[peer, 0] = plane


def backward(words, own, other, w_out, w_heads, packed, prob, normed):
    def image(i):
        return jnp.minimum(i, IMG - 1)

    quarter = pl.BlockSpec((4, 1, 16, WIDTH), lambda i: (0, image(i), 0, 0))
    plane = pl.BlockSpec((4, 1, 16, WIDTH), lambda i: (0, i, 0, 0))
    rows = pl.BlockSpec((TILE, WIDTH), lambda i: (image(i), 0))
    return pl.pallas_call(
        backward_kernel,
        grid=(IMG + 1,),
        out_shape=(
            jax.ShapeDtypeStruct((ROWS, WIDTH), BF),
            jax.ShapeDtypeStruct((ROWS, 6 * HEAD), BF),
            jax.ShapeDtypeStruct((4, IMG + 1, 16, WIDTH), BF),
            jax.ShapeDtypeStruct((4, IMG + 1, 16, WIDTH), BF),
        ),
        in_specs=[
            smem(),
            quarter,
            quarter,
            pl.BlockSpec((2 * HEAD, WIDTH), lambda i: (0, 0)),
            pl.BlockSpec((6 * HEAD, WIDTH), lambda i: (0, 0)),
            pl.BlockSpec((TILE, 6 * LANE), lambda i: (image(i), 0)),
            pl.BlockSpec((1, 2, TILE, TILE), lambda i: (image(i), 0, 0, 0)),
            rows,
        ],
        out_specs=(
            rows,
            pl.BlockSpec((TILE, 6 * HEAD), lambda i: (image(i), 0)),
            plane,
            plane,
        ),
        scratch_shapes=[
            pltpu.VMEM((1, WIDTH), F32),
            pltpu.VMEM((6 * LANE, WIDTH), BF),
            pltpu.VMEM((2 * LANE, WIDTH), BF),
        ],
        cost_estimate=pl.CostEstimate(
            flops=10_000_000_000, bytes_accessed=10_000_000, transcendentals=0
        ),
        name="backward",
    )(words, own, other, w_out, w_heads, packed, prob, normed)


def weights_kernel(
    words_ref, normed_ref, upstream_ref, packed_grad_ref, mixed_ref, *out_refs_and_scratch
):
    *out_refs, scratch = out_refs_and_scratch
    qkv = dot(normed_ref[...], packed_grad_ref[...], 0, 0)
    out = dot(upstream_ref[...], mixed_ref[...], 0, 0)
    term = jnp.concatenate([qkv, out], axis=1)
    for at in range(16):
        scratch[at] = term[at * 40 : (at + 1) * 40].astype(BF)
    for by, out_ref in enumerate(out_refs):
        near = lax.rem(words_ref[3] + by, 4)
        for far in range(4):
            out_ref[far] = scratch[far * 4 + near]


def weight_terms(words, normed, upstream, packed_grad, mixed):
    return pl.pallas_call(
        weights_kernel,
        grid=(2,),
        out_shape=(jax.ShapeDtypeStruct((8, 40, 640), BF),) * 4,
        in_specs=[
            smem(),
            pl.BlockSpec((ROWS, 640), lambda i: (0, i)),
            pl.BlockSpec((ROWS, 640), lambda i: (0, i)),
            pl.BlockSpec((ROWS, 6 * HEAD), lambda i: (0, 0)),
            pl.BlockSpec((ROWS, 2 * HEAD), lambda i: (0, 0)),
        ],
        out_specs=(pl.BlockSpec((4, 40, 640), lambda i: (i, 0, 0)),) * 4,
        scratch_shapes=[pltpu.VMEM((16, 40, 640), BF)],
        cost_estimate=pl.CostEstimate(
            flops=4_000_000_000, bytes_accessed=6_000_000, transcendentals=0
        ),
        name="weight_terms",
    )(words, normed, upstream, packed_grad, mixed)


def norm_back_kernel(arrived_ref, block_ref, upstream_ref, gain_ref, out_ref, term_ref):
    gain = gain_ref[...]
    results = []
    for image in range(IMG + 1):
        rows = slice(image * 16, image * 16 + 16)
        incoming = arrived_ref[0, rows].astype(F32)
        for peer in range(1, 4):
            incoming = incoming + arrived_ref[peer, rows].astype(F32)
        if image == IMG:
            term_ref[...] = incoming[:8]
            continue
        normed, inverse = normalize(block_ref[image].astype(F32))
        scaled = incoming * gain
        inner = jnp.mean(scaled * normed, axis=-1, keepdims=True)
        outgoing = inverse * (scaled - jnp.mean(scaled, axis=-1, keepdims=True) - normed * inner)
        results.append(upstream_ref[image].astype(F32) + outgoing)
    grads = jnp.concatenate(results, axis=0)
    for share in range(8):
        start = share * 160 // LANE * LANE
        offset = share * 160 - start
        lanes = min(256 if offset + 160 <= 256 else 384, WIDTH - start)
        window = grads[:, start : start + lanes]
        if offset:
            window = pltpu.roll(window, lanes - offset, 1)
        out_ref[share] = window[:, :160].astype(BF)


def norm_back(arrived, block_rows, upstream_rows, gain):
    return pl.pallas_call(
        norm_back_kernel,
        out_shape=(
            jax.ShapeDtypeStruct((8, 80, 160), BF),
            jax.ShapeDtypeStruct((8, WIDTH), F32),
        ),
        in_specs=[pl.BlockSpec(memory_space=pltpu.VMEM)] * 4,
        out_specs=(pl.BlockSpec(memory_space=pltpu.VMEM),) * 2,
        name="norm_back",
    )(arrived, block_rows, upstream_rows, gain)


def summed(blocks):
    return blocks.astype(F32).sum(axis=0)


def after(value, *earlier):
    return lax.optimization_barrier((value, *earlier))[0]


def rows_along(term, columns):
    blocks = term.reshape(8, 4, -1, columns)
    here = lax.axis_index("x")
    return [
        lax.dynamic_index_in_dim(blocks, lax.rem(here + at, 4), 1, keepdims=False)
        for at in range(4)
    ]


def near_sum(parts):
    got = [shifted(parts[at], "x", at) for at in (2, 1, 3)]
    total = parts[0].astype(F32)
    for rows in got:
        total = total + rows.astype(F32)
    return total.astype(BF)


def shards(grad_rows, features, block_in, patch_counts, owner, ln1_gain, w_qkv, w_out, w_proj):
    device = lax.axis_index(ENC)
    core = lax.axis_index("c")
    place = core * 4 + lax.axis_index("y")
    words = jnp.stack([core, place, lax.axis_index("y"), lax.axis_index("x")]).astype(jnp.int32)
    place_word = place.reshape(1).astype(jnp.int32)
    gain = ln1_gain.reshape(1, WIDTH)
    columns = grad_rows.shape[1]

    own_counts = lax.dynamic_index_in_dim(patch_counts, device, 0, keepdims=False)
    images = jnp.arange(PEERS * IMG, dtype=jnp.int32)
    block_of = images // IMG
    owners = owner.reshape(-1)
    ahead = (owners[:, None] == owners[None, :]) & (block_of[None, :] < block_of[:, None])
    target = owners * IMG + jnp.sum(ahead.astype(jnp.int32), axis=1)
    hits = target[None, :] == images[:, None]
    source_of = jnp.sum(jnp.where(hits, images[None, :], 0), axis=1)
    all_counts = jnp.sum(jnp.where(hits, patch_counts.reshape(1, -1), 0), axis=1)
    arrived_counts = lax.dynamic_slice_in_dim(all_counts, device * IMG, IMG, 0)

    own_half = core.reshape(1).astype(jnp.int32)
    part_other = projected(1 - own_half, grad_rows, w_proj)
    pair = projected(own_half, grad_rows, w_proj, swapped(part_other))
    features = after(features, pair)
    arrived = exchanged(pair.reshape(4, 80, WIDTH), "y").reshape(4, IMG, 16, WIDTH)

    line = jnp.arange(TILE, dtype=jnp.int32)
    live_own = (line[None, :] < own_counts[:, None]).reshape(-1)
    kept_rows = jnp.where(live_own[:, None], features, jnp.zeros_like(features))
    proj_term = dot(kept_rows, grad_rows, 0, 0).astype(BF)
    arrived = after(arrived, proj_term)
    pieces = spread(place_word, own_counts, arrived)
    proj_near = near_sum(rows_along(proj_term, columns))

    share = after(block_in.T, arrived)
    shares = [share] + [shifted(share, "y", at) for at in (1, 2, 3)]
    block_own = jnp.stack(shares)
    block_other = swapped(block_own)

    w_heads = w_qkv.transpose(1, 2, 0).reshape(6 * HEAD, WIDTH)
    normed_in, normed, block_rows, packed, prob, mixed = attention(
        words, arrived_counts, block_own, block_other, gain, w_heads
    )

    passing = exchanged(pieces, ENC)
    passing = forwarded(source_of, passing)
    landed = exchanged(passing, ENC)
    upstream_rows, copies = collected(landed)
    half_own = exchanged(copies.reshape(4, 80, WIDTH), "y").reshape(4, IMG, 16, WIDTH)
    half_other = swapped(half_own)

    proj_far = exchanged(after(proj_near, half_own), "z")

    upstream, packed_grad, in_own, in_other = backward(
        words, half_own, half_other, w_out, w_heads, packed, prob, normed
    )
    in_got = swapped(in_other)
    terms = weight_terms(words, normed_in, upstream, packed_grad, mixed)
    in_pair = (in_own.astype(F32) + in_got.astype(F32)).astype(BF)
    in_pair = in_pair.reshape(4, 96, WIDTH)
    in_pair, proj_far = lax.optimization_barrier((in_pair, proj_far))
    grad_proj = summed(proj_far)
    in_arrived = exchanged(in_pair, "y")
    term_near = near_sum(terms)
    shares, gain_term = norm_back(in_arrived, block_rows, upstream_rows, gain)
    shares = exchanged(shares, TP)
    grad_input = shares.reshape(4, 2, IMG, 16, 160).transpose(2, 1, 0, 3, 4)
    grad_input = grad_input.reshape(ROWS, 160)
    gain_rows = gain_term[0].astype(BF).reshape(8, 4, 40).transpose(1, 0, 2)
    gain_rows = gain_rows.reshape(4, 1, 320)
    here = lax.axis_index("x")
    gain_parts = [
        lax.dynamic_index_in_dim(gain_rows, lax.rem(here + at, 4), 0, keepdims=False)
        for at in range(4)
    ]
    gain_near = near_sum(gain_parts).reshape(8, 40, 1)
    last = jnp.concatenate([term_near, jnp.pad(gain_near, ((0, 0), (0, 0), (0, 127)))], axis=2)
    last = summed(exchanged(last, "z"))
    grad_qkv = last[:, :480].reshape(40, 2, 240)
    grad_out = last[:, 480:640].T
    grad_ln1 = last[:, 640]
    return (grad_input, grad_proj, grad_qkv, grad_out, grad_ln1)


def solution(mesh):
    torus = Mesh(mesh.devices.reshape(8, 4, 4, 2), ("z", "x", "y", "c"))

    return jax.shard_map(
        shards,
        mesh=torus,
        in_specs=(
            P(ENC, TP),
            P(ENC, None),
            P(ENC, TP),
            P(),
            P(),
            P(),
            P(None, TP, None),
            P(TP, None),
            P(None, TP),
        ),
        out_specs=(P(ENC, TP), P(ENC, TP), P(ENC, TP, None), P(TP, ENC), P(ENC)),
        check_vma=False,
    )
```

```python
import jax
import jax.numpy as jnp
from jax import lax
from jax.experimental import pallas as pl
from jax.experimental.pallas import tpu as pltpu
from jax.sharding import Mesh
from jax.sharding import PartitionSpec as P


TILE = 128
IMG = 5
ROWS = IMG * TILE
WIDTH = 1280
HEAD = 80
LANE = 128
PEERS = 32
ENC = ("z", "x")
TP = ("y", "c")
EPSILON = 1e-05
SCALING = 1.0 / HEAD**0.5
BF = jnp.bfloat16
F32 = jnp.float32
SWAP = ((0, 1), (1, 0))


def padded_heads(padded_ref, heads_ref):
    for at in range(heads_ref.shape[0] // HEAD):
        padded_ref[at * LANE : at * LANE + HEAD] = heads_ref[at * HEAD : (at + 1) * HEAD]
        padded_ref[at * LANE + HEAD : (at + 1) * LANE] = jnp.zeros((LANE - HEAD, WIDTH), BF)


def exchanged(blocks, axis):
    return lax.all_to_all(blocks, axis, split_axis=0, concat_axis=0, tiled=True)


def shifted(values, axis, by):
    pairs = tuple((i, (i + by) % 4) for i in range(4))
    return lax.ppermute(values, axis, pairs)


def swapped(values):
    return lax.ppermute(values, "c", SWAP)


def dot(left, right, dim_left, dim_right):
    return lax.dot_general(
        left, right, (((dim_left,), (dim_right,)), ((), ())), preferred_element_type=F32
    )


def smem():
    return pl.BlockSpec(memory_space=pltpu.SMEM)


def normalize(values):
    centred = values - jnp.mean(values, axis=-1, keepdims=True)
    variance = jnp.mean(centred * centred, axis=-1, keepdims=True)
    inverse = lax.rsqrt(variance + EPSILON)
    return (centred * inverse, inverse)


def shifted_sum(pieces, lanes):
    total = None
    for at, piece in enumerate(pieces):
        wide = jnp.concatenate(
            [piece, jnp.zeros((piece.shape[0], lanes - LANE), piece.dtype)], axis=1
        )
        if at:
            wide = pltpu.roll(wide, HEAD * at, 1)
        total = wide if total is None else total + wide
    return total


def spread_kernel(place_ref, counts_ref, arrived_ref, out_ref):
    first_row = place_ref[0] * 16
    for image in range(IMG):
        rows = arrived_ref[0, image].astype(F32)
        for peer in range(1, 4):
            rows = rows + arrived_ref[peer, image].astype(F32)
        line = first_row + lax.broadcasted_iota(jnp.int32, rows.shape, 0)
        rows = jnp.where(line < counts_ref[image], rows, 0.0).astype(BF)
        for half in range(2):
            for group in range(10):
                out_ref[half * 10 + group, image] = rows[
                    half * 8 : half * 8 + 8, group * LANE : (group + 1) * LANE
                ]
    out_ref[20:32] = jnp.zeros((12, IMG, 8, LANE), BF)


def spread(place, counts, arrived):
    return pl.pallas_call(
        spread_kernel,
        out_shape=jax.ShapeDtypeStruct((PEERS, IMG, 8, LANE), BF),
        in_specs=[smem(), smem(), pl.BlockSpec(memory_space=pltpu.VMEM)],
        out_specs=pl.BlockSpec(memory_space=pltpu.VMEM),
        name="spread",
    )(place, counts, arrived)


def forward_kernel(index_ref, pieces_ref, out_ref):
    def step(at, carry):
        out_ref[at] = pieces_ref[index_ref[at]]
        return carry

    lax.fori_loop(0, PEERS * IMG, step, 0, unroll=8)


def forwarded(index, pieces):
    flat = pieces.reshape(PEERS * IMG, 8, LANE)
    return pl.pallas_call(
        forward_kernel,
        out_shape=jax.ShapeDtypeStruct(flat.shape, BF),
        in_specs=[smem(), pl.BlockSpec(memory_space=pltpu.VMEM)],
        out_specs=pl.BlockSpec(memory_space=pltpu.VMEM),
        name="forwarded",
    )(index, flat).reshape(pieces.shape)


def collect_kernel(pieces_ref, rows_ref, copies_ref):
    for image in range(IMG):
        for half in range(2):
            for group in range(10):
                piece = pieces_ref[half * 10 + group, image]
                at = (slice(half * 8, half * 8 + 8), slice(group * LANE, (group + 1) * LANE))
                rows_ref[image, at[0], at[1]] = piece
                for peer in range(4):
                    copies_ref[peer, image, at[0], at[1]] = piece


def collected(pieces):
    return pl.pallas_call(
        collect_kernel,
        out_shape=(
            jax.ShapeDtypeStruct((IMG, 16, WIDTH), BF),
            jax.ShapeDtypeStruct((4, IMG, 16, WIDTH), BF),
        ),
        in_specs=[pl.BlockSpec(memory_space=pltpu.VMEM)],
        out_specs=(pl.BlockSpec(memory_space=pltpu.VMEM),) * 2,
        name="collected",
    )(pieces)


def attention_kernel(
    words_ref,
    counts_ref,
    own_ref,
    other_ref,
    gain_ref,
    w_ref,
    normed_in_ref,
    normed_ref,
    rows_ref,
    packed_ref,
    prob_ref,
    mixed_ref,
    scratch,
    w_pad,
):
    @pl.when(pl.program_id(0) == 0)
    def _():
        padded_heads(w_pad, w_ref)

    first = words_ref[0] == 0
    shares = []
    for near in range(4):
        at = lax.rem(words_ref[2] + 4 - near, 4)
        own, other = own_ref[at], other_ref[at]
        shares += [jnp.where(first, own, other), jnp.where(first, other, own)]
    values = jnp.concatenate(shares, axis=0).astype(F32).T
    scratch[...] = values
    rows_ref[0] = scratch[pl.ds(pl.multiple_of(words_ref[1] * 16, 16), 16), :].astype(BF)
    normed, _ = normalize(values)
    normed_ref[...] = normed.astype(BF)
    normed_in = (normed * gain_ref[...]).astype(BF)
    normed_in_ref[...] = normed_in
    packed = dot(normed_in, w_pad[...], 1, 1).astype(BF)
    packed_ref[...] = packed
    count = counts_ref[pl.program_id(0)]
    live_row = lax.broadcasted_iota(jnp.int32, (TILE, TILE), 0) < count
    live_col = lax.broadcasted_iota(jnp.int32, (TILE, TILE), 1) < count
    same_kind = (live_row & live_col) | (~live_row & ~live_col)
    mixed = []
    for head in range(2):
        query, key, value = (
            packed[:, (head * 3 + i) * LANE : (head * 3 + i + 1) * LANE] for i in range(3)
        )
        scores = jnp.where(same_kind, dot(query, key, 1, 1) * SCALING, -1e30)
        exp_terms = jnp.exp(scores - jnp.max(scores, axis=-1, keepdims=True))
        probability = exp_terms / jnp.sum(exp_terms, axis=-1, keepdims=True)
        prob_ref[0, head] = probability
        mixed.append(dot(probability.astype(BF), value, 1, 0))
    mixed_ref[...] = shifted_sum(mixed, 256)[:, :160].astype(BF)


def attention(words, counts, own, other, gain, w_heads):
    share = pl.BlockSpec((4, 160, TILE), lambda i: (0, 0, i))
    rows = pl.BlockSpec((TILE, WIDTH), lambda i: (i, 0))
    return pl.pallas_call(
        attention_kernel,
        grid=(IMG,),
        out_shape=(
            jax.ShapeDtypeStruct((ROWS, WIDTH), BF),
            jax.ShapeDtypeStruct((ROWS, WIDTH), BF),
            jax.ShapeDtypeStruct((IMG, 16, WIDTH), BF),
            jax.ShapeDtypeStruct((ROWS, 6 * LANE), BF),
            jax.ShapeDtypeStruct((IMG, 2, TILE, TILE), F32),
            jax.ShapeDtypeStruct((ROWS, 2 * HEAD), BF),
        ),
        in_specs=[
            smem(),
            smem(),
            share,
            share,
            pl.BlockSpec((1, WIDTH), lambda i: (0, 0)),
            pl.BlockSpec((6 * HEAD, WIDTH), lambda i: (0, 0)),
        ],
        out_specs=(
            rows,
            rows,
            pl.BlockSpec((1, 16, WIDTH), lambda i: (i, 0, 0)),
            pl.BlockSpec((TILE, 6 * LANE), lambda i: (i, 0)),
            pl.BlockSpec((1, 2, TILE, TILE), lambda i: (i, 0, 0, 0)),
            pl.BlockSpec((TILE, 2 * HEAD), lambda i: (i, 0)),
        ),
        scratch_shapes=[pltpu.VMEM((TILE, WIDTH), F32), pltpu.VMEM((6 * LANE, WIDTH), BF)],
        cost_estimate=pl.CostEstimate(
            flops=10_000_000_000, bytes_accessed=10_000_000, transcendentals=0
        ),
        name="attention",
    )(words, counts, own, other, gain, w_heads)


def backward_kernel(
    words_ref,
    own_ref,
    other_ref,
    wout_ref,
    w_ref,
    packed_ref,
    prob_ref,
    normed_ref,
    upstream_ref,
    packed_grad_ref,
    in_own_ref,
    in_other_ref,
    gain_term,
    wout_pad,
):
    step = pl.program_id(0)

    @pl.when(step == 0)
    def _():
        gain_term[...] = jnp.zeros_like(gain_term)
        padded_heads(wout_pad, wout_ref)

    @pl.when(step < IMG)
    def _():
        first = words_ref[0] == 0
        own = own_ref[...].reshape(64, WIDTH)
        other = other_ref[...].reshape(64, WIDTH)
        upstream = jnp.concatenate(
            [jnp.where(first, own, other), jnp.where(first, other, own)], axis=0
        )
        upstream_ref[...] = upstream
        mixed_grads = dot(upstream, wout_pad[...], 1, 1).astype(BF)
        pieces = []
        for head in range(2):
            query, key, value = (
                packed_ref[:, (head * 3 + i) * LANE : (head * 3 + i + 1) * LANE]
                for i in range(3)
            )
            probability = prob_ref[0, head]
            mixed_grad = mixed_grads[:, head * LANE : (head + 1) * LANE]
            prob_grad = dot(mixed_grad, value, 1, 1)
            inner = jnp.sum(probability * prob_grad, axis=-1, keepdims=True)
            score_grad = (probability * (prob_grad - inner) * SCALING).astype(BF)
            pieces.append(dot(score_grad, key, 1, 0))
            pieces.append(dot(score_grad, query, 0, 0))
            pieces.append(dot(probability.astype(BF), mixed_grad, 0, 0))
        packed_grad = shifted_sum(pieces, 512)[:, :480].astype(BF)
        packed_grad_ref[...] = packed_grad
        in_part = dot(packed_grad, w_ref[...], 1, 0).astype(BF)
        gain_term[...] += jnp.sum(
            in_part.astype(F32) * normed_ref[...].astype(F32), axis=0, keepdims=True
        )
        low, high = in_part[:64], in_part[64:]
        in_own_ref[...] = jnp.where(first, low, high).reshape(4, 1, 16, WIDTH)
        in_other_ref[...] = jnp.where(first, high, low).reshape(4, 1, 16, WIDTH)

    @pl.when(step == IMG)
    def _():
        row = lax.broadcasted_iota(jnp.int32, (16, WIDTH), 0)
        plane = jnp.where(row == 0, gain_term[...], 0.0).astype(BF)
        for peer in range(4):
            in_own_ref[peer, 0] = plane
            in_other_ref[peer, 0] = plane


def backward(words, own, other, w_out, w_heads, packed, prob, normed):
    def image(i):
        return jnp.minimum(i, IMG - 1)

    quarter = pl.BlockSpec((4, 1, 16, WIDTH), lambda i: (0, image(i), 0, 0))
    plane = pl.BlockSpec((4, 1, 16, WIDTH), lambda i: (0, i, 0, 0))
    rows = pl.BlockSpec((TILE, WIDTH), lambda i: (image(i), 0))
    return pl.pallas_call(
        backward_kernel,
        grid=(IMG + 1,),
        out_shape=(
            jax.ShapeDtypeStruct((ROWS, WIDTH), BF),
            jax.ShapeDtypeStruct((ROWS, 6 * HEAD), BF),
            jax.ShapeDtypeStruct((4, IMG + 1, 16, WIDTH), BF),
            jax.ShapeDtypeStruct((4, IMG + 1, 16, WIDTH), BF),
        ),
        in_specs=[
            smem(),
            quarter,
            quarter,
            pl.BlockSpec((2 * HEAD, WIDTH), lambda i: (0, 0)),
            pl.BlockSpec((6 * HEAD, WIDTH), lambda i: (0, 0)),
            pl.BlockSpec((TILE, 6 * LANE), lambda i: (image(i), 0)),
            pl.BlockSpec((1, 2, TILE, TILE), lambda i: (image(i), 0, 0, 0)),
            rows,
        ],
        out_specs=(
            rows,
            pl.BlockSpec((TILE, 6 * HEAD), lambda i: (image(i), 0)),
            plane,
            plane,
        ),
        scratch_shapes=[
            pltpu.VMEM((1, WIDTH), F32),
            pltpu.VMEM((2 * LANE, WIDTH), BF),
        ],
        cost_estimate=pl.CostEstimate(
            flops=10_000_000_000, bytes_accessed=10_000_000, transcendentals=0
        ),
        name="backward",
    )(words, own, other, w_out, w_heads, packed, prob, normed)


def weights_kernel(
    words_ref, normed_ref, upstream_ref, packed_grad_ref, mixed_ref, *out_refs_and_scratch
):
    *out_refs, scratch = out_refs_and_scratch
    qkv = dot(normed_ref[...], packed_grad_ref[...], 0, 0)
    out = dot(upstream_ref[...], mixed_ref[...], 0, 0)
    term = jnp.concatenate([qkv, out], axis=1)
    for at in range(16):
        scratch[at] = term[at * 40 : (at + 1) * 40].astype(BF)
    for by, out_ref in enumerate(out_refs):
        near = lax.rem(words_ref[3] + by, 4)
        for far in range(4):
            out_ref[far] = scratch[far * 4 + near]


def weight_terms(words, normed, upstream, packed_grad, mixed):
    return pl.pallas_call(
        weights_kernel,
        grid=(2,),
        out_shape=(jax.ShapeDtypeStruct((8, 40, 640), BF),) * 4,
        in_specs=[
            smem(),
            pl.BlockSpec((ROWS, 640), lambda i: (0, i)),
            pl.BlockSpec((ROWS, 640), lambda i: (0, i)),
            pl.BlockSpec((ROWS, 6 * HEAD), lambda i: (0, 0)),
            pl.BlockSpec((ROWS, 2 * HEAD), lambda i: (0, 0)),
        ],
        out_specs=(pl.BlockSpec((4, 40, 640), lambda i: (i, 0, 0)),) * 4,
        scratch_shapes=[pltpu.VMEM((16, 40, 640), BF)],
        cost_estimate=pl.CostEstimate(
            flops=4_000_000_000, bytes_accessed=6_000_000, transcendentals=0
        ),
        name="weight_terms",
    )(words, normed, upstream, packed_grad, mixed)


def norm_back_kernel(arrived_ref, block_ref, upstream_ref, gain_ref, out_ref, term_ref):
    gain = gain_ref[...]
    results = []
    for image in range(IMG + 1):
        rows = slice(image * 16, image * 16 + 16)
        incoming = arrived_ref[0, rows].astype(F32)
        for peer in range(1, 4):
            incoming = incoming + arrived_ref[peer, rows].astype(F32)
        if image == IMG:
            term_ref[...] = incoming[:8]
            continue
        normed, inverse = normalize(block_ref[image].astype(F32))
        scaled = incoming * gain
        inner = jnp.mean(scaled * normed, axis=-1, keepdims=True)
        outgoing = inverse * (scaled - jnp.mean(scaled, axis=-1, keepdims=True) - normed * inner)
        results.append(upstream_ref[image].astype(F32) + outgoing)
    grads = jnp.concatenate(results, axis=0)
    for share in range(8):
        start = share * 160 // LANE * LANE
        offset = share * 160 - start
        lanes = min(256 if offset + 160 <= 256 else 384, WIDTH - start)
        window = grads[:, start : start + lanes]
        if offset:
            window = pltpu.roll(window, lanes - offset, 1)
        out_ref[share] = window[:, :160].astype(BF)


def norm_back(arrived, block_rows, upstream_rows, gain):
    return pl.pallas_call(
        norm_back_kernel,
        out_shape=(
            jax.ShapeDtypeStruct((8, 80, 160), BF),
            jax.ShapeDtypeStruct((8, WIDTH), F32),
        ),
        in_specs=[pl.BlockSpec(memory_space=pltpu.VMEM)] * 4,
        out_specs=(pl.BlockSpec(memory_space=pltpu.VMEM),) * 2,
        name="norm_back",
    )(arrived, block_rows, upstream_rows, gain)


def summed(blocks):
    return blocks.astype(F32).sum(axis=0)


def after(value, *earlier):
    return lax.optimization_barrier((value, *earlier))[0]


def rows_along(term, columns):
    blocks = term.reshape(8, 4, -1, columns)
    here = lax.axis_index("x")
    return [
        lax.dynamic_index_in_dim(blocks, lax.rem(here + at, 4), 1, keepdims=False)
        for at in range(4)
    ]


def near_sum(parts):
    got = [shifted(parts[at], "x", at) for at in (2, 1, 3)]
    total = parts[0].astype(F32)
    for rows in got:
        total = total + rows.astype(F32)
    return total.astype(BF)


def shards(grad_rows, features, block_in, patch_counts, owner, ln1_gain, w_qkv, w_out, w_proj):
    device = lax.axis_index(ENC)
    core = lax.axis_index("c")
    place = core * 4 + lax.axis_index("y")
    words = jnp.stack([core, place, lax.axis_index("y"), lax.axis_index("x")]).astype(jnp.int32)
    place_word = place.reshape(1).astype(jnp.int32)
    gain = ln1_gain.reshape(1, WIDTH)
    columns = grad_rows.shape[1]

    own_counts = lax.dynamic_index_in_dim(patch_counts, device, 0, keepdims=False)
    images = jnp.arange(PEERS * IMG, dtype=jnp.int32)
    block_of = images // IMG
    owners = owner.reshape(-1)
    ahead = (owners[:, None] == owners[None, :]) & (block_of[None, :] < block_of[:, None])
    target = owners * IMG + jnp.sum(ahead.astype(jnp.int32), axis=1)
    hits = target[None, :] == images[:, None]
    source_of = jnp.sum(jnp.where(hits, images[None, :], 0), axis=1)
    all_counts = jnp.sum(jnp.where(hits, patch_counts.reshape(1, -1), 0), axis=1)
    arrived_counts = lax.dynamic_slice_in_dim(all_counts, device * IMG, IMG, 0)

    halves = grad_rows.reshape(IMG, 2, 64, columns)
    for_other = lax.dynamic_index_in_dim(halves, 1 - core, 1, keepdims=False)
    for_own = lax.dynamic_index_in_dim(halves, core, 1, keepdims=False)
    part_other = dot(for_other.reshape(ROWS // 2, columns), w_proj, 1, 1).astype(BF)
    from_other = swapped(part_other)
    part_own = dot(for_own.reshape(ROWS // 2, columns), w_proj, 1, 1)
    pair = (part_own + from_other.astype(F32)).astype(BF)
    pair = pair.reshape(IMG, 4, 16, WIDTH).transpose(1, 0, 2, 3)
    features = after(features, pair)
    arrived = exchanged(pair.reshape(4, 80, WIDTH), "y").reshape(4, IMG, 16, WIDTH)

    line = jnp.arange(TILE, dtype=jnp.int32)
    live_own = (line[None, :] < own_counts[:, None]).reshape(-1)
    kept_rows = jnp.where(live_own[:, None], features, jnp.zeros_like(features))
    proj_term = dot(kept_rows, grad_rows, 0, 0).astype(BF)
    arrived = after(arrived, proj_term)
    pieces = spread(place_word, own_counts, arrived)
    proj_near = near_sum(rows_along(proj_term, columns))

    share = after(block_in.T, arrived)
    shares = [share] + [shifted(share, "y", at) for at in (1, 2, 3)]
    block_own = jnp.stack(shares)
    block_other = swapped(block_own)

    w_heads = w_qkv.transpose(1, 2, 0).reshape(6 * HEAD, WIDTH)
    normed_in, normed, block_rows, packed, prob, mixed = attention(
        words, arrived_counts, block_own, block_other, gain, w_heads
    )

    passing = exchanged(pieces, ENC)
    passing = forwarded(source_of, passing)
    landed = exchanged(passing, ENC)
    upstream_rows, copies = collected(landed)
    half_own = exchanged(copies.reshape(4, 80, WIDTH), "y").reshape(4, IMG, 16, WIDTH)
    half_other = swapped(half_own)

    proj_far = exchanged(after(proj_near, half_own), "z")

    upstream, packed_grad, in_own, in_other = backward(
        words, half_own, half_other, w_out, w_heads, packed, prob, normed
    )
    in_got = swapped(in_other)
    terms = weight_terms(words, normed_in, upstream, packed_grad, mixed)
    in_pair = (in_own.astype(F32) + in_got.astype(F32)).astype(BF)
    in_pair = in_pair.reshape(4, 96, WIDTH)
    in_pair, proj_far = lax.optimization_barrier((in_pair, proj_far))
    grad_proj = summed(proj_far)
    in_arrived = exchanged(in_pair, "y")
    term_near = near_sum(terms)
    shares, gain_term = norm_back(in_arrived, block_rows, upstream_rows, gain)
    shares = exchanged(shares, TP)
    grad_input = shares.reshape(4, 2, IMG, 16, 160).transpose(2, 1, 0, 3, 4)
    grad_input = grad_input.reshape(ROWS, 160)
    gain_rows = gain_term[0].astype(BF).reshape(8, 4, 40).transpose(1, 0, 2)
    gain_rows = gain_rows.reshape(4, 1, 320)
    here = lax.axis_index("x")
    gain_parts = [
        lax.dynamic_index_in_dim(gain_rows, lax.rem(here + at, 4), 0, keepdims=False)
        for at in range(4)
    ]
    gain_near = near_sum(gain_parts).reshape(8, 40, 1)
    last = jnp.concatenate([term_near, jnp.pad(gain_near, ((0, 0), (0, 0), (0, 127)))], axis=2)
    last = summed(exchanged(last, "z"))
    grad_qkv = last[:, :480].reshape(40, 2, 240)
    grad_out = last[:, 480:640].T
    grad_ln1 = last[:, 640]
    return (grad_input, grad_proj, grad_qkv, grad_out, grad_ln1)


def solution(mesh):
    torus = Mesh(mesh.devices.reshape(8, 4, 4, 2), ("z", "x", "y", "c"))

    return jax.shard_map(
        shards,
        mesh=torus,
        in_specs=(
            P(ENC, TP),
            P(ENC, None),
            P(ENC, TP),
            P(),
            P(),
            P(),
            P(None, TP, None),
            P(TP, None),
            P(None, TP),
        ),
        out_specs=(P(ENC, TP), P(ENC, TP), P(ENC, TP, None), P(TP, ENC), P(ENC)),
        check_vma=False,
    )
```

```python
import jax
import jax.numpy as jnp
from jax import lax
from jax.experimental import pallas as pl
from jax.experimental.pallas import tpu as pltpu
from jax.sharding import Mesh
from jax.sharding import PartitionSpec as P


TILE = 128
IMG = 5
ROWS = IMG * TILE
WIDTH = 1280
HEAD = 80
LANE = 128
PEERS = 32
ENC = ("z", "x")
TP = ("y", "c")
EPSILON = 1e-05
SCALING = 1.0 / HEAD**0.5
BF = jnp.bfloat16
F32 = jnp.float32
SWAP = ((0, 1), (1, 0))


def padded_heads(padded_ref, heads_ref):
    for at in range(heads_ref.shape[0] // HEAD):
        padded_ref[at * LANE : at * LANE + HEAD] = heads_ref[at * HEAD : (at + 1) * HEAD]
        padded_ref[at * LANE + HEAD : (at + 1) * LANE] = jnp.zeros((LANE - HEAD, WIDTH), BF)


def exchanged(blocks, axis):
    return lax.all_to_all(blocks, axis, split_axis=0, concat_axis=0, tiled=True)


def shifted(values, axis, by):
    pairs = tuple((i, (i + by) % 4) for i in range(4))
    return lax.ppermute(values, axis, pairs)


def swapped(values):
    return lax.ppermute(values, "c", SWAP)


def dot(left, right, dim_left, dim_right):
    return lax.dot_general(
        left, right, (((dim_left,), (dim_right,)), ((), ())), preferred_element_type=F32
    )


def smem():
    return pl.BlockSpec(memory_space=pltpu.SMEM)


def normalize(values):
    centred = values - jnp.mean(values, axis=-1, keepdims=True)
    variance = jnp.mean(centred * centred, axis=-1, keepdims=True)
    inverse = lax.rsqrt(variance + EPSILON)
    return (centred * inverse, inverse)


def shifted_sum(pieces, lanes):
    total = None
    for at, piece in enumerate(pieces):
        wide = jnp.concatenate(
            [piece, jnp.zeros((piece.shape[0], lanes - LANE), piece.dtype)], axis=1
        )
        if at:
            wide = pltpu.roll(wide, HEAD * at, 1)
        total = wide if total is None else total + wide
    return total


def spread_kernel(place_ref, counts_ref, arrived_ref, out_ref):
    first_row = place_ref[0] * 16
    for image in range(IMG):
        rows = arrived_ref[0, image].astype(F32)
        for peer in range(1, 4):
            rows = rows + arrived_ref[peer, image].astype(F32)
        line = first_row + lax.broadcasted_iota(jnp.int32, rows.shape, 0)
        rows = jnp.where(line < counts_ref[image], rows, 0.0).astype(BF)
        for half in range(2):
            for group in range(10):
                out_ref[half * 10 + group, image] = rows[
                    half * 8 : half * 8 + 8, group * LANE : (group + 1) * LANE
                ]
    out_ref[20:32] = jnp.zeros((12, IMG, 8, LANE), BF)


def spread(place, counts, arrived):
    return pl.pallas_call(
        spread_kernel,
        out_shape=jax.ShapeDtypeStruct((PEERS, IMG, 8, LANE), BF),
        in_specs=[smem(), smem(), pl.BlockSpec(memory_space=pltpu.VMEM)],
        out_specs=pl.BlockSpec(memory_space=pltpu.VMEM),
        name="spread",
    )(place, counts, arrived)


def forward_kernel(index_ref, pieces_ref, out_ref):
    def step(at, carry):
        out_ref[at] = pieces_ref[index_ref[at]]
        return carry

    lax.fori_loop(0, PEERS * IMG, step, 0, unroll=8)


def forwarded(index, pieces):
    flat = pieces.reshape(PEERS * IMG, 8, LANE)
    return pl.pallas_call(
        forward_kernel,
        out_shape=jax.ShapeDtypeStruct(flat.shape, BF),
        in_specs=[smem(), pl.BlockSpec(memory_space=pltpu.VMEM)],
        out_specs=pl.BlockSpec(memory_space=pltpu.VMEM),
        name="forwarded",
    )(index, flat).reshape(pieces.shape)


def collect_kernel(pieces_ref, rows_ref, copies_ref):
    for image in range(IMG):
        for half in range(2):
            for group in range(10):
                piece = pieces_ref[half * 10 + group, image]
                at = (slice(half * 8, half * 8 + 8), slice(group * LANE, (group + 1) * LANE))
                rows_ref[image, at[0], at[1]] = piece
                for peer in range(4):
                    copies_ref[peer, image, at[0], at[1]] = piece


def collected(pieces):
    return pl.pallas_call(
        collect_kernel,
        out_shape=(
            jax.ShapeDtypeStruct((IMG, 16, WIDTH), BF),
            jax.ShapeDtypeStruct((4, IMG, 16, WIDTH), BF),
        ),
        in_specs=[pl.BlockSpec(memory_space=pltpu.VMEM)],
        out_specs=(pl.BlockSpec(memory_space=pltpu.VMEM),) * 2,
        name="collected",
    )(pieces)


def attention_kernel(
    words_ref,
    counts_ref,
    own_ref,
    other_ref,
    gain_ref,
    w_ref,
    normed_in_ref,
    normed_ref,
    rows_ref,
    packed_ref,
    prob_ref,
    mixed_ref,
    scratch,
    w_pad,
):
    @pl.when(pl.program_id(0) == 0)
    def _():
        padded_heads(w_pad, w_ref)

    first = words_ref[0] == 0
    shares = []
    for near in range(4):
        at = lax.rem(words_ref[2] + 4 - near, 4)
        own, other = own_ref[at], other_ref[at]
        shares += [jnp.where(first, own, other), jnp.where(first, other, own)]
    values = jnp.concatenate(shares, axis=0).astype(F32).T
    scratch[...] = values
    rows_ref[0] = scratch[pl.ds(pl.multiple_of(words_ref[1] * 16, 16), 16), :].astype(BF)
    normed, _ = normalize(values)
    normed_ref[...] = normed.astype(BF)
    normed_in = (normed * gain_ref[...]).astype(BF)
    normed_in_ref[...] = normed_in
    packed = dot(normed_in, w_pad[...], 1, 1).astype(BF)
    packed_ref[...] = packed
    count = counts_ref[pl.program_id(0)]
    live_row = lax.broadcasted_iota(jnp.int32, (TILE, TILE), 0) < count
    live_col = lax.broadcasted_iota(jnp.int32, (TILE, TILE), 1) < count
    same_kind = (live_row & live_col) | (~live_row & ~live_col)
    mixed = []
    for head in range(2):
        query, key, value = (
            packed[:, (head * 3 + i) * LANE : (head * 3 + i + 1) * LANE] for i in range(3)
        )
        scores = jnp.where(same_kind, dot(query, key, 1, 1) * SCALING, -1e30)
        exp_terms = jnp.exp(scores - jnp.max(scores, axis=-1, keepdims=True))
        probability = exp_terms / jnp.sum(exp_terms, axis=-1, keepdims=True)
        prob_ref[0, head] = probability
        mixed.append(dot(probability.astype(BF), value, 1, 0))
    mixed_ref[...] = shifted_sum(mixed, 256)[:, :160].astype(BF)


def attention(words, counts, own, other, gain, w_heads):
    share = pl.BlockSpec((4, 160, TILE), lambda i: (0, 0, i))
    rows = pl.BlockSpec((TILE, WIDTH), lambda i: (i, 0))
    return pl.pallas_call(
        attention_kernel,
        grid=(IMG,),
        out_shape=(
            jax.ShapeDtypeStruct((ROWS, WIDTH), BF),
            jax.ShapeDtypeStruct((ROWS, WIDTH), BF),
            jax.ShapeDtypeStruct((IMG, 16, WIDTH), BF),
            jax.ShapeDtypeStruct((ROWS, 6 * LANE), BF),
            jax.ShapeDtypeStruct((IMG, 2, TILE, TILE), F32),
            jax.ShapeDtypeStruct((ROWS, 2 * HEAD), BF),
        ),
        in_specs=[
            smem(),
            smem(),
            share,
            share,
            pl.BlockSpec((1, WIDTH), lambda i: (0, 0)),
            pl.BlockSpec((6 * HEAD, WIDTH), lambda i: (0, 0)),
        ],
        out_specs=(
            rows,
            rows,
            pl.BlockSpec((1, 16, WIDTH), lambda i: (i, 0, 0)),
            pl.BlockSpec((TILE, 6 * LANE), lambda i: (i, 0)),
            pl.BlockSpec((1, 2, TILE, TILE), lambda i: (i, 0, 0, 0)),
            pl.BlockSpec((TILE, 2 * HEAD), lambda i: (i, 0)),
        ),
        scratch_shapes=[pltpu.VMEM((TILE, WIDTH), F32), pltpu.VMEM((6 * LANE, WIDTH), BF)],
        cost_estimate=pl.CostEstimate(
            flops=10_000_000_000, bytes_accessed=10_000_000, transcendentals=0
        ),
        name="attention",
    )(words, counts, own, other, gain, w_heads)


def backward_kernel(
    words_ref,
    own_ref,
    other_ref,
    wout_ref,
    w_ref,
    packed_ref,
    prob_ref,
    normed_ref,
    upstream_ref,
    packed_grad_ref,
    in_own_ref,
    in_other_ref,
    wout_pad,
):
    padded_heads(wout_pad, wout_ref)
    first = words_ref[0] == 0
    for image in range(IMG):
        own = own_ref[:, image].reshape(64, WIDTH)
        other = other_ref[:, image].reshape(64, WIDTH)
        at = image * TILE
        upstream_ref[at : at + 64] = jnp.where(first, own, other)
        upstream_ref[at + 64 : at + TILE] = jnp.where(first, other, own)
    mixed_grads = dot(upstream_ref[...], wout_pad[...], 1, 1).astype(BF)

    units = [(image, head) for image in range(IMG) for head in range(2)]

    def part(image, head, which):
        lane = (head * 3 + which) * LANE
        return packed_ref[image * TILE : (image + 1) * TILE, lane : lane + LANE]

    grads = [
        mixed_grads[image * TILE : (image + 1) * TILE, head * LANE : (head + 1) * LANE]
        for image, head in units
    ]
    prob_grads = [dot(grad, part(*unit, 2), 1, 1) for grad, unit in zip(grads, units)]
    score_grads = []
    for (image, head), prob_grad in zip(units, prob_grads):
        probability = prob_ref[image, head]
        inner = jnp.sum(probability * prob_grad, axis=-1, keepdims=True)
        score_grads.append((probability * (prob_grad - inner) * SCALING).astype(BF))
    query_grads = [dot(grad, part(*unit, 1), 1, 0) for grad, unit in zip(score_grads, units)]
    key_grads = [dot(grad, part(*unit, 0), 0, 0) for grad, unit in zip(score_grads, units)]
    value_grads = [
        dot(prob_ref[image, head].astype(BF), grad, 0, 0)
        for grad, (image, head) in zip(grads, units)
    ]
    for image in range(IMG):
        pieces = []
        for head in range(2):
            at = image * 2 + head
            pieces += [query_grads[at], key_grads[at], value_grads[at]]
        packed_grad_ref[image * TILE : (image + 1) * TILE] = shifted_sum(pieces, 512)[
            :, :480
        ].astype(BF)
    in_parts = dot(packed_grad_ref[...], w_ref[...], 1, 0).astype(BF)
    gain_term = jnp.sum(in_parts.astype(F32) * normed_ref[...].astype(F32), axis=0, keepdims=True)
    row = lax.broadcasted_iota(jnp.int32, (16, WIDTH), 0)
    plane = jnp.where(row == 0, gain_term, 0.0).astype(BF)
    for near in range(4):
        to = lax.rem(near + 4 - words_ref[2], 4)
        for image in range(IMG):
            at = image * TILE + near * 16
            low, high = in_parts[at : at + 16], in_parts[at + 64 : at + 80]
            in_own_ref[to, image] = jnp.where(first, low, high)
            in_other_ref[to, image] = jnp.where(first, high, low)
        in_own_ref[near, IMG] = plane
        in_other_ref[near, IMG] = plane


def backward(words, own, other, w_out, w_heads, packed, prob, normed):
    return pl.pallas_call(
        backward_kernel,
        out_shape=(
            jax.ShapeDtypeStruct((ROWS, WIDTH), BF),
            jax.ShapeDtypeStruct((ROWS, 6 * HEAD), BF),
            jax.ShapeDtypeStruct((4, IMG + 1, 16, WIDTH), BF),
            jax.ShapeDtypeStruct((4, IMG + 1, 16, WIDTH), BF),
        ),
        in_specs=[smem()] + [pl.BlockSpec(memory_space=pltpu.VMEM)] * 7,
        out_specs=(pl.BlockSpec(memory_space=pltpu.VMEM),) * 4,
        scratch_shapes=[pltpu.VMEM((2 * LANE, WIDTH), BF)],
        cost_estimate=pl.CostEstimate(
            flops=10_000_000_000, bytes_accessed=10_000_000, transcendentals=0
        ),
        name="backward",
    )(words, own, other, w_out, w_heads, packed, prob, normed)


def weights_kernel(
    words_ref, normed_ref, upstream_ref, packed_grad_ref, mixed_ref, *out_refs_and_scratch
):
    *out_refs, scratch = out_refs_and_scratch
    qkv = dot(normed_ref[...], packed_grad_ref[...], 0, 0)
    out = dot(upstream_ref[...], mixed_ref[...], 0, 0)
    term = jnp.concatenate([qkv, out], axis=1)
    for at in range(16):
        scratch[at] = term[at * 40 : (at + 1) * 40].astype(BF)
    for by, out_ref in enumerate(out_refs):
        near = lax.rem(words_ref[3] + by, 4)
        for far in range(4):
            out_ref[far] = scratch[far * 4 + near]


def weight_terms(words, normed, upstream, packed_grad, mixed):
    return pl.pallas_call(
        weights_kernel,
        grid=(2,),
        out_shape=(jax.ShapeDtypeStruct((8, 40, 640), BF),) * 4,
        in_specs=[
            smem(),
            pl.BlockSpec((ROWS, 640), lambda i: (0, i)),
            pl.BlockSpec((ROWS, 640), lambda i: (0, i)),
            pl.BlockSpec((ROWS, 6 * HEAD), lambda i: (0, 0)),
            pl.BlockSpec((ROWS, 2 * HEAD), lambda i: (0, 0)),
        ],
        out_specs=(pl.BlockSpec((4, 40, 640), lambda i: (i, 0, 0)),) * 4,
        scratch_shapes=[pltpu.VMEM((16, 40, 640), BF)],
        cost_estimate=pl.CostEstimate(
            flops=4_000_000_000, bytes_accessed=6_000_000, transcendentals=0
        ),
        name="weight_terms",
    )(words, normed, upstream, packed_grad, mixed)


def norm_back_kernel(
    own_ref, got_ref, got2_ref, got3_ref, block_ref, upstream_ref, gain_ref, out_ref, term_ref
):
    gain = gain_ref[...]
    results = []
    for image in range(IMG + 1):
        incoming = own_ref[image].astype(F32)
        for more_ref in (got_ref, got2_ref, got3_ref):
            incoming = incoming + more_ref[image].astype(F32)
        if image == IMG:
            term_ref[...] = incoming[:8]
            continue
        normed, inverse = normalize(block_ref[image].astype(F32))
        scaled = incoming * gain
        inner = jnp.mean(scaled * normed, axis=-1, keepdims=True)
        outgoing = inverse * (scaled - jnp.mean(scaled, axis=-1, keepdims=True) - normed * inner)
        results.append(upstream_ref[image].astype(F32) + outgoing)
    grads = jnp.concatenate(results, axis=0)
    for share in range(8):
        start = share * 160 // LANE * LANE
        offset = share * 160 - start
        lanes = min(256 if offset + 160 <= 256 else 384, WIDTH - start)
        window = grads[:, start : start + lanes]
        if offset:
            window = pltpu.roll(window, lanes - offset, 1)
        out_ref[share] = window[:, :160].astype(BF)


def norm_back(parts, block_rows, upstream_rows, gain):
    return pl.pallas_call(
        norm_back_kernel,
        out_shape=(
            jax.ShapeDtypeStruct((8, 80, 160), BF),
            jax.ShapeDtypeStruct((8, WIDTH), F32),
        ),
        in_specs=[pl.BlockSpec(memory_space=pltpu.VMEM)] * 7,
        out_specs=(pl.BlockSpec(memory_space=pltpu.VMEM),) * 2,
        name="norm_back",
    )(*parts, block_rows, upstream_rows, gain)


def summed(blocks):
    return blocks.astype(F32).sum(axis=0)


def after(value, *earlier):
    return lax.optimization_barrier((value, *earlier))[0]


def rows_along(term, columns):
    blocks = term.reshape(8, 4, -1, columns)
    here = lax.axis_index("x")
    return [
        lax.dynamic_index_in_dim(blocks, lax.rem(here + at, 4), 1, keepdims=False)
        for at in range(4)
    ]


def near_sum(parts):
    got = [shifted(parts[at], "x", at) for at in (2, 1, 3)]
    total = parts[0].astype(F32)
    for rows in got:
        total = total + rows.astype(F32)
    return total.astype(BF)


def shards(grad_rows, features, block_in, patch_counts, owner, ln1_gain, w_qkv, w_out, w_proj):
    device = lax.axis_index(ENC)
    core = lax.axis_index("c")
    place = core * 4 + lax.axis_index("y")
    words = jnp.stack([core, place, lax.axis_index("y"), lax.axis_index("x")]).astype(jnp.int32)
    place_word = place.reshape(1).astype(jnp.int32)
    gain = ln1_gain.reshape(1, WIDTH)
    columns = grad_rows.shape[1]

    own_counts = lax.dynamic_index_in_dim(patch_counts, device, 0, keepdims=False)
    images = jnp.arange(PEERS * IMG, dtype=jnp.int32)
    block_of = images // IMG
    owners = owner.reshape(-1)
    ahead = (owners[:, None] == owners[None, :]) & (block_of[None, :] < block_of[:, None])
    target = owners * IMG + jnp.sum(ahead.astype(jnp.int32), axis=1)
    hits = target[None, :] == images[:, None]
    source_of = jnp.sum(jnp.where(hits, images[None, :], 0), axis=1)
    all_counts = jnp.sum(jnp.where(hits, patch_counts.reshape(1, -1), 0), axis=1)
    arrived_counts = lax.dynamic_slice_in_dim(all_counts, device * IMG, IMG, 0)

    halves = grad_rows.reshape(IMG, 2, 64, columns)
    for_other = lax.dynamic_index_in_dim(halves, 1 - core, 1, keepdims=False)
    for_own = lax.dynamic_index_in_dim(halves, core, 1, keepdims=False)
    part_other = dot(for_other.reshape(ROWS // 2, columns), w_proj, 1, 1).astype(BF)
    from_other = swapped(part_other)
    part_own = dot(for_own.reshape(ROWS // 2, columns), w_proj, 1, 1)
    pair = (part_own + from_other.astype(F32)).astype(BF)
    pair = pair.reshape(IMG, 4, 16, WIDTH).transpose(1, 0, 2, 3)
    features = after(features, pair)
    arrived = exchanged(pair.reshape(4, 80, WIDTH), "y").reshape(4, IMG, 16, WIDTH)

    line = jnp.arange(TILE, dtype=jnp.int32)
    live_own = (line[None, :] < own_counts[:, None]).reshape(-1)
    kept_rows = jnp.where(live_own[:, None], features, jnp.zeros_like(features))
    proj_term = dot(kept_rows, grad_rows, 0, 0).astype(BF)
    arrived = after(arrived, proj_term)
    pieces = spread(place_word, own_counts, arrived)
    proj_near = near_sum(rows_along(proj_term, columns))

    share = after(block_in.T, arrived)
    shares = [share] + [shifted(share, "y", at) for at in (1, 2, 3)]
    block_own = jnp.stack(shares)
    block_other = swapped(block_own)

    w_heads = w_qkv.transpose(1, 2, 0).reshape(6 * HEAD, WIDTH)
    normed_in, normed, block_rows, packed, prob, mixed = attention(
        words, arrived_counts, block_own, block_other, gain, w_heads
    )

    passing = exchanged(pieces, ENC)
    passing = forwarded(source_of, passing)
    landed = exchanged(passing, ENC)
    upstream_rows, copies = collected(landed)
    half_own = exchanged(copies.reshape(4, 80, WIDTH), "y").reshape(4, IMG, 16, WIDTH)
    half_other = swapped(half_own)

    proj_far = exchanged(after(proj_near, half_own), "z")

    upstream, packed_grad, in_own, in_other = backward(
        words, half_own, half_other, w_out, w_heads, packed, prob, normed
    )
    in_got = swapped(in_other)
    terms = weight_terms(words, normed_in, upstream, packed_grad, mixed)
    grad_proj = summed(proj_far)
    in_pair = [
        (own.astype(F32) + got.astype(F32)).astype(BF) for own, got in zip(in_own, in_got)
    ]
    in_parts = [in_pair[0]] + [shifted(in_pair[at], "y", at) for at in (2, 1, 3)]
    term_near = near_sum(terms)
    shares, gain_term = norm_back(in_parts, block_rows, upstream_rows, gain)
    shares = exchanged(shares, TP)
    grad_input = shares.reshape(4, 2, IMG, 16, 160).transpose(2, 1, 0, 3, 4)
    grad_input = grad_input.reshape(ROWS, 160)
    gain_rows = gain_term[0].astype(BF).reshape(8, 4, 40).transpose(1, 0, 2)
    gain_rows = gain_rows.reshape(4, 1, 320)
    here = lax.axis_index("x")
    gain_parts = [
        lax.dynamic_index_in_dim(gain_rows, lax.rem(here + at, 4), 0, keepdims=False)
        for at in range(4)
    ]
    gain_near = near_sum(gain_parts).reshape(8, 40, 1)
    last = jnp.concatenate([term_near, jnp.pad(gain_near, ((0, 0), (0, 0), (0, 127)))], axis=2)
    last = summed(exchanged(last, "z"))
    grad_qkv = last[:, :480].reshape(40, 2, 240)
    grad_out = last[:, 480:640].T
    grad_ln1 = last[:, 640]
    return (grad_input, grad_proj, grad_qkv, grad_out, grad_ln1)


def solution(mesh):
    torus = Mesh(mesh.devices.reshape(8, 4, 4, 2), ("z", "x", "y", "c"))

    return jax.shard_map(
        shards,
        mesh=torus,
        in_specs=(
            P(ENC, TP),
            P(ENC, None),
            P(ENC, TP),
            P(),
            P(),
            P(),
            P(None, TP, None),
            P(TP, None),
            P(None, TP),
        ),
        out_specs=(P(ENC, TP), P(ENC, TP), P(ENC, TP, None), P(TP, ENC), P(ENC)),
        check_vma=False,
    )
```

```python
import jax
import jax.numpy as jnp
from jax import lax
from jax.experimental import pallas as pl
from jax.experimental.pallas import tpu as pltpu
from jax.sharding import Mesh
from jax.sharding import PartitionSpec as P


TILE = 128
IMG = 5
ROWS = IMG * TILE
WIDTH = 1280
HEAD = 80
LANE = 128
PEERS = 32
ENC = ("z", "x")
TP = ("y", "c")
EPSILON = 1e-05
SCALING = 1.0 / HEAD**0.5
BF = jnp.bfloat16
F32 = jnp.float32
SWAP = ((0, 1), (1, 0))


def padded_heads(padded_ref, heads_ref):
    for at in range(heads_ref.shape[0] // HEAD):
        padded_ref[at * LANE : at * LANE + HEAD] = heads_ref[at * HEAD : (at + 1) * HEAD]
        padded_ref[at * LANE + HEAD : (at + 1) * LANE] = jnp.zeros((LANE - HEAD, WIDTH), BF)


def exchanged(blocks, axis):
    return lax.all_to_all(blocks, axis, split_axis=0, concat_axis=0, tiled=True)


def shifted(values, axis, by):
    pairs = tuple((i, (i + by) % 4) for i in range(4))
    return lax.ppermute(values, axis, pairs)


def swapped(values):
    return lax.ppermute(values, "c", SWAP)


def dot(left, right, dim_left, dim_right):
    return lax.dot_general(
        left, right, (((dim_left,), (dim_right,)), ((), ())), preferred_element_type=F32
    )


def smem():
    return pl.BlockSpec(memory_space=pltpu.SMEM)


def normalize(values):
    centred = values - jnp.mean(values, axis=-1, keepdims=True)
    variance = jnp.mean(centred * centred, axis=-1, keepdims=True)
    inverse = lax.rsqrt(variance + EPSILON)
    return (centred * inverse, inverse)


def shifted_sum(pieces, lanes):
    total = None
    for at, piece in enumerate(pieces):
        wide = jnp.concatenate(
            [piece, jnp.zeros((piece.shape[0], lanes - LANE), piece.dtype)], axis=1
        )
        if at:
            wide = pltpu.roll(wide, HEAD * at, 1)
        total = wide if total is None else total + wide
    return total


def spread_kernel(place_ref, counts_ref, arrived_ref, out_ref):
    first_row = place_ref[0] * 16
    for image in range(IMG):
        rows = arrived_ref[0, image].astype(F32)
        for peer in range(1, 4):
            rows = rows + arrived_ref[peer, image].astype(F32)
        line = first_row + lax.broadcasted_iota(jnp.int32, rows.shape, 0)
        rows = jnp.where(line < counts_ref[image], rows, 0.0).astype(BF)
        for half in range(2):
            for group in range(10):
                out_ref[half * 10 + group, image] = rows[
                    half * 8 : half * 8 + 8, group * LANE : (group + 1) * LANE
                ]
    out_ref[20:32] = jnp.zeros((12, IMG, 8, LANE), BF)


def spread(place, counts, arrived):
    return pl.pallas_call(
        spread_kernel,
        out_shape=jax.ShapeDtypeStruct((PEERS, IMG, 8, LANE), BF),
        in_specs=[smem(), smem(), pl.BlockSpec(memory_space=pltpu.VMEM)],
        out_specs=pl.BlockSpec(memory_space=pltpu.VMEM),
        name="spread",
    )(place, counts, arrived)


def forward_kernel(index_ref, pieces_ref, out_ref):
    def step(at, carry):
        out_ref[at] = pieces_ref[index_ref[at]]
        return carry

    lax.fori_loop(0, PEERS * IMG, step, 0, unroll=8)


def forwarded(index, pieces):
    flat = pieces.reshape(PEERS * IMG, 8, LANE)
    return pl.pallas_call(
        forward_kernel,
        out_shape=jax.ShapeDtypeStruct(flat.shape, BF),
        in_specs=[smem(), pl.BlockSpec(memory_space=pltpu.VMEM)],
        out_specs=pl.BlockSpec(memory_space=pltpu.VMEM),
        name="forwarded",
    )(index, flat).reshape(pieces.shape)


def collect_kernel(pieces_ref, rows_ref, copies_ref):
    for image in range(IMG):
        for half in range(2):
            for group in range(10):
                piece = pieces_ref[half * 10 + group, image]
                at = (slice(half * 8, half * 8 + 8), slice(group * LANE, (group + 1) * LANE))
                rows_ref[image, at[0], at[1]] = piece
                for peer in range(4):
                    copies_ref[peer, image, at[0], at[1]] = piece


def collected(pieces):
    return pl.pallas_call(
        collect_kernel,
        out_shape=(
            jax.ShapeDtypeStruct((IMG, 16, WIDTH), BF),
            jax.ShapeDtypeStruct((4, IMG, 16, WIDTH), BF),
        ),
        in_specs=[pl.BlockSpec(memory_space=pltpu.VMEM)],
        out_specs=(pl.BlockSpec(memory_space=pltpu.VMEM),) * 2,
        name="collected",
    )(pieces)


def attention_kernel(
    words_ref,
    counts_ref,
    own_ref,
    other_ref,
    gain_ref,
    w_ref,
    normed_in_ref,
    normed_ref,
    rows_ref,
    packed_ref,
    prob_ref,
    mixed_ref,
    scratch,
    w_pad,
):
    padded_heads(w_pad, w_ref)
    first = words_ref[0] == 0
    gain = gain_ref[...]
    for image in range(IMG):
        lanes = slice(image * TILE, (image + 1) * TILE)
        shares = []
        for near in range(4):
            at = lax.rem(words_ref[2] + 4 - near, 4)
            own, other = own_ref[at, :, lanes], other_ref[at, :, lanes]
            shares += [jnp.where(first, own, other), jnp.where(first, other, own)]
        values = jnp.concatenate(shares, axis=0).astype(F32).T
        scratch[image] = values
        rows = scratch[image, pl.ds(pl.multiple_of(words_ref[1] * 16, 16), 16), :]
        rows_ref[image] = rows.astype(BF)
        normed, _ = normalize(values)
        normed_ref[lanes] = normed.astype(BF)
        normed_in_ref[lanes] = (normed * gain).astype(BF)
    packed_ref[...] = dot(normed_in_ref[...], w_pad[...], 1, 1).astype(BF)

    units = [(image, head) for image in range(IMG) for head in range(2)]

    def part(image, head, which):
        lane = (head * 3 + which) * LANE
        return packed_ref[image * TILE : (image + 1) * TILE, lane : lane + LANE]

    scores = [dot(part(*unit, 0), part(*unit, 1), 1, 1) * SCALING for unit in units]
    line = lax.broadcasted_iota(jnp.int32, (TILE, TILE), 0)
    column = lax.broadcasted_iota(jnp.int32, (TILE, TILE), 1)
    for (image, head), score in zip(units, scores):
        live_row, live_col = line < counts_ref[image], column < counts_ref[image]
        same_kind = (live_row & live_col) | (~live_row & ~live_col)
        score = jnp.where(same_kind, score, -1e30)
        exp_terms = jnp.exp(score - jnp.max(score, axis=-1, keepdims=True))
        prob_ref[image, head] = exp_terms / jnp.sum(exp_terms, axis=-1, keepdims=True)
    mixed = [
        dot(prob_ref[image, head].astype(BF), part(image, head, 2), 1, 0) for image, head in units
    ]
    for image in range(IMG):
        pair = shifted_sum(mixed[image * 2 : image * 2 + 2], 256)[:, :160]
        mixed_ref[image * TILE : (image + 1) * TILE] = pair.astype(BF)


def attention(words, counts, own, other, gain, w_heads):
    whole = pl.BlockSpec(memory_space=pltpu.VMEM)
    return pl.pallas_call(
        attention_kernel,
        out_shape=(
            jax.ShapeDtypeStruct((ROWS, WIDTH), BF),
            jax.ShapeDtypeStruct((ROWS, WIDTH), BF),
            jax.ShapeDtypeStruct((IMG, 16, WIDTH), BF),
            jax.ShapeDtypeStruct((ROWS, 6 * LANE), BF),
            jax.ShapeDtypeStruct((IMG, 2, TILE, TILE), F32),
            jax.ShapeDtypeStruct((ROWS, 2 * HEAD), BF),
        ),
        in_specs=[smem(), smem(), whole, whole, whole, whole],
        out_specs=(whole,) * 6,
        scratch_shapes=[
            pltpu.VMEM((IMG, TILE, WIDTH), F32),
            pltpu.VMEM((6 * LANE, WIDTH), BF),
        ],
        cost_estimate=pl.CostEstimate(
            flops=10_000_000_000, bytes_accessed=10_000_000, transcendentals=0
        ),
        name="attention",
    )(words, counts, own, other, gain, w_heads)


def backward_kernel(
    words_ref,
    own_ref,
    other_ref,
    wout_ref,
    w_ref,
    packed_ref,
    prob_ref,
    normed_ref,
    upstream_ref,
    packed_grad_ref,
    in_own_ref,
    in_other_ref,
    wout_pad,
):
    padded_heads(wout_pad, wout_ref)
    first = words_ref[0] == 0
    for image in range(IMG):
        own = own_ref[:, image].reshape(64, WIDTH)
        other = other_ref[:, image].reshape(64, WIDTH)
        at = image * TILE
        upstream_ref[at : at + 64] = jnp.where(first, own, other)
        upstream_ref[at + 64 : at + TILE] = jnp.where(first, other, own)
    mixed_grads = dot(upstream_ref[...], wout_pad[...], 1, 1).astype(BF)

    units = [(image, head) for image in range(IMG) for head in range(2)]

    def part(image, head, which):
        lane = (head * 3 + which) * LANE
        return packed_ref[image * TILE : (image + 1) * TILE, lane : lane + LANE]

    grads = [
        mixed_grads[image * TILE : (image + 1) * TILE, head * LANE : (head + 1) * LANE]
        for image, head in units
    ]
    prob_grads = [dot(grad, part(*unit, 2), 1, 1) for grad, unit in zip(grads, units)]
    score_grads = []
    for (image, head), prob_grad in zip(units, prob_grads):
        probability = prob_ref[image, head]
        inner = jnp.sum(probability * prob_grad, axis=-1, keepdims=True)
        score_grads.append((probability * (prob_grad - inner) * SCALING).astype(BF))
    query_grads = [dot(grad, part(*unit, 1), 1, 0) for grad, unit in zip(score_grads, units)]
    key_grads = [dot(grad, part(*unit, 0), 0, 0) for grad, unit in zip(score_grads, units)]
    value_grads = [
        dot(prob_ref[image, head].astype(BF), grad, 0, 0)
        for grad, (image, head) in zip(grads, units)
    ]
    for image in range(IMG):
        pieces = []
        for head in range(2):
            at = image * 2 + head
            pieces += [query_grads[at], key_grads[at], value_grads[at]]
        packed_grad_ref[image * TILE : (image + 1) * TILE] = shifted_sum(pieces, 512)[
            :, :480
        ].astype(BF)
    in_parts = dot(packed_grad_ref[...], w_ref[...], 1, 0).astype(BF)
    gain_term = jnp.sum(in_parts.astype(F32) * normed_ref[...].astype(F32), axis=0, keepdims=True)
    row = lax.broadcasted_iota(jnp.int32, (16, WIDTH), 0)
    plane = jnp.where(row == 0, gain_term, 0.0).astype(BF)
    for near in range(4):
        to = lax.rem(near + 4 - words_ref[2], 4)
        for image in range(IMG):
            at = image * TILE + near * 16
            low, high = in_parts[at : at + 16], in_parts[at + 64 : at + 80]
            in_own_ref[to, image] = jnp.where(first, low, high)
            in_other_ref[to, image] = jnp.where(first, high, low)
        in_own_ref[near, IMG] = plane
        in_other_ref[near, IMG] = plane


def backward(words, own, other, w_out, w_heads, packed, prob, normed):
    return pl.pallas_call(
        backward_kernel,
        out_shape=(
            jax.ShapeDtypeStruct((ROWS, WIDTH), BF),
            jax.ShapeDtypeStruct((ROWS, 6 * HEAD), BF),
            jax.ShapeDtypeStruct((4, IMG + 1, 16, WIDTH), BF),
            jax.ShapeDtypeStruct((4, IMG + 1, 16, WIDTH), BF),
        ),
        in_specs=[smem()] + [pl.BlockSpec(memory_space=pltpu.VMEM)] * 7,
        out_specs=(pl.BlockSpec(memory_space=pltpu.VMEM),) * 4,
        scratch_shapes=[pltpu.VMEM((2 * LANE, WIDTH), BF)],
        cost_estimate=pl.CostEstimate(
            flops=10_000_000_000, bytes_accessed=10_000_000, transcendentals=0
        ),
        name="backward",
    )(words, own, other, w_out, w_heads, packed, prob, normed)


def weights_kernel(
    words_ref, normed_ref, upstream_ref, packed_grad_ref, mixed_ref, *out_refs_and_scratch
):
    *out_refs, scratch = out_refs_and_scratch
    qkv = dot(normed_ref[...], packed_grad_ref[...], 0, 0)
    out = dot(upstream_ref[...], mixed_ref[...], 0, 0)
    term = jnp.concatenate([qkv, out], axis=1)
    for at in range(16):
        scratch[at] = term[at * 40 : (at + 1) * 40].astype(BF)
    for by, out_ref in enumerate(out_refs):
        near = lax.rem(words_ref[3] + by, 4)
        for far in range(4):
            out_ref[far] = scratch[far * 4 + near]


def weight_terms(words, normed, upstream, packed_grad, mixed):
    return pl.pallas_call(
        weights_kernel,
        grid=(2,),
        out_shape=(jax.ShapeDtypeStruct((8, 40, 640), BF),) * 4,
        in_specs=[
            smem(),
            pl.BlockSpec((ROWS, 640), lambda i: (0, i)),
            pl.BlockSpec((ROWS, 640), lambda i: (0, i)),
            pl.BlockSpec((ROWS, 6 * HEAD), lambda i: (0, 0)),
            pl.BlockSpec((ROWS, 2 * HEAD), lambda i: (0, 0)),
        ],
        out_specs=(pl.BlockSpec((4, 40, 640), lambda i: (i, 0, 0)),) * 4,
        scratch_shapes=[pltpu.VMEM((16, 40, 640), BF)],
        cost_estimate=pl.CostEstimate(
            flops=4_000_000_000, bytes_accessed=6_000_000, transcendentals=0
        ),
        name="weight_terms",
    )(words, normed, upstream, packed_grad, mixed)


def norm_back_kernel(
    words_ref,
    own_ref,
    got_ref,
    got2_ref,
    got3_ref,
    block_ref,
    upstream_ref,
    gain_ref,
    out_ref,
    other_ref,
    term_ref,
):
    gain = gain_ref[...]
    results = []
    for image in range(IMG + 1):
        incoming = own_ref[image].astype(F32)
        for more_ref in (got_ref, got2_ref, got3_ref):
            incoming = incoming + more_ref[image].astype(F32)
        if image == IMG:
            term_ref[...] = incoming[:8]
            continue
        normed, inverse = normalize(block_ref[image].astype(F32))
        scaled = incoming * gain
        inner = jnp.mean(scaled * normed, axis=-1, keepdims=True)
        outgoing = inverse * (scaled - jnp.mean(scaled, axis=-1, keepdims=True) - normed * inner)
        results.append(upstream_ref[image].astype(F32) + outgoing)
    grads = jnp.concatenate(results, axis=0)
    first = words_ref[0] == 0
    windows = []
    for share in range(8):
        start = share * 160 // LANE * LANE
        offset = share * 160 - start
        lanes = min(256 if offset + 160 <= 256 else 384, WIDTH - start)
        window = grads[:, start : start + lanes]
        if offset:
            window = pltpu.roll(window, lanes - offset, 1)
        windows.append(window[:, :160].astype(BF))
    for near in range(4):
        to = lax.rem(near + 4 - words_ref[2], 4)
        low, high = windows[near * 2], windows[near * 2 + 1]
        out_ref[to] = jnp.where(first, low, high)
        other_ref[to] = jnp.where(first, high, low)


def norm_back(words, parts, block_rows, upstream_rows, gain):
    whole = pl.BlockSpec(memory_space=pltpu.VMEM)
    return pl.pallas_call(
        norm_back_kernel,
        out_shape=(
            jax.ShapeDtypeStruct((4, 80, 160), BF),
            jax.ShapeDtypeStruct((4, 80, 160), BF),
            jax.ShapeDtypeStruct((8, WIDTH), F32),
        ),
        in_specs=[smem()] + [whole] * 7,
        out_specs=(whole,) * 3,
        name="norm_back",
    )(words, *parts, block_rows, upstream_rows, gain)


def assemble_kernel(words_ref, own_ref, got_ref, got2_ref, got3_ref, out_ref):
    for at, part_ref in enumerate((own_ref, got_ref, got2_ref, got3_ref)):
        near = lax.rem(words_ref[2] + 4 - at, 4)
        for image in range(IMG):
            rows = slice(image * 16, image * 16 + 16)
            out_ref[image, words_ref[0], near] = part_ref[0, rows]
            out_ref[image, 1 - words_ref[0], near] = part_ref[1, rows]


def assembled(words, parts):
    whole = pl.BlockSpec(memory_space=pltpu.VMEM)
    return pl.pallas_call(
        assemble_kernel,
        out_shape=jax.ShapeDtypeStruct((IMG, 2, 4, 16, 160), BF),
        in_specs=[smem()] + [whole] * 4,
        out_specs=whole,
        name="assembled",
    )(words, *parts)


def summed(blocks):
    return blocks.astype(F32).sum(axis=0)


def after(value, *earlier):
    return lax.optimization_barrier((value, *earlier))[0]


def rows_along(term, columns):
    blocks = term.reshape(8, 4, -1, columns)
    here = lax.axis_index("x")
    return [
        lax.dynamic_index_in_dim(blocks, lax.rem(here + at, 4), 1, keepdims=False)
        for at in range(4)
    ]


def near_sum(parts):
    got = [shifted(parts[at], "x", at) for at in (2, 1, 3)]
    total = parts[0].astype(F32)
    for rows in got:
        total = total + rows.astype(F32)
    return total.astype(BF)


def shards(grad_rows, features, block_in, patch_counts, owner, ln1_gain, w_qkv, w_out, w_proj):
    device = lax.axis_index(ENC)
    core = lax.axis_index("c")
    place = core * 4 + lax.axis_index("y")
    words = jnp.stack([core, place, lax.axis_index("y"), lax.axis_index("x")]).astype(jnp.int32)
    place_word = place.reshape(1).astype(jnp.int32)
    gain = ln1_gain.reshape(1, WIDTH)
    columns = grad_rows.shape[1]

    own_counts = lax.dynamic_index_in_dim(patch_counts, device, 0, keepdims=False)
    images = jnp.arange(PEERS * IMG, dtype=jnp.int32)
    block_of = images // IMG
    owners = owner.reshape(-1)
    ahead = (owners[:, None] == owners[None, :]) & (block_of[None, :] < block_of[:, None])
    target = owners * IMG + jnp.sum(ahead.astype(jnp.int32), axis=1)
    hits = target[None, :] == images[:, None]
    source_of = jnp.sum(jnp.where(hits, images[None, :], 0), axis=1)
    all_counts = jnp.sum(jnp.where(hits, patch_counts.reshape(1, -1), 0), axis=1)
    arrived_counts = lax.dynamic_slice_in_dim(all_counts, device * IMG, IMG, 0)

    halves = grad_rows.reshape(IMG, 2, 64, columns)
    for_other = lax.dynamic_index_in_dim(halves, 1 - core, 1, keepdims=False)
    for_own = lax.dynamic_index_in_dim(halves, core, 1, keepdims=False)
    part_other = dot(for_other.reshape(ROWS // 2, columns), w_proj, 1, 1).astype(BF)
    from_other = swapped(part_other)
    part_own = dot(for_own.reshape(ROWS // 2, columns), w_proj, 1, 1)
    pair = (part_own + from_other.astype(F32)).astype(BF)
    pair = pair.reshape(IMG, 4, 16, WIDTH).transpose(1, 0, 2, 3)
    features = after(features, pair)
    arrived = exchanged(pair.reshape(4, 80, WIDTH), "y").reshape(4, IMG, 16, WIDTH)

    line = jnp.arange(TILE, dtype=jnp.int32)
    live_own = (line[None, :] < own_counts[:, None]).reshape(-1)
    kept_rows = jnp.where(live_own[:, None], features, jnp.zeros_like(features))
    proj_term = dot(kept_rows, grad_rows, 0, 0).astype(BF)
    arrived = after(arrived, proj_term)
    pieces = spread(place_word, own_counts, arrived)
    proj_near = near_sum(rows_along(proj_term, columns))

    share = block_in.T
    shares = [share] + [shifted(share, "y", at) for at in (1, 2, 3)]
    block_own = jnp.stack(shares)
    block_other = swapped(block_own)

    w_heads = w_qkv.transpose(1, 2, 0).reshape(6 * HEAD, WIDTH)
    normed_in, normed, block_rows, packed, prob, mixed = attention(
        words, arrived_counts, block_own, block_other, gain, w_heads
    )

    passing = exchanged(pieces, ENC)
    passing = forwarded(source_of, passing)
    landed = exchanged(passing, ENC)
    upstream_rows, copies = collected(landed)
    half_own = exchanged(copies.reshape(4, 80, WIDTH), "y").reshape(4, IMG, 16, WIDTH)
    half_other = swapped(half_own)

    proj_far = exchanged(after(proj_near, half_own), "z")

    upstream, packed_grad, in_own, in_other = backward(
        words, half_own, half_other, w_out, w_heads, packed, prob, normed
    )
    in_got = swapped(in_other)
    terms = weight_terms(words, normed_in, upstream, packed_grad, mixed)
    grad_proj = summed(proj_far)
    in_pair = [
        (own.astype(F32) + got.astype(F32)).astype(BF) for own, got in zip(in_own, in_got)
    ]
    in_parts = [in_pair[0]] + [shifted(in_pair[at], "y", at) for at in (2, 1, 3)]
    term_near = near_sum(terms)
    for_own, for_other, gain_term = norm_back(words, in_parts, block_rows, upstream_rows, gain)
    from_other = swapped(for_other)
    blocks = jnp.stack([for_own, from_other], axis=1)
    parts = [blocks[0]] + [shifted(blocks[at], "y", at) for at in (1, 2, 3)]
    grad_input = assembled(words, parts).reshape(ROWS, 160)
    gain_rows = gain_term[0].astype(BF).reshape(8, 4, 40).transpose(1, 0, 2)
    gain_rows = gain_rows.reshape(4, 1, 320)
    here = lax.axis_index("x")
    gain_parts = [
        lax.dynamic_index_in_dim(gain_rows, lax.rem(here + at, 4), 0, keepdims=False)
        for at in range(4)
    ]
    gain_near = near_sum(gain_parts).reshape(8, 40, 1)
    last = jnp.concatenate([term_near, jnp.pad(gain_near, ((0, 0), (0, 0), (0, 127)))], axis=2)
    last = summed(exchanged(last, "z"))
    grad_qkv = last[:, :480].reshape(40, 2, 240)
    grad_out = last[:, 480:640].T
    grad_ln1 = last[:, 640]
    return (grad_input, grad_proj, grad_qkv, grad_out, grad_ln1)


def solution(mesh):
    torus = Mesh(mesh.devices.reshape(8, 4, 4, 2), ("z", "x", "y", "c"))

    return jax.shard_map(
        shards,
        mesh=torus,
        in_specs=(
            P(ENC, TP),
            P(ENC, None),
            P(ENC, TP),
            P(),
            P(),
            P(),
            P(None, TP, None),
            P(TP, None),
            P(None, TP),
        ),
        out_specs=(P(ENC, TP), P(ENC, TP), P(ENC, TP, None), P(TP, ENC), P(ENC)),
        check_vma=False,
    )
```
